32 devices in a mesh: gx: 4 (over z), gy: 4 (over y, x), gz: 2 (over core).
Axes of the slice: x: 2, y: 2, z: 4, core: 2. Of those that a mesh axis runs over, the one named last changes fastest.
Arguments:
- right_side: float32 [4, 96, 96, 48], P(None, 'gx', 'gy', 'gz'), may hold values from -6 to 6
- iterate: float32 [4, 96, 96, 48], P(None, 'gx', 'gy', 'gz'), may hold values from -6 to 6
- coefficient: float32 [96, 96, 48], P('gx', 'gy', 'gz'), may hold values from 0.1 to 2
- ordering: int32 [4, 4, 2, 216], P('gx', 'gy', 'gz'), may hold values from 0 to 215, as said below
- leaf_inverse: float32 [4, 4, 2, 125, 125], P('gx', 'gy', 'gz'), may hold values from -2 to 3
- leaf_first: float32 [4, 4, 2, 125, 50], P('gx', 'gy', 'gz'), may hold values from -0.5 to 0.5
- leaf_second: float32 [4, 4, 2, 125, 60], P('gx', 'gy', 'gz'), may hold values from -0.5 to 0.5
- leaf_top: float32 [4, 4, 2, 125, 72], P('gx', 'gy', 'gz'), may hold values from -0.5 to 0.5
- first_inverse: float32 [4, 4, 50, 50], P('gx', 'gy', 'gz'), may hold values from -2 to 3
- first_second: float32 [4, 4, 2, 25, 60], P('gx', 'gy', 'gz'), may hold values from -1.25 to 1.25
- first_top: float32 [4, 4, 2, 25, 72], P('gx', 'gy', 'gz'), may hold values from -1.25 to 1.25
- second_inverse: float32 [4, 240, 240], P('gx', ('gy', 'gz')), may hold values from -2 to 3
- second_top: float32 [4, 4, 2, 30, 72], P('gx', 'gy', 'gz'), may hold values from -1 to 1
- top_inverse: float32 [1152, 1152], P(('gx', 'gy', 'gz')), may hold values from -2 to 3
Outputs:
- correction: float32 [4, 96, 96, 48], P(None, 'gx', 'gy', 'gz')
The draws below stay inside these ranges and needn't reach their ends.
Inputs may be any that keep to these rules, and one draw needn't show every extreme that they name: `ordering`: each device's row names each of its 216 coarse cells once (cell x 6^2 + y * 6 + z): first the 125 cells with x, y and z all below 5, then the 25 cells with z = 5 and x, y below it, then the 30 cells with y = 5 and x below it, then the 36 cells with x = 5, each group in any order.
All inputs are finite; a program needn't handle non-finite values.
Results may differ from the reference program's by a relative error of at most 0.0003.
Values sent between devices are 32-bit elements; how exact they have to be, the bound alone decides.
A program may use at most 64 MiB of HBM per device.

```python
import math
import jax
import jax.numpy as jnp
from jax import lax

NRHS = 4
SIDE = 6
COARSE_DEV = 216
FIRST_DEV = 25
SECOND_DEV = 30
TOP_DEV = 36
LEAF = 125
FIRST_SEP = 50
SECOND_SEP = 240
TOP_SEP = 1152
NX = 96
NY = 96
NZ = 48
N_GX = 4
N_GY = 4
N_GZ = 2


def inverse_block(key, leading, extent):
    full_shape = tuple(leading) + (extent, extent)
    jitter = jnp.clip(jax.random.normal(key, full_shape, jnp.float32), -4.0, 4.0) * 0.5
    return jnp.eye(extent, dtype=jnp.float32) + jitter / extent ** 0.5


def draw_leaf_inverse(key, part):
    return inverse_block(jax.random.fold_in(key, 11), (N_GX, N_GY, N_GZ), LEAF)


def draw_first_inverse(key, part):
    return inverse_block(jax.random.fold_in(key, 23), (N_GX, N_GY), FIRST_SEP)


def draw_second_inverse(key, part):
    return inverse_block(jax.random.fold_in(key, 37), (N_GX,), SECOND_SEP)


def draw_top_inverse(key, part):
    return inverse_block(jax.random.fold_in(key, 41), (), TOP_SEP)


def draw_ordering(key, part):
    cells = jnp.arange(COARSE_DEV, dtype=jnp.int32)
    first_coord = cells // (SIDE * SIDE)
    second_coord = cells // SIDE % SIDE
    third_coord = cells % SIDE
    edge = SIDE - 1
    classes = jnp.where(first_coord == edge, 3, jnp.where(second_coord == edge, 2, jnp.where(third_coord == edge, 1, 0))).astype(jnp.int32)
    subkeys = jax.random.split(jax.random.fold_in(key, 53), N_GX * N_GY * N_GZ)

    def one_row(subkey):
        shuffled = jax.random.permutation(subkey, COARSE_DEV).astype(jnp.int32)
        rank = jnp.argsort(classes[shuffled], stable=True)
        return shuffled[rank].astype(jnp.int32)
    return jax.vmap(one_row)(subkeys).reshape(N_GX, N_GY, N_GZ, COARSE_DEV)


def levels(own_key, dims, shards, low, top_value):
    factor_of = 1.0
    for axis_at, blocks in shards:
        draws = jax.random.uniform(jax.random.fold_in(jax.random.fold_in(own_key, 6), axis_at), (blocks,), jnp.float32, low / len(shards), top_value / len(shards))
        factor_of = factor_of * jnp.repeat(jnp.exp(draws), dims[axis_at] // blocks).reshape((-1,) + (1,) * (len(dims) - 1 - axis_at))
    return factor_of


def normal_values(stream_key, dims, scale, most, cuts=(), kind=jnp.bfloat16):
    gain = levels(stream_key, dims, cuts, -0.22, 0.18) if cuts else 1.0
    drawn = jax.random.normal(stream_key, dims, jnp.float32) * scale * gain
    return jnp.minimum(jnp.maximum(drawn, -most), most).astype(kind)


def setup_inputs(seed: int = 0) -> dict:
    keys = jax.random.split(jax.random.key(seed), 15)
    return {
        "right_side": normal_values(keys[0], (NRHS, NX, NY, NZ), 1.0, 6.0, ((1, 4), (2, 4), (3, 2)), jnp.float32),
        "iterate": normal_values(keys[1], (NRHS, NX, NY, NZ), 1.0, 6.0, ((1, 4), (2, 4), (3, 2)), jnp.float32),
        "coefficient": jnp.clip(jnp.exp(math.log(2.0) - 2.9957323 * jax.random.uniform(keys[2], (NX, NY, NZ), jnp.float32) ** levels(keys[2], (NX, NY, NZ), ((0, 4), (1, 4), (2, 2)), -0.2, 0.2)), 0.1, 2.0),
        "ordering": draw_ordering(jax.random.fold_in(keys[14], 71), 0),
        "leaf_inverse": draw_leaf_inverse(jax.random.fold_in(keys[14], 71), 0),
        "leaf_first": normal_values(keys[5], (N_GX, N_GY, N_GZ, LEAF, 2 * FIRST_DEV), LEAF ** -0.5, 0.5, ((0, 4), (1, 4), (2, 2)), jnp.float32),
        "leaf_second": normal_values(keys[6], (N_GX, N_GY, N_GZ, LEAF, 2 * SECOND_DEV), LEAF ** -0.5, 0.5, ((0, 4), (1, 4), (2, 2)), jnp.float32),
        "leaf_top": normal_values(keys[7], (N_GX, N_GY, N_GZ, LEAF, 2 * TOP_DEV), LEAF ** -0.5, 0.5, ((0, 4), (1, 4), (2, 2)), jnp.float32),
        "first_inverse": draw_first_inverse(jax.random.fold_in(keys[14], 71), 0),
        "first_second": normal_values(keys[9], (N_GX, N_GY, N_GZ, FIRST_DEV, 2 * SECOND_DEV), FIRST_DEV ** -0.5, 1.25, ((0, 4), (1, 4), (2, 2)), jnp.float32),
        "first_top": normal_values(keys[10], (N_GX, N_GY, N_GZ, FIRST_DEV, 2 * TOP_DEV), FIRST_DEV ** -0.5, 1.25, ((0, 4), (1, 4), (2, 2)), jnp.float32),
        "second_inverse": draw_second_inverse(jax.random.fold_in(keys[14], 71), 0),
        "second_top": normal_values(keys[12], (N_GX, N_GY, N_GZ, SECOND_DEV, 2 * TOP_DEV), SECOND_DEV ** -0.5, 1.0, ((0, 4), (1, 4), (2, 2)), jnp.float32),
        "top_inverse": draw_top_inverse(jax.random.fold_in(keys[14], 71), 0),
    }


precise = lax.Precision.HIGHEST


def contract(pattern, operand, matrix):
    return jnp.einsum(pattern, operand, matrix, precision=precise, preferred_element_type=jnp.float32)


def weigh(extended, dimension):
    length = extended.shape[dimension] - 1
    previous = lax.slice_in_dim(extended, 0, length, 2, dimension)
    centre = lax.slice_in_dim(extended, 1, length + 1, 2, dimension)
    following = lax.slice_in_dim(extended, 2, length + 1, 2, dimension)
    return 0.25 * previous + 0.5 * centre + 0.25 * following


def spread(extended, dimension):
    length = extended.shape[dimension] - 1
    current = lax.slice_in_dim(extended, 0, length, 1, dimension)
    following = lax.slice_in_dim(extended, 1, length + 1, 1, dimension)
    paired = jnp.stack([current, 0.5 * (current + following)], axis=dimension + 1)
    new_shape = list(current.shape)
    new_shape[dimension] = 2 * length
    return paired.reshape(new_shape)


def restrict(values):
    extended = jnp.pad(values, ((0, 0), (1, 0), (1, 0), (1, 0)))
    for dimension in (1, 2, 3):
        extended = weigh(extended, dimension)
    return extended


def prolong(values):
    extended = jnp.pad(values, ((0, 0), (0, 1), (0, 1), (0, 1)))
    for dimension in (1, 2, 3):
        extended = spread(extended, dimension)
    return extended


def residual_of(right_side, iterate, coefficient):
    padded = jnp.pad(iterate, ((0, 0), (1, 1), (1, 1), (1, 1)))
    beside = padded[:, 2:, 1:-1, 1:-1] + padded[:, :-2, 1:-1, 1:-1]
    beside = beside + padded[:, 1:-1, 2:, 1:-1] + padded[:, 1:-1, :-2, 1:-1]
    beside = beside + padded[:, 1:-1, 1:-1, 2:] + padded[:, 1:-1, 1:-1, :-2]
    return right_side - ((6.0 + coefficient) * iterate - beside)


def from_above(values, axis):
    length = values.shape[axis]
    kept = lax.slice_in_dim(values, 1, length, 1, axis)
    widths = [(0, 0)] * values.ndim
    widths[axis] = (0, 1)
    return jnp.pad(kept, widths)


def from_below(values, axis):
    length = values.shape[axis]
    kept = lax.slice_in_dim(values, 0, length - 1, 1, axis)
    widths = [(0, 0)] * values.ndim
    widths[axis] = (1, 0)
    return jnp.pad(kept, widths)


def reference(right_side, iterate, coefficient, ordering, leaf_inverse, leaf_first, leaf_second, leaf_top, first_inverse, first_second, first_top, second_inverse, second_top, top_inverse):
    coarse = restrict(restrict(residual_of(right_side, iterate, coefficient)))
    blocks = coarse.reshape(NRHS, N_GX, SIDE, N_GY, SIDE, N_GZ, SIDE)
    blocks = blocks.transpose(0, 1, 3, 5, 2, 4, 6).reshape(NRHS, N_GX, N_GY, N_GZ, COARSE_DEV)
    chosen = jnp.take_along_axis(blocks, jnp.broadcast_to(ordering[None], blocks.shape), axis=4)
    first_end = LEAF + FIRST_DEV
    second_end = first_end + SECOND_DEV
    leaf_rhs = chosen[..., :LEAF]
    first_rhs = chosen[..., LEAF:first_end]
    second_rhs = chosen[..., first_end:second_end]
    top_rhs = chosen[..., second_end:]

    leaf_solved = contract('rabcl,abclk->rabck', leaf_rhs, leaf_inverse)
    toward = contract('rabcl,abclk->rabck', leaf_solved, leaf_first)
    first_target = first_rhs - toward[..., :FIRST_DEV] - from_above(toward[..., FIRST_DEV:], 3)
    first_target = first_target.reshape(NRHS, N_GX, N_GY, FIRST_SEP)
    first_solved = contract('rabi,abik->rabk', first_target, first_inverse).reshape(NRHS, N_GX, N_GY, N_GZ, FIRST_DEV)

    toward = contract('rabcl,abclk->rabck', leaf_solved, leaf_second) + contract('rabcl,abclk->rabck', first_solved, first_second)
    second_target = second_rhs - toward[..., :SECOND_DEV] - from_above(toward[..., SECOND_DEV:], 2)
    second_target = second_target.reshape(NRHS, N_GX, SECOND_SEP)
    second_solved = contract('rai,aik->rak', second_target, second_inverse).reshape(NRHS, N_GX, N_GY, N_GZ, SECOND_DEV)

    toward = contract('rabcl,abclk->rabck', leaf_solved, leaf_top) + contract('rabcl,abclk->rabck', first_solved, first_top)
    toward = toward + contract('rabcl,abclk->rabck', second_solved, second_top)
    top_target = top_rhs - toward[..., :TOP_DEV] - from_above(toward[..., TOP_DEV:], 1)
    top_target = top_target.reshape(NRHS, TOP_SEP)
    top_solved = contract('ri,ik->rk', top_target, top_inverse)

    top_back = contract('rk,ik->ri', top_solved, top_inverse).reshape(NRHS, N_GX, N_GY, N_GZ, TOP_DEV)
    top_pair = jnp.concatenate([top_back, from_below(top_back, 1)], axis=4)
    second_gap = second_solved - contract('rabck,abcik->rabci', top_pair, second_top)
    second_gap = second_gap.reshape(NRHS, N_GX, SECOND_SEP)
    second_back = contract('rak,aik->rai', second_gap, second_inverse).reshape(NRHS, N_GX, N_GY, N_GZ, SECOND_DEV)
    second_pair = jnp.concatenate([second_back, from_below(second_back, 2)], axis=4)
    first_gap = first_solved - contract('rabck,abcik->rabci', second_pair, first_second)
    first_gap = first_gap - contract('rabck,abcik->rabci', top_pair, first_top)
    first_gap = first_gap.reshape(NRHS, N_GX, N_GY, FIRST_SEP)
    first_back = contract('rabk,abik->rabi', first_gap, first_inverse).reshape(NRHS, N_GX, N_GY, N_GZ, FIRST_DEV)
    first_pair = jnp.concatenate([first_back, from_below(first_back, 3)], axis=4)
    leaf_gap = leaf_solved - contract('rabck,abcik->rabci', first_pair, leaf_first)
    leaf_gap = leaf_gap - contract('rabck,abcik->rabci', second_pair, leaf_second)
    leaf_gap = leaf_gap - contract('rabck,abcik->rabci', top_pair, leaf_top)
    leaf_back = contract('rabck,abclk->rabcl', leaf_gap, leaf_inverse)

    ordered = jnp.concatenate([leaf_back, first_back, second_back, top_back], axis=4)
    inverse_order = jnp.argsort(ordering, axis=-1).astype(jnp.int32)
    listed = jnp.take_along_axis(ordered, jnp.broadcast_to(inverse_order[None], ordered.shape), axis=4)
    listed = listed.reshape(NRHS, N_GX, N_GY, N_GZ, SIDE, SIDE, SIDE)
    coarse_grid = listed.transpose(0, 1, 4, 2, 5, 3, 6).reshape(NRHS, N_GX * SIDE, N_GY * SIDE, N_GZ * SIDE)
    return prolong(prolong(coarse_grid))
```

```python
import functools
import itertools

import jax
import jax.numpy as jnp
import numpy as np
from jax import lax
from jax.experimental import pallas as pl
from jax.experimental.pallas import tpu as pltpu
from jax.sharding import PartitionSpec as P

AXES = ("gx", "gy", "gz")
LANES = 128
TILE = 8
PITCH = 32
UNROLL = 64
SIDES = (0, 1, -1)
MESH = pl.DeviceIdType.MESH
f32 = jnp.float32
bf16 = jnp.bfloat16

SHARES = [
    (i, j, k)
    for i in SIDES
    for j in SIDES
    for k in SIDES
    if (i, j, k) != (0, 0, 0) and (i, j, k).count(-1) <= 1
]
RIMS = [(i, j, k) for i in (0, 1) for j in (0, 1) for k in (0, 1) if (i, j, k) != (0, 0, 0)]


def up_to(n, unit):
    return -(-n // unit) * unit


def weight(k):
    return max(0, 4 - abs(k)) / 16.0


def weight_beside(k):
    return weight(k - 1) + weight(k + 1)


def single(a, b):
    return jnp.dot(a, b, preferred_element_type=f32)


def single_back(a, b):
    return lax.dot_general(a, b, (((1,), (1,)), ((), ())), preferred_element_type=f32)


def halves(x):
    high = x.astype(bf16)
    return high, (x - high.astype(f32)).astype(bf16)


def stacked(x):
    high = x.astype(bf16).astype(f32)
    return jnp.concatenate([high, x - high], axis=0).astype(bf16)


def dot_exact(a, b, product=single):
    count = a.shape[0]
    both = product(stacked(a), b)
    return both[:count] + both[count:]


def dot(a, b, product=single):
    count = a.shape[0]
    both = product(stacked(a), b[0][...])
    return both[:count] + both[count:] + product(a.astype(bf16), b[1][...])


def dot_back(a, b):
    return dot(a, b, single_back)


def coarse_at(side, row, count):
    if side == 0:
        return row if row < count else None
    if side == 1:
        return count if row == 0 else None
    return -1 if row == count - 1 else None


def restriction(fine, pad, stencil):
    count = fine // 4
    out = np.zeros((3, pad, fine), np.float32)
    for s, side in enumerate(SIDES):
        for row in range(pad):
            at = coarse_at(side, row, count)
            if at is not None:
                for y in range(fine):
                    out[s, row, y] = stencil(y - 4 * at)
    return out


def at_first(table):
    table = table.copy()
    table[0, 0, 0] -= weight(-1)
    return table


def interpolation(fine, pad):
    count = fine // 4
    out = np.zeros((2, fine, pad), np.float32)
    for y in range(fine):
        for at in (y // 4, y // 4 + 1):
            value = 1.0 - abs(y - 4 * at) / 4.0
            if at < count:
                out[0, y, at] = value
            else:
                out[1, y, 0] = value
    return out


def constants(rhs, ny, nz, side, pad_y, pad_z):
    slabs = side + 2
    edge_rows = up_to(slabs, TILE)
    last = ny // 4 - 1
    eye = np.eye(slabs, dtype=np.float32)
    eye_edge = np.eye(edge_rows, slabs, dtype=np.float32)

    def over_rows(table):
        return np.concatenate([
            np.kron(eye, table[0]),
            np.kron(eye_edge, table[1][0:1]),
            np.kron(eye_edge, table[2][last:last + 1]),
        ], 0)

    plain = over_rows(restriction(ny, pad_y, weight))
    beside = restriction(ny, pad_y, weight_beside)
    rows = np.stack([
        np.concatenate([plain, over_rows(b)], 1) for b in (at_first(beside), beside)
    ])

    def over_lanes(table):
        out = np.zeros((3, rhs * nz, LANES), np.float32)
        for s in range(3):
            for r in range(rhs):
                out[s, r * nz:(r + 1) * nz, r * pad_z:(r + 1) * pad_z] = table[s].T
        return np.concatenate(list(out), 1)

    lanes = over_lanes(restriction(nz, pad_z, weight))
    table = restriction(nz, pad_z, weight_beside)
    lanes_beside = np.stack([over_lanes(at_first(table)), over_lanes(table)])
    grow = interpolation(nz, pad_z)
    wide = np.zeros((2, LANES, rhs * nz), np.float32)
    for s in range(2):
        for r in range(rhs):
            wide[s, r * pad_z:(r + 1) * pad_z, r * nz:(r + 1) * nz] = grow[s].T
    wide = wide.reshape(2 * LANES, rhs * nz)
    tall_of = interpolation(ny, pad_y)
    slab_rows = side * pad_y
    face_rows = up_to(side, TILE)
    tall = np.zeros(((side + 1) * ny, slab_rows + pad_y + 2 * face_rows), np.float32)
    for at in range(side + 1):
        here = slice(at * ny, (at + 1) * ny)
        tall[here, at * pad_y:(at + 1) * pad_y] = tall_of[0]
        beyond = slab_rows + pad_y + (at if at < side else face_rows)
        tall[here, beyond] = tall_of[1][:, 0]
    return rows, lanes, lanes_beside, wide, tall


def kernel(
    sizes,
    right_ref, u_ref, coef_ref, order_ref, leaf_ref, first_ref, second_ref, top_ref,
    fs_ref, ft_ref, st_ref, rows_first, rows_second, rows_top,
    mat_rows, mat_lanes, mat_beside, mat_wide, mat_tall,
    out_ref,
    right_in, u_in, coef_in, order_in, leaf_in, first_in, second_in, top_in,
    fs_in, ft_in, st_in, rows_in, m_rows, m_lanes, m_beside, m_wide, m_tall,
    leaf_split, link_split, fs_seat, ftst_seat, row_seat, rows0, rows1, big, w0, zed, kay,
    packed, shares, share_in, prev, scatter_out, scatter_in, gather_in, top_all, val,
    picked, slots, order_seat, ordered, rim, face, stage, k_own, k_all,
    in_sem, share_send, share_recv, prev_send, prev_recv, k_sem, s_send, s_recv, g_send, g_recv,
    r_send, r_recv,
):
    rhs, nx, ny, nz = u_in.shape
    side = nx // 4
    side_y, side_z = ny // 4, nz // 4
    slabs = side + 2
    pad_y, pad_z = sizes["pad_y"], sizes["pad_z"]
    spans, seats, widths = sizes["spans"], sizes["seats"], sizes["widths"]
    leaf = leaf_in.shape[0]
    at_first_level, at_second, at_top = sizes["starts"]
    peers = sizes["peers"]
    me = {a: lax.axis_index(a) for a in AXES}
    groups = (("gz",), ("gy", "gz"), AXES)
    shift_axis = ("gz", "gy", "gx")
    counts = [int(np.prod([peers[a] for a in g])) for g in groups]
    n_gz = peers["gz"]

    def place(group):
        at = 0
        for a in group:
            at = at * peers[a] + me[a]
        return at

    def coords(group, at):
        found = {}
        for a in reversed(group):
            found[a] = at % peers[a]
            at = at // peers[a]
        return {a: found[a] if a in found else me[a] for a in AXES}

    turned = {a: [me[a]] for a in AXES}
    for a in AXES:
        for k in range(1, peers[a]):
            at = me[a] + k
            turned[a].append(jnp.where(at >= peers[a], at - peers[a], at))

    def for_others(group, send):
        count = int(np.prod([peers[a] for a in group]))
        if count <= UNROLL:
            for steps in itertools.product(*[range(peers[a]) for a in group]):
                if any(steps):
                    target = dict(me)
                    at = 0
                    for a, k in zip(group, steps):
                        target[a] = turned[a][k]
                        at = at * peers[a] + turned[a][k]
                    send(target, at)
        else:
            mine = place(group)

            def step(k, carry):
                at = (mine + k) % count
                send(coords(group, at), at)
                return carry

            lax.fori_loop(1, count, step, 0)

    barrier = pltpu.get_barrier_semaphore()
    everyone = counts[2]

    def greet(target, at):
        pl.semaphore_signal(barrier, inc=1, device_id=target, device_id_type=MESH)

    at_y, at_z = jnp.minimum(me["gy"], 1), jnp.minimum(me["gz"], 1)
    loads = {}

    def load(name, source, into):
        loads[name] = pltpu.make_async_copy(source, into, in_sem.at[len(loads)])
        loads[name].start()

    load("coef", coef_ref, coef_in)
    for r in range(rhs):
        load(("u", r), u_ref.at[r], u_in.at[r])
        load(("right", r), right_ref.at[r], right_in.at[r])
    load("m_rows", mat_rows.at[at_y], m_rows)
    load("m_lanes", mat_lanes, m_lanes)
    load("m_beside", mat_beside.at[at_z], m_beside)
    row_sources = (rows_first, rows_second, rows_top)
    for level in range(3):
        load(("rows", level), row_sources[level], rows_in[level])
    load("leaf", leaf_ref, leaf_in)
    load("first", first_ref, first_in)
    load("second", second_ref, second_in)
    load("top", top_ref, top_in)
    load("order", order_ref, order_in)
    load("fs", fs_ref, fs_in)
    load("ft", ft_ref, ft_in)
    load("st", st_ref, st_in)
    load("m_wide", mat_wide, m_wide)
    load("m_tall", mat_tall, m_tall)

    def clear(ref):
        ref[...] = jnp.zeros(ref.shape, ref.dtype)

    for buffer in share_in:
        clear(buffer)
    clear(rim)
    for_others(AXES, greet)

    for level in range(3):
        @pl.when(me[shift_axis[level]] == 0)
        def _():
            clear(prev[level])
    clear(k_own)
    for level in range(2):
        clear(scatter_out[level])

    half = slabs * ny
    loads["coef"].wait()
    for r in range(rhs):
        loads["u", r].wait()
        loads["right", r].wait()
        acc_p = {}
        acc_u = {}

        def add(acc, at, factor, value):
            term = factor * value
            acc[at] = acc[at] + term if at in acc else term

        for x in range(nx):
            u = u_in[r, x]
            q = right_in[r, x] - (6.0 + coef_in[x]) * u
            for at in range(-1, side + 1):
                k = x - 4 * at
                if weight(k):
                    add(acc_p, at, weight(k), q)
                    add(acc_u, at, weight(k), u)
                if at == 0 and x == 0:
                    below = jnp.where(me["gx"] > 0, weight(-1), 0.0)
                    add(acc_p, at, weight(1) + below, u)
                elif weight_beside(k):
                    add(acc_p, at, weight_beside(k), u)
        for at in range(-1, side + 1):
            rows = slice((at + 1) * ny, (at + 2) * ny)
            packed[rows, r * nz:(r + 1) * nz] = acc_p[at]
            rows = slice(half + (at + 1) * ny, half + (at + 2) * ny)
            packed[rows, r * nz:(r + 1) * nz] = acc_u.get(at, jnp.zeros((ny, nz), f32))
    loads["m_rows"].wait()
    loads["m_lanes"].wait()
    loads["m_beside"].wait()
    high, low = halves(packed[...])
    a = single(m_rows[...], high) + single(m_rows[...], low)
    b = single(m_rows[:, :half], high[half:]) + single(m_rows[:, :half], low[half:])
    c = dot_exact(a, m_lanes[...]) + dot_exact(b, m_beside[...])
    for t in range(3):
        shares[t] = c[:, t * LANES:(t + 1) * LANES]

    def valid(step, sign):
        ok = None
        for a, d in zip(AXES, step):
            if d:
                at = me[a] + sign * d
                this = (at >= 0) & (at < peers[a])
                ok = this if ok is None else ok & this
        return ok

    def toward(step, sign):
        return {a: (me[a] + sign * d + peers[a]) % peers[a] for a, d in zip(AXES, step)}

    for level in range(3):
        loads["rows", level].wait()
    pl.semaphore_wait(barrier, everyone - 1)

    edge_rows = up_to(slabs, TILE)
    main = side * pad_y
    share_copies = []
    for n, step in enumerate(SHARES):
        dx, dy, dz = step
        if dy == 0:
            cut = {0: pl.ds(pad_y, main), 1: pl.ds((side + 1) * pad_y, pad_y), -1: pl.ds(0, pad_y)}[dx]
        else:
            cut = pl.ds(slabs * pad_y + (edge_rows if dy < 0 else 0), edge_rows)
        copy = pltpu.make_async_remote_copy(
            src_ref=shares.at[SIDES.index(dz), cut], dst_ref=share_in[n],
            send_sem=share_send.at[n], recv_sem=share_recv.at[n],
            device_id=toward(step, 1), device_id_type=MESH,
        )
        share_copies.append(copy)

        @pl.when(valid(step, 1))
        def _():
            copy.start()

    prev_copies = []
    for level in range(3):
        axis = shift_axis[level]
        target = dict(me)
        target[axis] = (me[axis] + 1) % peers[axis]
        copy = pltpu.make_async_remote_copy(
            src_ref=rows_in[level], dst_ref=prev[level],
            send_sem=prev_send.at[level], recv_sem=prev_recv.at[level],
            device_id=target, device_id_type=MESH,
        )
        prev_copies.append(copy)

        @pl.when(me[axis] < peers[axis] - 1)
        def _():
            copy.start()

    def keep(where, value, rows=None):
        high, low = halves(value)
        if rows is None:
            where[0][...], where[1][...] = high, low
        else:
            where[0][rows, :] = high
            where[1][rows, :] = low

    def rows_of(raw):
        return raw[:, 0, :] if len(raw.shape) == 3 else raw[...]

    for name in ("leaf", "first", "second", "top", "fs", "ft", "st", "order"):
        loads[name].wait()
    keep(leaf_split, rows_of(leaf_in))
    link_at = [0, 2 * seats[0], 2 * (seats[0] + seats[1])]
    for pair in (link_split, rows0, rows1, big, w0):
        for part in pair:
            clear(part)
    for level, raw in enumerate((first_in, second_in, top_in)):
        value = rows_of(raw)
        span = spans[level]
        for s in range(2):
            at = link_at[level] + s * seats[level]
            keep(link_split, value[s * span:(s + 1) * span], slice(at, at + span))

    clear(fs_seat)
    clear(ftst_seat)
    for s in range(2):
        span, seat = spans[1], seats[1]
        fs_seat[:spans[0], s * seat:s * seat + span] = rows_of(fs_in)[:, s * span:(s + 1) * span]
        span, seat = spans[2], seats[2]
        ftst_seat[:spans[1], s * seat:s * seat + span] = rows_of(st_in)[:, s * span:(s + 1) * span]
        ftst_seat[PITCH:PITCH + spans[0], s * seat:s * seat + span] = (
            rows_of(ft_in)[:, s * span:(s + 1) * span]
        )

    clear(order_seat)
    starts = (0, leaf, leaf + spans[0], leaf + spans[0] + spans[1], order_in.shape[1])
    seated = (0, at_first_level, at_second, at_top)
    order_seat[...] = jnp.full(order_seat.shape, -1e6, f32)
    for begin, end, at in zip(starts, starts[1:], seated):
        order_seat[:, at:at + end - begin] = order_in[:, begin:end].astype(f32)
    order = order_seat[...]
    first = jnp.floor((order + 0.5) / (side_y * side_z))
    rest = order - first * (side_y * side_z)
    second = jnp.floor((rest + 0.5) / side_z)
    third = rest - second * side_z
    cells = order.shape[1]

    def row_iota(count):
        return lax.broadcasted_iota(jnp.int32, (count, cells), 0).astype(f32)

    main_hot = (row_iota(main) == first * pad_y + second).astype(f32)
    edge_id = row_iota(edge_rows)
    near = (edge_id == first + 1) | ((edge_id == slabs - 1) & (first == 0)) | (
        (edge_id == 0) & (first == side - 1)
    )
    pick_hot = jnp.concatenate([
        main_hot,
        (near & (second == 0)).astype(f32),
        (near & (second == side_y - 1)).astype(f32),
    ], 0)
    face_rows = face.shape[0]
    face_hot = ((row_iota(face_rows) == first) & (second == 0)).astype(f32)
    back_hot = jnp.concatenate([main_hot, face_hot], 0)
    lane_id = lax.broadcasted_iota(jnp.int32, (LANES, cells), 0).astype(f32)

    def lane_hot(r):
        return (lane_id == third + r * pad_z).astype(f32).astype(bf16)

    def wait_prev(level):
        @pl.when(me[shift_axis[level]] > 0)
        def _():
            prev_copies[level].wait_recv()

    def seat_lanes(value, level):
        span = spans[level]
        row_seat[level][...] = jnp.zeros(row_seat[level].shape, f32)
        for d in range(counts[level]):
            row_seat[level][:, d * PITCH:d * PITCH + span] = value[:, d * span:(d + 1) * span]
        return row_seat[level][...]

    links = dot_back(rows_of(leaf_in), link_split)
    wait_prev(0)
    own0 = seat_lanes(rows_of(rows_in[0]), 0)
    keep(rows0, own0, slice(0, spans[0]))
    keep(w0, own0, slice(at_first_level, at_first_level + spans[0]))
    keep(rows0, seat_lanes(rows_of(prev[0]), 0), slice(seats[0], seats[0] + spans[0]))
    e0 = dot(links[:, :2 * seats[0]], rows0)
    keep(w0, -e0, slice(0, leaf))
    wait_prev(1)
    own1 = seat_lanes(rows_of(rows_in[1]), 1)
    keep(rows1, own1, slice(0, spans[1]))
    keep(rows1, seat_lanes(rows_of(prev[1]), 1), slice(seats[1], seats[1] + spans[1]))
    k_own[...] = dot(fs_seat[...], rows1)
    mine0 = place(groups[0])

    def send_k(target, at):
        pltpu.make_async_remote_copy(
            src_ref=k_own, dst_ref=k_all.at[mine0],
            send_sem=k_sem.at[0], recv_sem=k_sem.at[1],
            device_id=target, device_id_type=MESH,
        ).start()

    for_others(groups[0], send_k)
    k_all[mine0] = k_own[...]

    def all_slots(buffer, sem, count):
        return pltpu.make_async_copy(
            buffer.at[pl.ds(0, count - 1)], buffer.at[pl.ds(0, count - 1)], sem
        )

    e1 = dot(links[:, 2 * seats[0]:2 * (seats[0] + seats[1])], rows1)
    w1_value = jnp.concatenate([
        -e1, jnp.zeros((at_second - leaf, e1.shape[1]), f32), own1,
        jnp.zeros((at_top - at_second - spans[1], e1.shape[1]), f32),
    ], 0)
    all_slots(k_all, k_sem.at[1], n_gz).wait()
    keep(kay, k_all[...].reshape(n_gz * PITCH, k_own.shape[1]))
    w0_value = w0[0][...].astype(f32) + w0[1][...].astype(f32)
    gap_width = widths[1]
    zed_value = w1_value - dot(w0_value, kay)
    high, low = halves(zed_value)
    zed[0][:, :gap_width], zed[1][:, :gap_width] = high, low
    zed[0][:, gap_width:], zed[1][:, gap_width:] = w0[0][...], w0[1][...]

    received = {}
    for n, step in enumerate(SHARES):
        @pl.when(valid(step, -1))
        def _():
            share_copies[n].wait_recv()
    for n, step in enumerate(SHARES):
        dx, dy, dz = step
        received[dx, dy] = received[dx, dy] + share_in[n][...] if (dx, dy) in received else share_in[n][...]

    total = shares[0, pad_y:pad_y + main] + received[0, 0]
    pieces = [total[:pad_y] + received[1, 0], total[pad_y:main - pad_y], total[main - pad_y:] + received[-1, 0]]
    edge_lane = lax.broadcasted_iota(jnp.int32, (edge_rows, LANES), 0)
    inside = (edge_lane >= 1) & (edge_lane <= side)
    for dy in (1, -1):
        tile = jnp.where(inside, received[0, dy], 0.0)
        tile = tile + jnp.where(edge_lane == slabs - 1, received[1, dy], 0.0)
        if (-1, dy) in received:
            tile = tile + jnp.where(edge_lane == 0, received[-1, dy], 0.0)
        pieces.append(tile)
    coarse = jnp.concatenate(pieces, 0)
    for r in range(rhs):
        spread = dot_exact(coarse, lane_hot(r))
        picked[r:r + 1, :] = jnp.sum(spread * pick_hot, axis=0, keepdims=True)

    def scatter(level, terms, pitch, lane):
        span, group = spans[level], groups[level]
        out, into = scatter_out[level], scatter_in[level]
        for d in range(counts[level]):
            out[d, :, lane:lane + span] = terms[:, d * pitch:d * pitch + span]
        mine = place(group)

        def send(target, d):
            pltpu.make_async_remote_copy(
                src_ref=out.at[d], dst_ref=into.at[mine],
                send_sem=s_send.at[level], recv_sem=s_recv.at[level],
                device_id=target, device_id_type=MESH,
            ).start()

        for_others(group, send)
        into[mine] = out[mine]

    def scatter_end(level):
        into = scatter_in[level]
        all_slots(into, s_recv.at[level], counts[level]).wait()
        return jnp.sum(into[...], axis=0)

    def gather(level, value):
        group = groups[level]
        into, own = gather_in[level], stage[level]
        mine = place(group)
        own[...] = value

        def send(target, d):
            pltpu.make_async_remote_copy(
                src_ref=own, dst_ref=into.at[mine],
                send_sem=g_send.at[level], recv_sem=g_recv.at[level],
                device_id=target, device_id_type=MESH,
            ).start()

        for_others(group, send)
        into[mine] = own[...]

    def gather_end(level):
        into = gather_in[level]
        all_slots(into, g_recv.at[level], counts[level]).wait()
        return into

    below_top = picked[:, :at_top]
    scatter(1, dot(below_top, (zed[0][:, :gap_width], zed[1][:, :gap_width])), PITCH, 0)
    scatter(0, dot(below_top, w0), PITCH, PITCH)

    wait_prev(2)
    keep(big, rows_of(rows_in[2]), slice(0, spans[2]))
    keep(big, rows_of(prev[2]), slice(seats[2], seats[2] + spans[2]))
    pair2 = 2 * seats[2]
    rows2 = (big[0].at[pl.ds(0, pair2)], big[1].at[pl.ds(0, pair2)])
    queue = slice(LANES, LANES + 2 * PITCH)
    keep(big, dot(ftst_seat[...], rows2), queue)
    leaf_rhs = picked[:, :leaf]
    tops = dot(leaf_rhs, halves(links[:, 2 * (seats[0] + seats[1]):]))
    slots[...] = -tops
    slots[:, :spans[2]] = picked[:, at_top:at_top + spans[2]] - tops[:, :spans[2]]
    base2 = dot(slots[...], rows2)
    first_own = scatter_end(0)
    queue_rows = (big[0].at[queue], big[1].at[queue])
    base2 = base2 - dot(first_own[:, :2 * PITCH], queue_rows)
    leaf_solved = dot(leaf_rhs, leaf_split)
    second_own = scatter_end(1)
    scatter(2, base2 - dot(second_own[:, :2 * PITCH], queue_rows), spans[2], 0)
    both_own = (first_own + second_own)[:, :2 * PITCH]
    top_own = scatter_end(2)
    gather(2, top_own)
    into = gather_end(2)
    for d in range(counts[2]):
        top_all[:, d * spans[2]:(d + 1) * spans[2]] = into[d, :, :spans[2]]
    solved = dot_back(top_all[...], big)
    gather(1, jnp.concatenate([
        both_own - solved[:, LANES:LANES + 2 * PITCH], jnp.zeros((rhs, LANES - 2 * PITCH), f32)
    ], 1))
    top_link = (link_split[0].at[pl.ds(link_at[2], pair2)], link_split[1].at[pl.ds(link_at[2], pair2)])
    base = dot_back(leaf_solved - dot(solved[:, :pair2], top_link), leaf_split)

    for level in range(3):
        @pl.when(me[shift_axis[level]] < peers[shift_axis[level]] - 1)
        def _():
            prev_copies[level].wait_send()

        all_slots(scatter_out[level], s_send.at[level], counts[level]).wait()
    all_slots(k_all, k_sem.at[0], n_gz).wait()
    all_slots(gather_in[2], g_send.at[2], counts[2]).wait()
    for n, step in enumerate(SHARES):
        @pl.when(valid(step, 1))
        def _():
            share_copies[n].wait_send()

    into = gather_end(1)
    clear(val)
    for d in range(counts[1]):
        val[:, d * PITCH:d * PITCH + spans[1]] = into[d, :, :spans[1]]
    for d in range(n_gz):
        at = gap_width + d * PITCH
        val[:, at:at + spans[0]] = into[me["gy"] * n_gz + d, :, PITCH:PITCH + spans[0]]
    back = dot_back(val[...], zed)
    clear(ordered)
    ordered[:, :at_top] = back
    ordered[:, :leaf] = back[:, :leaf] + base
    ordered[:, at_top:at_top + spans[2]] = solved[:, :spans[2]]

    cells_back = None
    for r in range(rhs):
        term = dot_exact(back_hot * ordered[r:r + 1, :], lane_hot(r), single_back)
        cells_back = term if cells_back is None else cells_back + term
    rim[0, 0:main] = cells_back[:main]
    face[...] = cells_back[main:]

    rim_copies = []
    for n, step in enumerate(RIMS):
        dx, dy, dz = step
        if dy:
            source, at = face, main + pad_y + (face_rows if dx else 0)
        elif dx:
            source, at = rim.at[0, pl.ds(0, pad_y)], main
        else:
            source, at = rim.at[0, pl.ds(0, main)], 0
        rows = face_rows if dy else (pad_y if dx else main)
        copy = pltpu.make_async_remote_copy(
            src_ref=source, dst_ref=rim.at[dz, pl.ds(at, rows)],
            send_sem=r_send.at[n], recv_sem=r_recv.at[n],
            device_id=toward(step, -1), device_id_type=MESH,
        )
        rim_copies.append(copy)

        @pl.when(valid(step, -1))
        def _():
            copy.start()

    loads["m_wide"].wait()
    loads["m_tall"].wait()
    all_slots(gather_in[1], g_send.at[1], counts[1]).wait()
    for n, step in enumerate(RIMS):
        @pl.when(valid(step, 1))
        def _():
            rim_copies[n].wait_recv()

    wide = dot_exact(jnp.concatenate([rim[0], rim[1]], 1), m_wide[...])
    high, low = halves(wide)
    out_ref[...] = single(m_tall[...], high) + single(m_tall[...], low)

    for n, step in enumerate(RIMS):
        @pl.when(valid(step, -1))
        def _():
            rim_copies[n].wait_send()


def spread_kernel(grown_ref, out_ref):
    rhs, nx, ny, nz = out_ref.shape
    side = nx // 4
    for r in range(rhs):
        slices = [
            grown_ref[at * ny:(at + 1) * ny, r * nz:(r + 1) * nz] for at in range(side + 1)
        ]
        for x in range(nx):
            at, k = x // 4, x % 4
            if k == 0:
                out_ref[r, x] = slices[at]
            else:
                out_ref[r, x] = (1 - k / 4) * slices[at] + (k / 4) * slices[at + 1]


def per_device(peers, right_side, iterate, coefficient, ordering, leaf_inverse, leaf_first,
               leaf_second, leaf_top, first_inverse, first_second, first_top, second_inverse,
               second_top, top_inverse):
    rhs, nx, ny, nz = iterate.shape
    side = nx // 4
    slabs = side + 2
    pad_y = up_to(ny // 4, TILE)
    pad_z = LANES // rhs // 4 if nz // 4 <= LANES // rhs // 4 else LANES // rhs
    mats = [jnp.asarray(m, bf16) for m in constants(rhs, ny, nz, side, pad_y, pad_z)]
    flip = lambda m: jnp.swapaxes(m, -1, -2)
    flat = lambda m: m.reshape(m.shape[-2:])
    single_rows = lambda m: m.reshape(m.shape[-2], 1, m.shape[-1])
    rows = [single_rows(first_inverse), single_rows(second_inverse), top_inverse]
    spans = [m.shape[0] for m in rows]
    counts = [m.shape[-1] // s for m, s in zip(rows, spans)]
    seats = [up_to(s, 16) for s in spans]
    seats[0] = seats[1] = PITCH
    widths = [counts[0] * PITCH, up_to(counts[1] * PITCH, LANES), rows[2].shape[-1]]
    leaf = leaf_inverse.shape[-1]
    cells = ordering.shape[-1]
    at_first_level = up_to(leaf, 16)
    at_second = at_first_level + PITCH
    at_top = at_second + PITCH
    slots = up_to(at_top + spans[2], LANES)
    vmem = lambda *shape: pltpu.VMEM(shape, f32)
    split = lambda *shape: [pltpu.VMEM(shape, bf16)] * 2
    like = lambda m: pltpu.VMEM(m.shape, m.dtype)
    dma = lambda n: pltpu.SemaphoreType.DMA((n,))
    sizes = {
        "peers": peers, "pad_y": pad_y, "pad_z": pad_z, "spans": spans, "seats": seats,
        "widths": widths, "starts": (at_first_level, at_second, at_top),
    }
    matrices = (
        ordering.reshape(1, cells), single_rows(leaf_inverse),
        single_rows(flip(leaf_first)), single_rows(flip(leaf_second)), flat(flip(leaf_top)),
        single_rows(first_second), single_rows(first_top), single_rows(second_top),
    )
    operands = (right_side, iterate, coefficient, *matrices, *rows, *mats)
    edge_rows = up_to(slabs, TILE)
    face_rows = up_to(side, TILE)
    main = side * pad_y

    def share_shape(step):
        dx, dy, _ = step
        return (edge_rows if dy else (pad_y if dx else main), LANES)

    in_vmem = pl.BlockSpec(memory_space=pltpu.VMEM)
    anywhere = pl.BlockSpec(memory_space=pl.ANY)
    links = 2 * sum(seats)
    big_rows = LANES + 2 * PITCH
    grown = pl.pallas_call(
        functools.partial(kernel, sizes),
        out_shape=jax.ShapeDtypeStruct(((side + 1) * ny, rhs * nz), f32),
        in_specs=jax.tree.map(lambda _: anywhere, operands),
        out_specs=in_vmem,
        scratch_shapes=[
            like(right_side), like(iterate), like(coefficient), *[like(m) for m in matrices],
            [like(m) for m in rows],
            pltpu.VMEM(mats[0].shape[1:], bf16), like(mats[1]),
            pltpu.VMEM(mats[2].shape[1:], bf16), like(mats[3]), like(mats[4]),
            split(leaf, leaf),
            split(links, leaf),
            vmem(PITCH, 2 * seats[1]),
            vmem(2 * PITCH, 2 * seats[2]),
            [vmem(spans[level], widths[level]) for level in range(2)],
            split(2 * seats[0], widths[0]),
            split(2 * seats[1], widths[1]),
            split(big_rows, widths[2]),
            split(at_top, widths[0]),
            split(at_top, widths[1] + widths[0]),
            split(counts[0] * PITCH, widths[1]),
            vmem(2 * slabs * ny, rhs * nz),
            vmem(3, slabs * pad_y + 2 * edge_rows, LANES),
            [vmem(*share_shape(step)) for step in SHARES],
            [like(m) for m in rows],
            [vmem(n, rhs, LANES) for n in counts],
            [vmem(n, rhs, LANES) for n in counts],
            [vmem(n, rhs, LANES) for n in counts],
            vmem(rhs, widths[2]),
            vmem(rhs, widths[1] + widths[0]),
            vmem(rhs, slots),
            vmem(rhs, 2 * seats[2]),
            vmem(1, slots),
            vmem(rhs, slots),
            vmem(2, main + pad_y + 2 * face_rows, LANES),
            vmem(face_rows, LANES),
            [vmem(rhs, LANES) for _ in rows],
            vmem(PITCH, widths[1]),
            vmem(counts[0], PITCH, widths[1]),
            dma(2 * rhs + 24), dma(len(SHARES)), dma(len(SHARES)), dma(3), dma(3), dma(2),
            dma(3), dma(3), dma(3), dma(3), dma(len(RIMS)), dma(len(RIMS)),
        ],
        compiler_params=pltpu.CompilerParams(has_side_effects=True, collective_id=0),
    )(*operands)
    return pl.pallas_call(
        spread_kernel,
        out_shape=jax.ShapeDtypeStruct(iterate.shape, f32),
        in_specs=[in_vmem],
        out_specs=in_vmem,
    )(grown)


def solution(mesh):
    peers = dict(mesh.shape)
    return jax.shard_map(
        functools.partial(per_device, peers),
        mesh=mesh,
        in_specs=(
            P(None, "gx", "gy", "gz"),
            P(None, "gx", "gy", "gz"),
            P("gx", "gy", "gz"),
            P("gx", "gy", "gz", None),
            P("gx", "gy", "gz", None, None),
            P("gx", "gy", "gz", None, None),
            P("gx", "gy", "gz", None, None),
            P("gx", "gy", "gz", None, None),
            P("gx", "gy", "gz", None),
            P("gx", "gy", "gz", None, None),
            P("gx", "gy", "gz", None, None),
            P("gx", ("gy", "gz"), None),
            P("gx", "gy", "gz", None, None),
            P(("gx", "gy", "gz"), None),
        ),
        out_specs=P(None, "gx", "gy", "gz"),
        check_vma=False,
    )
```

```python
import functools
import itertools

import jax
import jax.numpy as jnp
import numpy as np
from jax import lax
from jax.experimental import pallas as pl
from jax.experimental.pallas import tpu as pltpu
from jax.sharding import PartitionSpec as P

AXES = ("gx", "gy", "gz")
LANES = 128
TILE = 8
PITCH = 32
UNROLL = 64
SIDES = (0, 1, -1)
MESH = pl.DeviceIdType.MESH
f32 = jnp.float32
bf16 = jnp.bfloat16

SHARES = [
    (i, j, k)
    for i in SIDES
    for j in SIDES
    for k in SIDES
    if (i, j, k) != (0, 0, 0) and (i, j, k).count(-1) <= 1
]
RIMS = [(i, j, k) for i in (0, 1) for j in (0, 1) for k in (0, 1) if (i, j, k) != (0, 0, 0)]


def up_to(n, unit):
    return -(-n // unit) * unit


def weight(k):
    return max(0, 4 - abs(k)) / 16.0


def weight_beside(k):
    return weight(k - 1) + weight(k + 1)


def single(a, b):
    return jnp.dot(a, b, preferred_element_type=f32)


def single_back(a, b):
    return lax.dot_general(a, b, (((1,), (1,)), ((), ())), preferred_element_type=f32)


def halves(x):
    high = x.astype(bf16)
    return high, (x - high.astype(f32)).astype(bf16)


def stacked(x):
    high = x.astype(bf16).astype(f32)
    return jnp.concatenate([high, x - high], axis=0).astype(bf16)


def dot_exact(a, b, product=single):
    count = a.shape[0]
    both = product(stacked(a), b)
    return both[:count] + both[count:]


def dot(a, b, product=single):
    count = a.shape[0]
    both = product(stacked(a), b[0][...])
    return both[:count] + both[count:] + product(a.astype(bf16), b[1][...])


def dot_back(a, b):
    return dot(a, b, single_back)


def coarse_at(side, row, count):
    if side == 0:
        return row if row < count else None
    if side == 1:
        return count if row == 0 else None
    return -1 if row == count - 1 else None


def restriction(fine, pad, stencil):
    count = fine // 4
    out = np.zeros((3, pad, fine), np.float32)
    for s, side in enumerate(SIDES):
        for row in range(pad):
            at = coarse_at(side, row, count)
            if at is not None:
                for y in range(fine):
                    out[s, row, y] = stencil(y - 4 * at)
    return out


def at_first(table):
    table = table.copy()
    table[0, 0, 0] -= weight(-1)
    return table


def interpolation(fine, pad):
    count = fine // 4
    out = np.zeros((2, fine, pad), np.float32)
    for y in range(fine):
        for at in (y // 4, y // 4 + 1):
            value = 1.0 - abs(y - 4 * at) / 4.0
            if at < count:
                out[0, y, at] = value
            else:
                out[1, y, 0] = value
    return out


def constants(rhs, ny, nz, side, pad_y, pad_z):
    slabs = side + 2
    edge_rows = up_to(slabs, TILE)
    last = ny // 4 - 1
    eye = np.eye(slabs, dtype=np.float32)
    eye_edge = np.eye(edge_rows, slabs, dtype=np.float32)

    def over_rows(table):
        return np.concatenate([
            np.kron(eye, table[0]),
            np.kron(eye_edge, table[1][0:1]),
            np.kron(eye_edge, table[2][last:last + 1]),
        ], 0)

    plain = over_rows(restriction(ny, pad_y, weight))
    beside = restriction(ny, pad_y, weight_beside)
    rows = np.stack([
        np.concatenate([plain, over_rows(b)], 1) for b in (at_first(beside), beside)
    ])

    def over_lanes(table):
        out = np.zeros((3, rhs * nz, LANES), np.float32)
        for s in range(3):
            for r in range(rhs):
                out[s, r * nz:(r + 1) * nz, r * pad_z:(r + 1) * pad_z] = table[s].T
        return np.concatenate(list(out), 1)

    lanes = over_lanes(restriction(nz, pad_z, weight))
    table = restriction(nz, pad_z, weight_beside)
    lanes_beside = np.stack([over_lanes(at_first(table)), over_lanes(table)])
    grow = interpolation(nz, pad_z)
    wide = np.zeros((2, LANES, rhs * nz), np.float32)
    for s in range(2):
        for r in range(rhs):
            wide[s, r * pad_z:(r + 1) * pad_z, r * nz:(r + 1) * nz] = grow[s].T
    wide = wide.reshape(2 * LANES, rhs * nz)
    tall_of = interpolation(ny, pad_y)
    slab_rows = side * pad_y
    face_rows = up_to(side, TILE)
    tall = np.zeros(((side + 1) * ny, slab_rows + pad_y + 2 * face_rows), np.float32)
    for at in range(side + 1):
        here = slice(at * ny, (at + 1) * ny)
        tall[here, at * pad_y:(at + 1) * pad_y] = tall_of[0]
        beyond = slab_rows + pad_y + (at if at < side else face_rows)
        tall[here, beyond] = tall_of[1][:, 0]
    return rows, lanes, lanes_beside, wide, tall


def kernel(
    sizes,
    right_ref, u_ref, coef_ref, order_ref, leaf_ref, first_ref, second_ref, top_ref,
    fs_ref, ft_ref, st_ref, rows_first, rows_second, rows_top,
    mat_rows, mat_lanes, mat_beside, mat_wide, mat_tall,
    out_ref,
    right_in, u_in, coef_in, order_in, leaf_in, first_in, second_in, top_in,
    fs_in, ft_in, st_in, rows_in, m_rows, m_lanes, m_beside, m_wide, m_tall,
    leaf_split, link_split, fs_seat, ftst_seat, row_seat, rows0, rows1, big, w0, zed, kay,
    packed, shares, share_in, prev, scatter_out, scatter_in, gather_in, top_all, val,
    picked, inner, slots, order_seat, ordered, rim, face, stage, k_own, k_all,
    in_sem, ready, share_send, share_recv, prev_send, prev_recv, k_sem, s_send, s_recv, g_send, g_recv,
    r_send, r_recv,
):
    rhs, nx, ny, nz = u_in.shape
    side = nx // 4
    side_y, side_z = ny // 4, nz // 4
    slabs = side + 2
    pad_y, pad_z = sizes["pad_y"], sizes["pad_z"]
    spans, seats, widths = sizes["spans"], sizes["seats"], sizes["widths"]
    leaf = leaf_in.shape[0]
    at_first_level, at_second, at_top = sizes["starts"]
    peers = sizes["peers"]
    me = {a: lax.axis_index(a) for a in AXES}
    groups = (("gz",), ("gy", "gz"), AXES)
    shift_axis = ("gz", "gy", "gx")
    counts = [int(np.prod([peers[a] for a in g])) for g in groups]
    n_gz = peers["gz"]

    def place(group):
        at = 0
        for a in group:
            at = at * peers[a] + me[a]
        return at

    def coords(group, at):
        found = {}
        for a in reversed(group):
            found[a] = at % peers[a]
            at = at // peers[a]
        return {a: found[a] if a in found else me[a] for a in AXES}

    turned = {a: [me[a]] for a in AXES}
    for a in AXES:
        for k in range(1, peers[a]):
            at = me[a] + k
            turned[a].append(jnp.where(at >= peers[a], at - peers[a], at))

    n_gx = peers["gx"]
    far = [jnp.where(2 * me["gx"] < n_gx, n_gx - 1 - k, k) for k in range(n_gx)]

    def for_others(group, send):
        count = int(np.prod([peers[a] for a in group]))
        if count <= UNROLL:
            for steps in itertools.product(*[range(peers[a]) for a in group]):
                target = dict(me)
                at = 0
                for a, k in zip(group, steps):
                    target[a] = far[k] if a == "gx" else turned[a][k]
                    at = at * peers[a] + target[a]
                if any(steps[-2:]):
                    send(target, at)
                elif len(steps) == 3:
                    @pl.when(target["gx"] != me["gx"])
                    def _():
                        send(target, at)
        else:
            mine = place(group)

            def step(k, carry):
                at = (mine + k) % count
                send(coords(group, at), at)
                return carry

            lax.fori_loop(1, count, step, 0)

    def valid(step, sign):
        ok = None
        for a, d in zip(AXES, step):
            if d:
                at = me[a] + sign * d
                this = (at >= 0) & (at < peers[a])
                ok = this if ok is None else ok & this
        return ok

    def toward(step, sign):
        return {a: (me[a] + sign * d + peers[a]) % peers[a] for a, d in zip(AXES, step)}

    barrier = pltpu.get_barrier_semaphore()

    def greet(target, at):
        pl.semaphore_signal(barrier, inc=1, device_id=target, device_id_type=MESH)

    at_y, at_z = jnp.minimum(me["gy"], 1), jnp.minimum(me["gz"], 1)
    loads = {}

    def load(name, source, into):
        loads[name] = pltpu.make_async_copy(source, into, in_sem.at[len(loads)])
        loads[name].start()

    load("coef", coef_ref, coef_in)
    for r in range(rhs):
        load(("u", r), u_ref.at[r], u_in.at[r])
        load(("right", r), right_ref.at[r], right_in.at[r])
    load("m_rows", mat_rows.at[at_y], m_rows)
    load("m_lanes", mat_lanes, m_lanes)
    load("m_beside", mat_beside.at[at_z], m_beside)
    pack = rhs // 2

    def slot(r):
        return r % 2 * pack + r // 2

    row_sources = (rows_first, rows_second, rows_top)
    for level in range(3):
        load(("rows", level), row_sources[level], rows_in[level])
    load("leaf", leaf_ref, leaf_in)
    load("first", first_ref, first_in)
    load("second", second_ref, second_in)
    load("top", top_ref, top_in)
    load("order", order_ref, order_in)
    load("fs", fs_ref, fs_in)
    load("ft", ft_ref, ft_in)
    load("st", st_ref, st_in)
    load("m_wide", mat_wide, m_wide)
    load("m_tall", mat_tall, m_tall)

    def clear(ref):
        ref[...] = jnp.zeros(ref.shape, ref.dtype)

    for buffer in share_in:
        clear(buffer)
    clear(rim)
    for_others(groups[1], greet)
    for step in itertools.product((1, -1), SIDES, SIDES):
        @pl.when(valid(step, 1))
        def _():
            greet(toward(step, 1), 0)

    def beside(a):
        return jnp.where(me[a] > 0, 1, 0) + jnp.where(me[a] < peers[a] - 1, 1, 0)

    near_count = counts[1] - 1 + beside("gx") * (1 + beside("gy")) * (1 + beside("gz"))

    def relay(step):
        if step:
            @pl.when(me["gx"] >= step)
            def _():
                pl.semaphore_wait(ready.at[0, step - 1], 1)

            @pl.when(me["gx"] + step < n_gx)
            def _():
                pl.semaphore_wait(ready.at[1, step - 1], 1)

        if step < n_gx - 1:
            @pl.when((me["gx"] < n_gx - 1) & (me["gx"] >= step))
            def _():
                pl.semaphore_signal(
                    ready.at[0, step], inc=1, device_id=toward((1, 0, 0), 1), device_id_type=MESH
                )

            @pl.when((me["gx"] > 0) & (me["gx"] + step < n_gx))
            def _():
                pl.semaphore_signal(
                    ready.at[1, step], inc=1, device_id=toward((1, 0, 0), -1), device_id_type=MESH
                )

    for level in range(3):
        @pl.when(me[shift_axis[level]] == 0)
        def _():
            clear(prev[level])
    clear(k_own)
    for level in range(2):
        clear(scatter_out[level])

    half = slabs * ny
    loads["coef"].wait()
    for r in range(rhs):
        loads["u", r].wait()
        loads["right", r].wait()
        acc_p = {}
        acc_u = {}

        def add(acc, at, factor, value):
            term = factor * value
            acc[at] = acc[at] + term if at in acc else term

        for x in range(nx):
            u = u_in[r, x]
            q = right_in[r, x] - (6.0 + coef_in[x]) * u
            for at in range(-1, side + 1):
                k = x - 4 * at
                if weight(k):
                    add(acc_p, at, weight(k), q)
                    add(acc_u, at, weight(k), u)
                if at == 0 and x == 0:
                    below = jnp.where(me["gx"] > 0, weight(-1), 0.0)
                    add(acc_p, at, weight(1) + below, u)
                elif weight_beside(k):
                    add(acc_p, at, weight_beside(k), u)
        for at in range(-1, side + 1):
            rows = slice((at + 1) * ny, (at + 2) * ny)
            packed[rows, r * nz:(r + 1) * nz] = acc_p[at]
            rows = slice(half + (at + 1) * ny, half + (at + 2) * ny)
            packed[rows, r * nz:(r + 1) * nz] = acc_u.get(at, jnp.zeros((ny, nz), f32))
    loads["m_rows"].wait()
    loads["m_lanes"].wait()
    loads["m_beside"].wait()
    high, low = halves(packed[...])
    a = single(m_rows[...], high) + single(m_rows[...], low)
    b = single(m_rows[:, :half], high[half:]) + single(m_rows[:, :half], low[half:])
    c = dot_exact(a, m_lanes[...]) + dot_exact(b, m_beside[...])
    for t in range(3):
        shares[t] = c[:, t * LANES:(t + 1) * LANES]

    for level in range(3):
        loads["rows", level].wait()
    pl.semaphore_wait(barrier, near_count)

    edge_rows = up_to(slabs, TILE)
    main = side * pad_y
    share_copies = []
    for n, step in enumerate(SHARES):
        dx, dy, dz = step
        if dy == 0:
            cut = {0: pl.ds(pad_y, main), 1: pl.ds((side + 1) * pad_y, pad_y), -1: pl.ds(0, pad_y)}[dx]
        else:
            cut = pl.ds(slabs * pad_y + (edge_rows if dy < 0 else 0), edge_rows)
        copy = pltpu.make_async_remote_copy(
            src_ref=shares.at[SIDES.index(dz), cut], dst_ref=share_in[n],
            send_sem=share_send.at[n], recv_sem=share_recv.at[n],
            device_id=toward(step, 1), device_id_type=MESH,
        )
        share_copies.append(copy)

        @pl.when(valid(step, 1))
        def _():
            copy.start()

    prev_copies = []
    for level in range(3):
        axis = shift_axis[level]
        target = dict(me)
        target[axis] = (me[axis] + 1) % peers[axis]
        copy = pltpu.make_async_remote_copy(
            src_ref=rows_in[level], dst_ref=prev[level],
            send_sem=prev_send.at[level], recv_sem=prev_recv.at[level],
            device_id=target, device_id_type=MESH,
        )
        prev_copies.append(copy)

        @pl.when(me[axis] < peers[axis] - 1)
        def _():
            copy.start()

    relay(0)

    def keep(where, value, rows=None):
        high, low = halves(value)
        if rows is None:
            where[0][...], where[1][...] = high, low
        else:
            where[0][rows, :] = high
            where[1][rows, :] = low

    def rows_of(raw):
        return raw[:, 0, :] if len(raw.shape) == 3 else raw[...]

    for name in ("leaf", "first", "second", "top", "fs", "ft", "st", "order"):
        loads[name].wait()
    keep(leaf_split, rows_of(leaf_in))
    link_at = [0, 2 * seats[0], 2 * (seats[0] + seats[1])]
    for pair in (link_split, rows0, rows1, big, w0):
        for part in pair:
            clear(part)
    for level, raw in enumerate((first_in, second_in, top_in)):
        value = rows_of(raw)
        span = spans[level]
        for s in range(2):
            at = link_at[level] + s * seats[level]
            keep(link_split, value[s * span:(s + 1) * span], slice(at, at + span))

    clear(fs_seat)
    clear(ftst_seat)
    for s in range(2):
        span, seat = spans[1], seats[1]
        fs_seat[:spans[0], s * seat:s * seat + span] = rows_of(fs_in)[:, s * span:(s + 1) * span]
        span, seat = spans[2], seats[2]
        ftst_seat[:spans[1], s * seat:s * seat + span] = rows_of(st_in)[:, s * span:(s + 1) * span]
        ftst_seat[PITCH:PITCH + spans[0], s * seat:s * seat + span] = (
            rows_of(ft_in)[:, s * span:(s + 1) * span]
        )

    clear(order_seat)
    starts = (0, leaf, leaf + spans[0], leaf + spans[0] + spans[1], order_in.shape[1])
    seated = (0, at_first_level, at_second, at_top)
    order_seat[...] = jnp.full(order_seat.shape, -1e6, f32)
    for begin, end, at in zip(starts, starts[1:], seated):
        order_seat[:, at:at + end - begin] = order_in[:, begin:end].astype(f32)
    order = order_seat[...]
    first = jnp.floor((order + 0.5) / (side_y * side_z))
    rest = order - first * (side_y * side_z)
    second = jnp.floor((rest + 0.5) / side_z)
    third = rest - second * side_z
    cells = order.shape[1]

    def row_iota(count):
        return lax.broadcasted_iota(jnp.int32, (count, cells), 0).astype(f32)

    main_hot = (row_iota(main) == first * pad_y + second).astype(f32)
    edge_id = row_iota(edge_rows)
    near = (edge_id == first + 1) | ((edge_id == slabs - 1) & (first == 0)) | (
        (edge_id == 0) & (first == side - 1)
    )
    pick_hot = jnp.concatenate([
        main_hot,
        (near & (second == 0)).astype(f32),
        (near & (second == side_y - 1)).astype(f32),
    ], 0)
    face_rows = face.shape[0]
    face_hot = ((row_iota(face_rows) == first) & (second == 0)).astype(f32)
    back_hot = jnp.concatenate([main_hot, face_hot], 0)
    lane_id = lax.broadcasted_iota(jnp.int32, (LANES, cells), 0).astype(f32)

    def lane_hot(r):
        return (lane_id == third + r * pad_z).astype(f32).astype(bf16)

    def wait_prev(level):
        @pl.when(me[shift_axis[level]] > 0)
        def _():
            prev_copies[level].wait_recv()

    def seat_lanes(value, level):
        span = spans[level]
        row_seat[level][...] = jnp.zeros(row_seat[level].shape, f32)
        for d in range(counts[level]):
            row_seat[level][:, d * PITCH:d * PITCH + span] = value[:, d * span:(d + 1) * span]
        return row_seat[level][...]

    relay(1)
    links = dot_back(rows_of(leaf_in), link_split)
    wait_prev(0)
    own0 = seat_lanes(rows_of(rows_in[0]), 0)
    keep(rows0, own0, slice(0, spans[0]))
    keep(w0, own0, slice(at_first_level, at_first_level + spans[0]))
    keep(rows0, seat_lanes(rows_of(prev[0]), 0), slice(seats[0], seats[0] + spans[0]))
    e0 = dot(links[:, :2 * seats[0]], rows0)
    keep(w0, -e0, slice(0, leaf))
    own1 = seat_lanes(rows_of(rows_in[1]), 1)
    keep(rows1, own1, slice(0, spans[1]))
    mine0 = place(groups[0])

    def send_k(target, at):
        pltpu.make_async_remote_copy(
            src_ref=k_own, dst_ref=k_all.at[mine0],
            send_sem=k_sem.at[0], recv_sem=k_sem.at[1],
            device_id=target, device_id_type=MESH,
        ).start()

    def all_slots(buffer, sem, count):
        return pltpu.make_async_copy(
            buffer.at[pl.ds(0, count - 1)], buffer.at[pl.ds(0, count - 1)], sem
        )

    relay(2)
    received = {}
    for n, step in enumerate(SHARES):
        @pl.when(valid(step, -1))
        def _():
            share_copies[n].wait_recv()
    for n, step in enumerate(SHARES):
        dx, dy, dz = step
        received[dx, dy] = received[dx, dy] + share_in[n][...] if (dx, dy) in received else share_in[n][...]

    total = shares[0, pad_y:pad_y + main] + received[0, 0]
    pieces = [total[:pad_y] + received[1, 0], total[pad_y:main - pad_y], total[main - pad_y:] + received[-1, 0]]
    edge_lane = lax.broadcasted_iota(jnp.int32, (edge_rows, LANES), 0)
    inside = (edge_lane >= 1) & (edge_lane <= side)
    for dy in (1, -1):
        tile = jnp.where(inside, received[0, dy], 0.0)
        tile = tile + jnp.where(edge_lane == slabs - 1, received[1, dy], 0.0)
        if (-1, dy) in received:
            tile = tile + jnp.where(edge_lane == 0, received[-1, dy], 0.0)
        pieces.append(tile)
    coarse = jnp.concatenate(pieces, 0)
    for r in range(rhs):
        spread = dot_exact(coarse, lane_hot(r))
        picked[slot(r):slot(r) + 1, :] = jnp.sum(spread * pick_hot, axis=0, keepdims=True)

    def scatter(level, terms, pitch, lane):
        span, group = spans[level], groups[level]
        out, into = scatter_out[level], scatter_in[level]
        for d in range(counts[level]):
            part = terms[:, d * pitch:d * pitch + span]
            if level == 2:
                out[d, :, :span] = part[:pack]
                out[d, :, LANES // 2:LANES // 2 + span] = part[pack:]
            else:
                out[d, :, lane:lane + span] = part
        mine = place(group)

        def send(target, d):
            pltpu.make_async_remote_copy(
                src_ref=out.at[d], dst_ref=into.at[mine],
                send_sem=s_send.at[level], recv_sem=s_recv.at[level],
                device_id=target, device_id_type=MESH,
            ).start()

        for_others(group, send)
        into[mine] = out[mine]

    def scatter_end(level):
        into = scatter_in[level]
        all_slots(into, s_recv.at[level], counts[level]).wait()
        return jnp.sum(into[...], axis=0)

    def gather(level, value):
        group = groups[level]
        into, own = gather_in[level], stage[level]
        mine = place(group)
        own[...] = value

        def send(target, d):
            pltpu.make_async_remote_copy(
                src_ref=own, dst_ref=into.at[mine],
                send_sem=g_send.at[level], recv_sem=g_recv.at[level],
                device_id=target, device_id_type=MESH,
            ).start()

        for_others(group, send)
        into[mine] = own[...]

    def gather_end(level):
        into = gather_in[level]
        all_slots(into, g_recv.at[level], counts[level]).wait()
        return into

    scatter(0, dot(picked[:, :at_top], w0), PITCH, PITCH)
    leaf_rhs = picked[:, :leaf]
    lows = dot(leaf_rhs, halves(links[:, 2 * seats[0]:]))
    pair1, pair2 = 2 * seats[1], 2 * seats[2]
    inner[...] = -lows[:, :pair1]
    inner[:, :spans[1]] = picked[:, at_second:at_second + spans[1]] - lows[:, :spans[1]]
    slots[...] = -lows[:, pair1:]
    slots[:, :spans[2]] = picked[:, at_top:at_top + spans[2]] - lows[:, pair1:pair1 + spans[2]]
    wait_prev(1)
    keep(rows1, seat_lanes(rows_of(prev[1]), 1), slice(seats[1], seats[1] + spans[1]))
    k_own[...] = dot(fs_seat[...], rows1)
    base1 = dot(inner[...], rows1)
    k_halves = halves(k_own[...])
    first_own = scatter_end(0)
    scatter(1, base1 - dot(first_own[:, PITCH:2 * PITCH], k_halves), PITCH, 0)
    for_others(groups[0], send_k)
    k_all[mine0] = k_own[...]

    wait_prev(2)
    keep(big, rows_of(rows_in[2]), slice(0, spans[2]))
    keep(big, rows_of(prev[2]), slice(seats[2], seats[2] + spans[2]))
    rows2 = (big[0].at[pl.ds(0, pair2)], big[1].at[pl.ds(0, pair2)])
    queue = slice(LANES, LANES + 2 * PITCH)
    keep(big, dot(ftst_seat[...], rows2), queue)
    base2 = dot(slots[...], rows2)
    queue_rows = (big[0].at[queue], big[1].at[queue])
    base2 = base2 - dot(first_own[:, :2 * PITCH], queue_rows)
    leaf_solved = dot(leaf_rhs, leaf_split)
    second_own = scatter_end(1)
    for step in range(3, n_gx):
        relay(step)
    scatter(2, base2 - dot(second_own[:, :2 * PITCH], queue_rows), spans[2], 0)
    both_own = (first_own + second_own)[:, :2 * PITCH]
    e1 = dot(links[:, 2 * seats[0]:2 * (seats[0] + seats[1])], rows1)
    w1_value = jnp.concatenate([
        -e1, jnp.zeros((at_second - leaf, e1.shape[1]), f32), own1,
        jnp.zeros((at_top - at_second - spans[1], e1.shape[1]), f32),
    ], 0)
    all_slots(k_all, k_sem.at[1], n_gz).wait()
    keep(kay, k_all[...].reshape(n_gz * PITCH, k_own.shape[1]))
    w0_value = w0[0][...].astype(f32) + w0[1][...].astype(f32)
    gap_width = widths[1]
    high, low = halves(w1_value - dot(w0_value, kay))
    zed[0][:, :gap_width], zed[1][:, :gap_width] = high, low
    zed[0][:, gap_width:], zed[1][:, gap_width:] = w0[0][...], w0[1][...]
    top_own = scatter_end(2)
    gather(2, top_own)
    into = gather_end(2)
    for d in range(counts[2]):
        at = slice(d * spans[2], (d + 1) * spans[2])
        top_all[:pack, at] = into[d, :, :spans[2]]
        top_all[pack:, at] = into[d, :, LANES // 2:LANES // 2 + spans[2]]
    solved = dot_back(top_all[...], big)
    gather(1, jnp.concatenate([
        both_own - solved[:, LANES:LANES + 2 * PITCH], jnp.zeros((rhs, LANES - 2 * PITCH), f32)
    ], 1))
    top_link = (link_split[0].at[pl.ds(link_at[2], pair2)], link_split[1].at[pl.ds(link_at[2], pair2)])
    base = dot_back(leaf_solved - dot(solved[:, :pair2], top_link), leaf_split)

    for level in range(3):
        @pl.when(me[shift_axis[level]] < peers[shift_axis[level]] - 1)
        def _():
            prev_copies[level].wait_send()

        all_slots(scatter_out[level], s_send.at[level], counts[level]).wait()
    all_slots(k_all, k_sem.at[0], n_gz).wait()
    all_slots(gather_in[2], g_send.at[2], counts[2]).wait()
    for n, step in enumerate(SHARES):
        @pl.when(valid(step, 1))
        def _():
            share_copies[n].wait_send()

    into = gather_end(1)
    clear(val)
    for d in range(counts[1]):
        val[:, d * PITCH:d * PITCH + spans[1]] = into[d, :, :spans[1]]
    for d in range(n_gz):
        at = gap_width + d * PITCH
        val[:, at:at + spans[0]] = into[me["gy"] * n_gz + d, :, PITCH:PITCH + spans[0]]
    back = dot_back(val[...], zed)
    clear(ordered)
    ordered[:, :at_top] = back
    ordered[:, :leaf] = back[:, :leaf] + base
    ordered[:, at_top:at_top + spans[2]] = solved[:, :spans[2]]

    cells_back = None
    for r in range(rhs):
        term = dot_exact(back_hot * ordered[slot(r):slot(r) + 1, :], lane_hot(r), single_back)
        cells_back = term if cells_back is None else cells_back + term
    rim[0, 0:main] = cells_back[:main]
    face[...] = cells_back[main:]

    rim_copies = []
    for n, step in enumerate(RIMS):
        dx, dy, dz = step
        if dy:
            source, at = face, main + pad_y + (face_rows if dx else 0)
        elif dx:
            source, at = rim.at[0, pl.ds(0, pad_y)], main
        else:
            source, at = rim.at[0, pl.ds(0, main)], 0
        rows = face_rows if dy else (pad_y if dx else main)
        copy = pltpu.make_async_remote_copy(
            src_ref=source, dst_ref=rim.at[dz, pl.ds(at, rows)],
            send_sem=r_send.at[n], recv_sem=r_recv.at[n],
            device_id=toward(step, -1), device_id_type=MESH,
        )
        rim_copies.append(copy)

        @pl.when(valid(step, -1))
        def _():
            copy.start()

    loads["m_wide"].wait()
    loads["m_tall"].wait()
    all_slots(gather_in[1], g_send.at[1], counts[1]).wait()
    for n, step in enumerate(RIMS):
        @pl.when(valid(step, 1))
        def _():
            rim_copies[n].wait_recv()

    wide = dot_exact(jnp.concatenate([rim[0], rim[1]], 1), m_wide[...])
    high, low = halves(wide)
    out_ref[...] = single(m_tall[...], high) + single(m_tall[...], low)

    for n, step in enumerate(RIMS):
        @pl.when(valid(step, -1))
        def _():
            rim_copies[n].wait_send()


def spread_kernel(grown_ref, out_ref, held, sem):
    rhs, nx, ny, nz = out_ref.shape
    side = nx // 4
    copies = []
    for r in range(rhs):
        slices = [
            grown_ref[at * ny:(at + 1) * ny, r * nz:(r + 1) * nz] for at in range(side + 1)
        ]
        for x in range(nx):
            at, k = x // 4, x % 4
            if k == 0:
                held[r, x] = slices[at]
            else:
                held[r, x] = (1 - k / 4) * slices[at] + (k / 4) * slices[at + 1]
        copy = pltpu.make_async_copy(held.at[r], out_ref.at[r], sem.at[r])
        copy.start()
        copies.append(copy)
    for copy in copies:
        copy.wait()


def per_device(peers, right_side, iterate, coefficient, ordering, leaf_inverse, leaf_first,
               leaf_second, leaf_top, first_inverse, first_second, first_top, second_inverse,
               second_top, top_inverse):
    rhs, nx, ny, nz = iterate.shape
    side = nx // 4
    slabs = side + 2
    pad_y = up_to(ny // 4, TILE)
    pad_z = LANES // rhs // 4 if nz // 4 <= LANES // rhs // 4 else LANES // rhs
    mats = [jnp.asarray(m, bf16) for m in constants(rhs, ny, nz, side, pad_y, pad_z)]
    flip = lambda m: jnp.swapaxes(m, -1, -2)
    flat = lambda m: m.reshape(m.shape[-2:])
    single_rows = lambda m: m.reshape(m.shape[-2], 1, m.shape[-1])
    rows = [single_rows(first_inverse), single_rows(second_inverse), top_inverse]
    spans = [m.shape[0] for m in rows]
    counts = [m.shape[-1] // s for m, s in zip(rows, spans)]
    seats = [up_to(s, 16) for s in spans]
    seats[0] = seats[1] = PITCH
    widths = [counts[0] * PITCH, up_to(counts[1] * PITCH, LANES), rows[2].shape[-1]]
    leaf = leaf_inverse.shape[-1]
    cells = ordering.shape[-1]
    at_first_level = up_to(leaf, 16)
    at_second = at_first_level + PITCH
    at_top = at_second + PITCH
    slots = up_to(at_top + spans[2], LANES)
    vmem = lambda *shape: pltpu.VMEM(shape, f32)
    split = lambda *shape: [pltpu.VMEM(shape, bf16)] * 2
    like = lambda m: pltpu.VMEM(m.shape, m.dtype)
    dma = lambda n: pltpu.SemaphoreType.DMA((n,))
    sizes = {
        "peers": peers, "pad_y": pad_y, "pad_z": pad_z, "spans": spans, "seats": seats,
        "widths": widths, "starts": (at_first_level, at_second, at_top),
    }
    matrices = (
        ordering.reshape(1, cells), single_rows(leaf_inverse),
        single_rows(flip(leaf_first)), single_rows(flip(leaf_second)), flat(flip(leaf_top)),
        single_rows(first_second), single_rows(first_top), single_rows(second_top),
    )
    operands = (right_side, iterate, coefficient, *matrices, *rows, *mats)
    edge_rows = up_to(slabs, TILE)
    face_rows = up_to(side, TILE)
    main = side * pad_y

    def share_shape(step):
        dx, dy, _ = step
        return (edge_rows if dy else (pad_y if dx else main), LANES)

    in_vmem = pl.BlockSpec(memory_space=pltpu.VMEM)
    anywhere = pl.BlockSpec(memory_space=pl.ANY)
    links = 2 * sum(seats)
    packs = (rhs, rhs, rhs // 2)
    big_rows = LANES + 2 * PITCH
    grown = pl.pallas_call(
        functools.partial(kernel, sizes),
        out_shape=pltpu.VMEM(((side + 1) * ny, rhs * nz), f32),
        in_specs=jax.tree.map(lambda _: anywhere, operands),
        out_specs=in_vmem,
        scratch_shapes=[
            like(right_side), like(iterate), like(coefficient), *[like(m) for m in matrices],
            [like(m) for m in rows],
            pltpu.VMEM(mats[0].shape[1:], bf16), like(mats[1]),
            pltpu.VMEM(mats[2].shape[1:], bf16), like(mats[3]), like(mats[4]),
            split(leaf, leaf),
            split(links, leaf),
            vmem(PITCH, 2 * seats[1]),
            vmem(2 * PITCH, 2 * seats[2]),
            [vmem(spans[level], widths[level]) for level in range(2)],
            split(2 * seats[0], widths[0]),
            split(2 * seats[1], widths[1]),
            split(big_rows, widths[2]),
            split(at_top, widths[0]),
            split(at_top, widths[1] + widths[0]),
            split(counts[0] * PITCH, widths[1]),
            vmem(2 * slabs * ny, rhs * nz),
            vmem(3, slabs * pad_y + 2 * edge_rows, LANES),
            [vmem(*share_shape(step)) for step in SHARES],
            [like(m) for m in rows],
            [vmem(n, p, LANES) for n, p in zip(counts, packs)],
            [vmem(n, p, LANES) for n, p in zip(counts, packs)],
            [vmem(n, p, LANES) for n, p in zip(counts, packs)],
            vmem(rhs, widths[2]),
            vmem(rhs, widths[1] + widths[0]),
            vmem(rhs, slots),
            vmem(rhs, 2 * seats[1]),
            vmem(rhs, 2 * seats[2]),
            vmem(1, slots),
            vmem(rhs, slots),
            vmem(2, main + pad_y + 2 * face_rows, LANES),
            vmem(face_rows, LANES),
            [vmem(p, LANES) for p in packs],
            vmem(PITCH, widths[1]),
            vmem(counts[0], PITCH, widths[1]),
            dma(2 * rhs + 24), pltpu.SemaphoreType.REGULAR((2, max(peers["gx"] - 1, 1))), dma(len(SHARES)), dma(len(SHARES)), dma(3), dma(3), dma(2),
            dma(3), dma(3), dma(3), dma(3), dma(len(RIMS)), dma(len(RIMS)),
        ],
        compiler_params=pltpu.CompilerParams(has_side_effects=True, collective_id=0),
    )(*operands)
    return pl.pallas_call(
        spread_kernel,
        out_shape=jax.ShapeDtypeStruct(iterate.shape, f32),
        in_specs=[in_vmem],
        out_specs=anywhere,
        scratch_shapes=[like(iterate), dma(rhs)],
    )(pltpu.with_memory_space_constraint(grown, pltpu.VMEM))


def solution(mesh):
    peers = dict(mesh.shape)
    return jax.shard_map(
        functools.partial(per_device, peers),
        mesh=mesh,
        in_specs=(
            P(None, "gx", "gy", "gz"),
            P(None, "gx", "gy", "gz"),
            P("gx", "gy", "gz"),
            P("gx", "gy", "gz", None),
            P("gx", "gy", "gz", None, None),
            P("gx", "gy", "gz", None, None),
            P("gx", "gy", "gz", None, None),
            P("gx", "gy", "gz", None, None),
            P("gx", "gy", "gz", None),
            P("gx", "gy", "gz", None, None),
            P("gx", "gy", "gz", None, None),
            P("gx", ("gy", "gz"), None),
            P("gx", "gy", "gz", None, None),
            P(("gx", "gy", "gz"), None),
        ),
        out_specs=P(None, "gx", "gy", "gz"),
        check_vma=False,
    )
```

```python
import functools
import itertools

import jax
import jax.numpy as jnp
import numpy as np
from jax import lax
from jax.experimental import pallas as pl
from jax.experimental.pallas import tpu as pltpu
from jax.sharding import PartitionSpec as P

AXES = ("gx", "gy", "gz")
LANES = 128
TILE = 8
PITCH = 32
UNROLL = 64
SIDES = (0, 1, -1)
MESH = pl.DeviceIdType.MESH
f32 = jnp.float32
bf16 = jnp.bfloat16

SHARES = [
    (i, j, k)
    for i in SIDES
    for j in SIDES
    for k in SIDES
    if (i, j, k) != (0, 0, 0) and (i, j, k).count(-1) <= 1
]
SHARES.sort(key=lambda step: -2 * abs(step[1]) - abs(step[0]))
RIMS = [(i, j, k) for i in (0, 1) for j in (0, 1) for k in (0, 1) if (i, j, k) != (0, 0, 0)]
RIMS.sort(key=lambda step: -2 * step[1] - step[0])


def up_to(n, unit):
    return -(-n // unit) * unit


def weight(k):
    return max(0, 4 - abs(k)) / 16.0


def weight_beside(k):
    return weight(k - 1) + weight(k + 1)


def single(a, b):
    return jnp.dot(a, b, preferred_element_type=f32)


def single_back(a, b):
    return lax.dot_general(a, b, (((1,), (1,)), ((), ())), preferred_element_type=f32)


def halves(x):
    high = x.astype(bf16)
    return high, (x - high.astype(f32)).astype(bf16)


def stacked(x):
    high = x.astype(bf16).astype(f32)
    return jnp.concatenate([high, x - high], axis=0).astype(bf16)


def dot_exact(a, b, product=single):
    count = a.shape[0]
    both = product(stacked(a), b)
    return both[:count] + both[count:]


def dot(a, b, product=single):
    count = a.shape[0]
    both = product(stacked(a), b[0][...])
    return both[:count] + both[count:] + product(a.astype(bf16), b[1][...])


def dot_back(a, b):
    return dot(a, b, single_back)


def coarse_at(side, row, count):
    if side == 0:
        return row if row < count else None
    if side == 1:
        return count if row == 0 else None
    return -1 if row == count - 1 else None


def restriction(fine, pad, stencil):
    count = fine // 4
    out = np.zeros((3, pad, fine), np.float32)
    for s, side in enumerate(SIDES):
        for row in range(pad):
            at = coarse_at(side, row, count)
            if at is not None:
                for y in range(fine):
                    out[s, row, y] = stencil(y - 4 * at)
    return out


def at_first(table):
    table = table.copy()
    table[0, 0, 0] -= weight(-1)
    return table


def interpolation(fine, pad):
    count = fine // 4
    out = np.zeros((2, fine, pad), np.float32)
    for y in range(fine):
        for at in (y // 4, y // 4 + 1):
            value = 1.0 - abs(y - 4 * at) / 4.0
            if at < count:
                out[0, y, at] = value
            else:
                out[1, y, 0] = value
    return out


def constants(rhs, ny, nz, side, pad_y, pad_z):
    slabs = side + 2
    edge_rows = up_to(slabs, TILE)
    last = ny // 4 - 1
    eye = np.eye(slabs, dtype=np.float32)
    eye_edge = np.eye(edge_rows, slabs, dtype=np.float32)

    def over_rows(table):
        return np.concatenate([
            np.kron(eye, table[0]),
            np.kron(eye_edge, table[1][0:1]),
            np.kron(eye_edge, table[2][last:last + 1]),
        ], 0)

    plain = over_rows(restriction(ny, pad_y, weight))
    beside = restriction(ny, pad_y, weight_beside)
    rows = np.stack([
        np.concatenate([plain, over_rows(b)], 1) for b in (at_first(beside), beside)
    ])

    def over_lanes(table):
        out = np.zeros((3, rhs * nz, LANES), np.float32)
        for s in range(3):
            for r in range(rhs):
                out[s, r * nz:(r + 1) * nz, r * pad_z:(r + 1) * pad_z] = table[s].T
        return np.concatenate(list(out), 1)

    lanes = over_lanes(restriction(nz, pad_z, weight))
    table = restriction(nz, pad_z, weight_beside)
    lanes_beside = np.stack([over_lanes(at_first(table)), over_lanes(table)])
    grow = interpolation(nz, pad_z)
    wide = np.zeros((2, LANES, rhs * nz), np.float32)
    for s in range(2):
        for r in range(rhs):
            wide[s, r * pad_z:(r + 1) * pad_z, r * nz:(r + 1) * nz] = grow[s].T
    wide = wide.reshape(2 * LANES, rhs * nz)
    tall_of = interpolation(ny, pad_y)
    slab_rows = side * pad_y
    face_rows = up_to(side, TILE)
    tall = np.zeros(((side + 1) * ny, slab_rows + pad_y + 2 * face_rows), np.float32)
    for at in range(side + 1):
        here = slice(at * ny, (at + 1) * ny)
        tall[here, at * pad_y:(at + 1) * pad_y] = tall_of[0]
        beyond = slab_rows + pad_y + (at if at < side else face_rows)
        tall[here, beyond] = tall_of[1][:, 0]
    return rows, lanes, lanes_beside, wide, tall


def kernel(
    sizes,
    right_ref, u_ref, coef_ref, order_ref, leaf_ref, first_ref, second_ref, top_ref,
    fs_ref, ft_ref, st_ref, rows_first, rows_second, rows_top,
    mat_rows, mat_lanes, mat_beside, mat_wide, mat_tall, blank,
    out_ref,
    right_in, u_in, coef_in, order_in, leaf_in, first_in, second_in, top_in,
    fs_in, ft_in, st_in, rows_in, m_rows, m_lanes, m_beside, m_wide, m_tall,
    leaf_split, link_split, fs_seat, ftst_seat, row_seat, rows0, rows1, big, w0, w1, zed, kay,
    packed, shares, share_in, prev, scatter_out, scatter_in, gather_in, top_all, val,
    picked, slots, order_seat, ordered, rim, face, stage, k_own, k_all,
    in_sem, ready, share_recv, rim_recv, prev_recv, k_sem, s_recv, g_recv,
):
    rhs, nx, ny, nz = u_in.shape
    side = nx // 4
    side_y, side_z = ny // 4, nz // 4
    slabs = side + 2
    pad_y, pad_z = sizes["pad_y"], sizes["pad_z"]
    edge_rows = up_to(slabs, TILE)
    main = side * pad_y
    spans, seats, widths = sizes["spans"], sizes["seats"], sizes["widths"]
    leaf = leaf_in.shape[0]
    at_first_level, at_second, at_top = sizes["starts"]
    peers = sizes["peers"]
    me = {a: lax.axis_index(a) for a in AXES}
    groups = (("gz",), ("gy", "gz"), AXES)
    shift_axis = ("gz", "gy", "gx")
    counts = [int(np.prod([peers[a] for a in g])) for g in groups]
    n_gz = peers["gz"]

    def place(group):
        at = 0
        for a in group:
            at = at * peers[a] + me[a]
        return at

    def coords(group, at):
        found = {}
        for a in reversed(group):
            found[a] = at % peers[a]
            at = at // peers[a]
        return {a: found[a] if a in found else me[a] for a in AXES}

    turned = {a: [me[a]] for a in AXES}
    for a in AXES:
        for k in range(1, peers[a]):
            at = me[a] + k
            if peers[a] & (peers[a] - 1):
                turned[a].append(jnp.where(at >= peers[a], at - peers[a], at))
            else:
                turned[a].append(me[a] ^ k)

    n_gx = peers["gx"]
    far = [jnp.where(2 * me["gx"] < n_gx, n_gx - 1 - k, k) for k in range(n_gx)]

    def for_others(group, send):
        count = int(np.prod([peers[a] for a in group]))
        if count <= UNROLL:
            for steps in itertools.product(*[range(peers[a]) for a in group]):
                target = dict(me)
                at = 0
                for a, k in zip(group, steps):
                    target[a] = far[k] if a == "gx" else turned[a][-k]
                    at = at * peers[a] + target[a]
                if any(steps[-2:]):
                    send(target, at)
                elif len(steps) == 3:
                    @pl.when(target["gx"] != me["gx"])
                    def _():
                        send(target, at)
        else:
            mine = place(group)

            def step(k, carry):
                at = (mine + k) % count
                send(coords(group, at), at)
                return carry

            lax.fori_loop(1, count, step, 0)

    def valid(step, sign):
        ok = None
        for a, d in zip(AXES, step):
            if d:
                at = me[a] + sign * d
                this = (at >= 0) & (at < peers[a])
                ok = this if ok is None else ok & this
        return ok

    def toward(step, sign):
        return {a: (me[a] + sign * d + peers[a]) % peers[a] for a, d in zip(AXES, step)}

    barrier = pltpu.get_barrier_semaphore()

    def greet(target, at):
        pl.semaphore_signal(barrier, inc=1, device_id=target, device_id_type=MESH)

    at_y, at_z = jnp.minimum(me["gy"], 1), jnp.minimum(me["gz"], 1)
    loads = {}

    def load(name, source, into):
        loads[name] = pltpu.make_async_copy(source, into, in_sem.at[len(loads)])
        loads[name].start()

    load("coef", coef_ref, coef_in)
    for r in range(rhs):
        load(("u", r), u_ref.at[r], u_in.at[r])
        load(("right", r), right_ref.at[r], right_in.at[r])
    load("m_rows", mat_rows.at[at_y], m_rows)
    load("m_lanes", mat_lanes, m_lanes)
    load("m_beside", mat_beside.at[at_z], m_beside)
    pack = rhs // 2

    def slot(r):
        return r % 2 * pack + r // 2

    row_sources = (rows_first, rows_second, rows_top)
    for level in range(3):
        load(("rows", level), row_sources[level], rows_in[level])
    load("leaf", leaf_ref, leaf_in)
    load("first", first_ref, first_in)
    load("second", second_ref, second_in)
    load("top", top_ref, top_in)
    load("order", order_ref, order_in)
    load("fs", fs_ref, fs_in)
    load("ft", ft_ref, ft_in)
    load("st", st_ref, st_in)
    load("m_wide", mat_wide, m_wide)
    load("m_tall", mat_tall, m_tall)

    share_at = [0]
    for step in SHARES:
        dx, dy, dz = step
        share_at.append(share_at[-1] + (edge_rows if dy else (pad_y if dx else main)))
    for n, step in enumerate(SHARES):
        @pl.when(jnp.logical_not(valid(step, -1)))
        def _():
            part = pl.ds(share_at[n], share_at[n + 1] - share_at[n])
            pltpu.make_async_copy(
                blank.at[pl.ds(0, share_at[n + 1] - share_at[n])], share_in.at[part], share_recv
            ).start()
    face_rows = face.shape[0]

    def rim_place(step):
        dx, dy, dz = step
        if dy:
            return face_rows, main + pad_y + (face_rows if dx else 0)
        return (pad_y, main) if dx else (main, 0)

    for n, step in enumerate(RIMS):
        @pl.when(jnp.logical_not(valid(step, 1)))
        def _():
            rows, at = rim_place(step)
            pltpu.make_async_copy(
                blank.at[pl.ds(0, rows)], rim.at[step[2], pl.ds(at, rows)], rim_recv
            ).start()

    def clear(ref):
        ref[...] = jnp.zeros(ref.shape, ref.dtype)

    for_others(groups[1], greet)
    for step in itertools.product((1, -1), SIDES, SIDES):
        @pl.when(valid(step, 1))
        def _():
            greet(toward(step, 1), 0)

    def beside(a):
        return jnp.where(me[a] > 0, 1, 0) + jnp.where(me[a] < peers[a] - 1, 1, 0)

    near_count = counts[1] - 1 + beside("gx") * (1 + beside("gy")) * (1 + beside("gz"))

    def relay(step):
        if step:
            @pl.when(me["gx"] >= step)
            def _():
                pl.semaphore_wait(ready.at[0, step - 1], 1)

            @pl.when(me["gx"] + step < n_gx)
            def _():
                pl.semaphore_wait(ready.at[1, step - 1], 1)

        if step < n_gx - 1:
            @pl.when((me["gx"] < n_gx - 1) & (me["gx"] >= step))
            def _():
                pl.semaphore_signal(
                    ready.at[0, step], inc=1, device_id=toward((1, 0, 0), 1), device_id_type=MESH
                )

            @pl.when((me["gx"] > 0) & (me["gx"] + step < n_gx))
            def _():
                pl.semaphore_signal(
                    ready.at[1, step], inc=1, device_id=toward((1, 0, 0), -1), device_id_type=MESH
                )

    for level in range(3):
        @pl.when(me[shift_axis[level]] == 0)
        def _():
            clear(prev[level])
    clear(k_own)
    for level in range(2):
        clear(scatter_out[level])

    half = slabs * ny
    loads["coef"].wait()
    for r in range(rhs):
        loads["u", r].wait()
        loads["right", r].wait()
        acc_p = {}
        acc_u = {}

        def add(acc, at, factor, value):
            term = factor * value
            acc[at] = acc[at] + term if at in acc else term

        for x in range(nx):
            u = u_in[r, x]
            q = right_in[r, x] - (6.0 + coef_in[x]) * u
            for at in range(-1, side + 1):
                k = x - 4 * at
                if weight(k):
                    add(acc_p, at, weight(k), q)
                    add(acc_u, at, weight(k), u)
                if at == 0 and x == 0:
                    below = jnp.where(me["gx"] > 0, weight(-1), 0.0)
                    add(acc_p, at, weight(1) + below, u)
                elif weight_beside(k):
                    add(acc_p, at, weight_beside(k), u)
        for at in range(-1, side + 1):
            rows = slice((at + 1) * ny, (at + 2) * ny)
            packed[rows, r * nz:(r + 1) * nz] = acc_p[at]
            rows = slice(half + (at + 1) * ny, half + (at + 2) * ny)
            packed[rows, r * nz:(r + 1) * nz] = acc_u.get(at, jnp.zeros((ny, nz), f32))
    loads["m_rows"].wait()
    loads["m_lanes"].wait()
    loads["m_beside"].wait()
    high, low = halves(packed[...])
    a = single(m_rows[...], high) + single(m_rows[...], low)
    b = single(m_rows[:, :half], high[half:]) + single(m_rows[:, :half], low[half:])
    c = dot_exact(a, m_lanes[...]) + dot_exact(b, m_beside[...])
    for t in range(3):
        shares[t] = c[:, t * LANES:(t + 1) * LANES]

    for name in loads:
        if name not in ("coef", "m_rows", "m_lanes", "m_beside") and name[0] not in ("u", "right"):
            loads[name].wait()
    pl.semaphore_wait(barrier, near_count)

    share_copies = []
    for n, step in enumerate(SHARES):
        dx, dy, dz = step
        if dy == 0:
            cut = {0: pl.ds(pad_y, main), 1: pl.ds((side + 1) * pad_y, pad_y), -1: pl.ds(0, pad_y)}[dx]
        else:
            cut = pl.ds(slabs * pad_y + (edge_rows if dy < 0 else 0), edge_rows)
        copy = pltpu.make_async_remote_copy(
            src_ref=shares.at[SIDES.index(dz), cut],
            dst_ref=share_in.at[pl.ds(share_at[n], share_at[n + 1] - share_at[n])],
            send_sem=in_sem.at[n], recv_sem=share_recv,
            device_id=toward(step, 1), device_id_type=MESH,
        )
        share_copies.append(copy)

        @pl.when(valid(step, 1))
        def _():
            copy.start()

    prev_copies = []
    for level in range(3):
        axis = shift_axis[level]
        target = dict(me)
        target[axis] = (me[axis] + 1) % peers[axis]
        copy = pltpu.make_async_remote_copy(
            src_ref=rows_in[level], dst_ref=prev[level],
            send_sem=in_sem.at[len(SHARES) + level], recv_sem=prev_recv.at[level],
            device_id=target, device_id_type=MESH,
        )
        prev_copies.append(copy)

        @pl.when(me[axis] < peers[axis] - 1)
        def _():
            copy.start()

    relay(0)

    def keep(where, value, rows=None):
        high, low = halves(value)
        if rows is None:
            where[0][...], where[1][...] = high, low
        else:
            where[0][rows, :] = high
            where[1][rows, :] = low

    def rows_of(raw):
        return raw[:, 0, :] if len(raw.shape) == 3 else raw[...]

    keep(leaf_split, rows_of(leaf_in))
    link_at = [0, 2 * seats[0], 2 * (seats[0] + seats[1])]
    for pair in (link_split, rows0, rows1, big, w0, w1):
        for part in pair:
            clear(part)
    for level, raw in enumerate((first_in, second_in, top_in)):
        value = rows_of(raw)
        span = spans[level]
        for s in range(2):
            at = link_at[level] + s * seats[level]
            keep(link_split, value[s * span:(s + 1) * span], slice(at, at + span))

    clear(fs_seat)
    clear(ftst_seat)
    for s in range(2):
        span, seat = spans[1], seats[1]
        fs_seat[:spans[0], s * seat:s * seat + span] = rows_of(fs_in)[:, s * span:(s + 1) * span]
        span, seat = spans[2], seats[2]
        ftst_seat[:spans[1], s * seat:s * seat + span] = rows_of(st_in)[:, s * span:(s + 1) * span]
        ftst_seat[PITCH:PITCH + spans[0], s * seat:s * seat + span] = (
            rows_of(ft_in)[:, s * span:(s + 1) * span]
        )

    clear(order_seat)
    starts = (0, leaf, leaf + spans[0], leaf + spans[0] + spans[1], order_in.shape[1])
    seated = (0, at_first_level, at_second, at_top)
    order_seat[...] = jnp.full(order_seat.shape, -1e6, f32)
    for begin, end, at in zip(starts, starts[1:], seated):
        order_seat[:, at:at + end - begin] = order_in[:, begin:end].astype(f32)
    order = order_seat[...]
    first = jnp.floor((order + 0.5) / (side_y * side_z))
    rest = order - first * (side_y * side_z)
    second = jnp.floor((rest + 0.5) / side_z)
    third = rest - second * side_z
    cells = order.shape[1]

    def row_iota(count):
        return lax.broadcasted_iota(jnp.int32, (count, cells), 0).astype(f32)

    main_hot = (row_iota(main) == first * pad_y + second).astype(f32)
    edge_id = row_iota(edge_rows)
    near = (edge_id == first + 1) | ((edge_id == slabs - 1) & (first == 0)) | (
        (edge_id == 0) & (first == side - 1)
    )
    pick_hot = jnp.concatenate([
        main_hot,
        (near & (second == 0)).astype(f32),
        (near & (second == side_y - 1)).astype(f32),
    ], 0)
    face_hot = ((row_iota(face_rows) == first) & (second == 0)).astype(f32)
    back_hot = jnp.concatenate([main_hot, face_hot], 0)
    lane_id = lax.broadcasted_iota(jnp.int32, (LANES, cells), 0).astype(f32)

    def lane_hot(r):
        return (lane_id == third + r * pad_z).astype(f32).astype(bf16)

    def wait_prev(level):
        @pl.when(me[shift_axis[level]] > 0)
        def _():
            prev_copies[level].wait_recv()

    def seat_lanes(value, level):
        span = spans[level]
        row_seat[level][...] = jnp.zeros(row_seat[level].shape, f32)
        for d in range(counts[level]):
            row_seat[level][:, d * PITCH:d * PITCH + span] = value[:, d * span:(d + 1) * span]
        return row_seat[level][...]

    relay(1)
    links = dot_back(rows_of(leaf_in), link_split)
    wait_prev(0)
    own0 = seat_lanes(rows_of(rows_in[0]), 0)
    keep(rows0, own0, slice(0, spans[0]))
    keep(w0, own0, slice(at_first_level, at_first_level + spans[0]))
    keep(rows0, seat_lanes(rows_of(prev[0]), 0), slice(seats[0], seats[0] + spans[0]))
    e0 = dot(links[:, :2 * seats[0]], rows0)
    keep(w0, -e0, slice(0, leaf))
    own1 = seat_lanes(rows_of(rows_in[1]), 1)
    keep(rows1, own1, slice(0, spans[1]))
    mine0 = place(groups[0])

    def send_k(target, at):
        pltpu.make_async_remote_copy(
            src_ref=k_own, dst_ref=k_all.at[mine0],
            send_sem=in_sem.at[len(SHARES) + 3], recv_sem=k_sem.at[0],
            device_id=target, device_id_type=MESH,
        ).start()

    def s_send(level):
        return in_sem.at[len(SHARES) + 4 + level]

    def g_send(level):
        return in_sem.at[len(SHARES) + 6 + level]

    def all_slots(buffer, sem, count):
        return pltpu.make_async_copy(
            buffer.at[pl.ds(0, count - 1)], buffer.at[pl.ds(0, count - 1)], sem
        )

    relay(2)
    wait_prev(1)
    keep(rows1, seat_lanes(rows_of(prev[1]), 1), slice(seats[1], seats[1] + spans[1]))
    k_own[...] = dot(fs_seat[...], rows1)
    for_others(groups[0], send_k)
    k_all[mine0] = k_own[...]
    e1 = dot(links[:, 2 * seats[0]:2 * (seats[0] + seats[1])], rows1)
    w1_value = jnp.concatenate([
        -e1, jnp.zeros((at_second - leaf, e1.shape[1]), f32), own1,
        jnp.zeros((at_top - at_second - spans[1], e1.shape[1]), f32),
    ], 0)
    keep(w1, w1_value)
    received = {}
    pltpu.make_async_copy(share_in, share_in, share_recv).wait()
    for n, step in enumerate(SHARES):
        part = share_in[share_at[n]:share_at[n + 1]]
        received[step[:2]] = received[step[:2]] + part if step[:2] in received else part

    total = shares[0, pad_y:pad_y + main] + received[0, 0]
    pieces = [total[:pad_y] + received[1, 0], total[pad_y:main - pad_y], total[main - pad_y:] + received[-1, 0]]
    edge_lane = lax.broadcasted_iota(jnp.int32, (edge_rows, LANES), 0)
    inside = (edge_lane >= 1) & (edge_lane <= side)
    for dy in (1, -1):
        tile = jnp.where(inside, received[0, dy], 0.0)
        tile = tile + jnp.where(edge_lane == slabs - 1, received[1, dy], 0.0)
        if (-1, dy) in received:
            tile = tile + jnp.where(edge_lane == 0, received[-1, dy], 0.0)
        pieces.append(tile)
    coarse = jnp.concatenate(pieces, 0)
    for r in range(rhs):
        spread = dot_exact(coarse, lane_hot(r))
        picked[slot(r):slot(r) + 1, :] = jnp.sum(spread * pick_hot, axis=0, keepdims=True)

    def scatter(level, terms, pitch, lane):
        span, group = spans[level], groups[level]
        out, into = scatter_out[level], scatter_in[level]
        for d in range(counts[level]):
            part = terms[:, d * pitch:d * pitch + span]
            if level == 2:
                out[d, :, :span] = part[:pack]
                out[d, :, LANES // 2:LANES // 2 + span] = part[pack:]
            else:
                out[d, :, lane:lane + span] = part
        mine = place(group)

        def send(target, d):
            pltpu.make_async_remote_copy(
                src_ref=out.at[d], dst_ref=into.at[mine],
                send_sem=s_send(level), recv_sem=s_recv.at[level],
                device_id=target, device_id_type=MESH,
            ).start()

        for_others(group, send)
        into[mine] = out[mine]

    def scatter_end(level):
        into = scatter_in[level]
        all_slots(into, s_recv.at[level], counts[level]).wait()
        return jnp.sum(into[...], axis=0)

    def gather(level, value):
        group = groups[level]
        into, own = gather_in[level], stage[level]
        mine = place(group)
        own[...] = value

        def send(target, d):
            pltpu.make_async_remote_copy(
                src_ref=own, dst_ref=into.at[mine],
                send_sem=g_send(level), recv_sem=g_recv.at[level - 1],
                device_id=target, device_id_type=MESH,
            ).start()

        for_others(group, send)
        into[mine] = own[...]

    def gather_end(level):
        into = gather_in[level]
        all_slots(into, g_recv.at[level - 1], counts[level]).wait()
        return into

    terms0 = dot(picked[:, :at_top], w0)
    base1 = dot(picked[:, :at_top], w1)
    all_slots(k_all, k_sem.at[0], n_gz).wait()
    keep(kay, k_all[...].reshape(n_gz * PITCH, k_own.shape[1]))
    scatter(1, base1 - dot(terms0, kay), PITCH, 0)
    scatter(0, terms0, PITCH, PITCH)
    leaf_rhs = picked[:, :leaf]
    lows = dot(leaf_rhs, halves(links[:, 2 * (seats[0] + seats[1]):]))
    pair2 = 2 * seats[2]
    slots[...] = -lows
    slots[:, :spans[2]] = picked[:, at_top:at_top + spans[2]] - lows[:, :spans[2]]

    wait_prev(2)
    keep(big, rows_of(rows_in[2]), slice(0, spans[2]))
    keep(big, rows_of(prev[2]), slice(seats[2], seats[2] + spans[2]))
    rows2 = (big[0].at[pl.ds(0, pair2)], big[1].at[pl.ds(0, pair2)])
    queue = slice(LANES, LANES + 2 * PITCH)
    keep(big, dot(ftst_seat[...], rows2), queue)
    base2 = dot(slots[...], rows2)
    first_own = scatter_end(0)
    queue_rows = (big[0].at[queue], big[1].at[queue])
    base2 = base2 - dot(first_own[:, :2 * PITCH], queue_rows)
    leaf_solved = dot(leaf_rhs, leaf_split)
    second_own = scatter_end(1)
    for step in range(3, n_gx):
        relay(step)
    scatter(2, base2 - dot(second_own[:, :2 * PITCH], queue_rows), spans[2], 0)
    both_own = (first_own + second_own)[:, :2 * PITCH]
    w0_value = w0[0][...].astype(f32) + w0[1][...].astype(f32)
    gap_width = widths[1]
    high, low = halves(w1_value - dot(w0_value, kay))
    zed[0][:, :gap_width], zed[1][:, :gap_width] = high, low
    zed[0][:, gap_width:], zed[1][:, gap_width:] = w0[0][...], w0[1][...]
    top_own = scatter_end(2)
    gather(2, top_own)
    into = gather_end(2)
    for d in range(counts[2]):
        at = slice(d * spans[2], (d + 1) * spans[2])
        top_all[:pack, at] = into[d, :, :spans[2]]
        top_all[pack:, at] = into[d, :, LANES // 2:LANES // 2 + spans[2]]
    solved = dot_back(top_all[...], big)
    gather(1, jnp.concatenate([
        both_own - solved[:, LANES:LANES + 2 * PITCH], jnp.zeros((rhs, LANES - 2 * PITCH), f32)
    ], 1))
    top_link = (link_split[0].at[pl.ds(link_at[2], pair2)], link_split[1].at[pl.ds(link_at[2], pair2)])
    base = dot_back(leaf_solved - dot(solved[:, :pair2], top_link), leaf_split)

    for level in range(3):
        @pl.when(me[shift_axis[level]] < peers[shift_axis[level]] - 1)
        def _():
            prev_copies[level].wait_send()

        all_slots(scatter_out[level], s_send(level), counts[level]).wait()
    all_slots(k_all, in_sem.at[len(SHARES) + 3], n_gz).wait()
    all_slots(gather_in[2], g_send(2), counts[2]).wait()
    for n, step in enumerate(SHARES):
        @pl.when(valid(step, 1))
        def _():
            share_copies[n].wait_send()

    into = gather_end(1)
    clear(val)
    for d in range(counts[1]):
        val[:, d * PITCH:d * PITCH + spans[1]] = into[d, :, :spans[1]]
    for d in range(n_gz):
        at = gap_width + d * PITCH
        val[:, at:at + spans[0]] = into[me["gy"] * n_gz + d, :, PITCH:PITCH + spans[0]]
    back = dot_back(val[...], zed)
    clear(ordered)
    ordered[:, :at_top] = back
    ordered[:, :leaf] = back[:, :leaf] + base
    ordered[:, at_top:at_top + spans[2]] = solved[:, :spans[2]]

    cells_back = None
    for r in range(rhs):
        term = dot_exact(back_hot * ordered[slot(r):slot(r) + 1, :], lane_hot(r), single_back)
        cells_back = term if cells_back is None else cells_back + term
    rim[0, 0:main] = cells_back[:main]
    face[...] = cells_back[main:]

    rim_copies = []
    for n, step in enumerate(RIMS):
        dx, dy, dz = step
        rows, at = rim_place(step)
        copy = pltpu.make_async_remote_copy(
            src_ref=face if dy else rim.at[0, pl.ds(0, rows)],
            dst_ref=rim.at[dz, pl.ds(at, rows)],
            send_sem=in_sem.at[n], recv_sem=rim_recv,
            device_id=toward(step, -1), device_id_type=MESH,
        )
        rim_copies.append(copy)

        @pl.when(valid(step, -1))
        def _():
            copy.start()

    all_slots(gather_in[1], g_send(1), counts[1]).wait()
    arrived = share_in.at[pl.ds(0, 2 * rim.shape[1] - main)]
    pltpu.make_async_copy(arrived, arrived, rim_recv).wait()

    wide = dot_exact(jnp.concatenate([rim[0], rim[1]], 1), m_wide[...])
    high, low = halves(wide)
    out_ref[...] = single(m_tall[...], high) + single(m_tall[...], low)

    for n, step in enumerate(RIMS):
        @pl.when(valid(step, -1))
        def _():
            rim_copies[n].wait_send()


def spread_kernel(grown_ref, out_ref, held, sem):
    rhs, nx, ny, nz = out_ref.shape
    side = nx // 4
    copies = []
    for r in range(rhs):
        slices = [
            grown_ref[at * ny:(at + 1) * ny, r * nz:(r + 1) * nz] for at in range(side + 1)
        ]
        for x in range(nx):
            at, k = x // 4, x % 4
            if k == 0:
                held[r, x] = slices[at]
            else:
                held[r, x] = (1 - k / 4) * slices[at] + (k / 4) * slices[at + 1]
        copy = pltpu.make_async_copy(held.at[r], out_ref.at[r], sem.at[r])
        copy.start()
        copies.append(copy)
    for copy in copies:
        copy.wait()


def per_device(peers, right_side, iterate, coefficient, ordering, leaf_inverse, leaf_first,
               leaf_second, leaf_top, first_inverse, first_second, first_top, second_inverse,
               second_top, top_inverse):
    rhs, nx, ny, nz = iterate.shape
    side = nx // 4
    slabs = side + 2
    pad_y = up_to(ny // 4, TILE)
    pad_z = LANES // rhs // 4 if nz // 4 <= LANES // rhs // 4 else LANES // rhs
    mats = [jnp.asarray(m, bf16) for m in constants(rhs, ny, nz, side, pad_y, pad_z)]
    flip = lambda m: jnp.swapaxes(m, -1, -2)
    flat = lambda m: m.reshape(m.shape[-2:])
    single_rows = lambda m: m.reshape(m.shape[-2], 1, m.shape[-1])
    rows = [single_rows(first_inverse), single_rows(second_inverse), top_inverse]
    spans = [m.shape[0] for m in rows]
    counts = [m.shape[-1] // s for m, s in zip(rows, spans)]
    seats = [up_to(s, 16) for s in spans]
    seats[0] = seats[1] = PITCH
    widths = [counts[0] * PITCH, up_to(counts[1] * PITCH, LANES), rows[2].shape[-1]]
    leaf = leaf_inverse.shape[-1]
    cells = ordering.shape[-1]
    at_first_level = up_to(leaf, 16)
    at_second = at_first_level + PITCH
    at_top = at_second + PITCH
    slots = up_to(at_top + spans[2], LANES)
    vmem = lambda *shape: pltpu.VMEM(shape, f32)
    split = lambda *shape: [pltpu.VMEM(shape, bf16)] * 2
    like = lambda m: pltpu.VMEM(m.shape, m.dtype)
    dma = lambda n: pltpu.SemaphoreType.DMA((n,))
    sizes = {
        "peers": peers, "pad_y": pad_y, "pad_z": pad_z, "spans": spans, "seats": seats,
        "widths": widths, "starts": (at_first_level, at_second, at_top),
    }
    matrices = (
        ordering.reshape(1, cells), single_rows(leaf_inverse),
        single_rows(flip(leaf_first)), single_rows(flip(leaf_second)), flat(flip(leaf_top)),
        single_rows(first_second), single_rows(first_top), single_rows(second_top),
    )
    edge_rows = up_to(slabs, TILE)
    face_rows = up_to(side, TILE)
    main = side * pad_y
    blank = np.zeros((main + TILE, LANES), np.float32)
    blank[main:] = 1.0
    operands = (right_side, iterate, coefficient, *matrices, *rows, *mats, jnp.asarray(blank))

    def share_shape(step):
        dx, dy, _ = step
        return (edge_rows if dy else (pad_y if dx else main), LANES)

    in_vmem = pl.BlockSpec(memory_space=pltpu.VMEM)
    anywhere = pl.BlockSpec(memory_space=pl.ANY)
    links = 2 * sum(seats)
    packs = (rhs, rhs, rhs // 2)
    big_rows = LANES + 2 * PITCH
    grown = pl.pallas_call(
        functools.partial(kernel, sizes),
        out_shape=pltpu.VMEM(((side + 1) * ny, rhs * nz), f32),
        in_specs=jax.tree.map(lambda _: anywhere, operands),
        out_specs=in_vmem,
        scratch_shapes=[
            like(right_side), like(iterate), like(coefficient), *[like(m) for m in matrices],
            [like(m) for m in rows],
            pltpu.VMEM(mats[0].shape[1:], bf16), like(mats[1]),
            pltpu.VMEM(mats[2].shape[1:], bf16), like(mats[3]), like(mats[4]),
            split(leaf, leaf),
            split(links, leaf),
            vmem(PITCH, 2 * seats[1]),
            vmem(2 * PITCH, 2 * seats[2]),
            [vmem(spans[level], widths[level]) for level in range(2)],
            split(2 * seats[0], widths[0]),
            split(2 * seats[1], widths[1]),
            split(big_rows, widths[2]),
            split(at_top, widths[0]),
            split(at_top, widths[1]),
            split(at_top, widths[1] + widths[0]),
            split(counts[0] * PITCH, widths[1]),
            vmem(2 * slabs * ny, rhs * nz),
            vmem(3, slabs * pad_y + 2 * edge_rows, LANES),
            vmem(sum(share_shape(step)[0] for step in SHARES), LANES),
            [like(m) for m in rows],
            [vmem(n, p, LANES) for n, p in zip(counts, packs)],
            [vmem(n, p, LANES) for n, p in zip(counts, packs)],
            [vmem(n, p, LANES) for n, p in zip(counts, packs)],
            vmem(rhs, widths[2]),
            vmem(rhs, widths[1] + widths[0]),
            vmem(rhs, slots),
            vmem(rhs, 2 * seats[2]),
            vmem(1, slots),
            vmem(rhs, slots),
            vmem(2, main + pad_y + 2 * face_rows, LANES),
            vmem(face_rows, LANES),
            [vmem(p, LANES) for p in packs],
            vmem(PITCH, widths[1]),
            vmem(counts[0], PITCH, widths[1]),
            dma(max(len(SHARES) + 9, 2 * rhs + len(operands) - 3)),
            pltpu.SemaphoreType.REGULAR((2, max(peers["gx"] - 1, 1))),
            pltpu.SemaphoreType.DMA, pltpu.SemaphoreType.DMA, dma(3), dma(1), dma(3), dma(2),
        ],
        compiler_params=pltpu.CompilerParams(has_side_effects=True, collective_id=0),
    )(*operands)
    return pl.pallas_call(
        spread_kernel,
        out_shape=jax.ShapeDtypeStruct(iterate.shape, f32),
        in_specs=[in_vmem],
        out_specs=anywhere,
        scratch_shapes=[like(iterate), dma(rhs)],
    )(pltpu.with_memory_space_constraint(grown, pltpu.VMEM))


def solution(mesh):
    peers = dict(mesh.shape)
    return jax.shard_map(
        functools.partial(per_device, peers),
        mesh=mesh,
        in_specs=(
            P(None, "gx", "gy", "gz"),
            P(None, "gx", "gy", "gz"),
            P("gx", "gy", "gz"),
            P("gx", "gy", "gz", None),
            P("gx", "gy", "gz", None, None),
            P("gx", "gy", "gz", None, None),
            P("gx", "gy", "gz", None, None),
            P("gx", "gy", "gz", None, None),
            P("gx", "gy", "gz", None),
            P("gx", "gy", "gz", None, None),
            P("gx", "gy", "gz", None, None),
            P("gx", ("gy", "gz"), None),
            P("gx", "gy", "gz", None, None),
            P(("gx", "gy", "gz"), None),
        ),
        out_specs=P(None, "gx", "gy", "gz"),
        check_vma=False,
    )
```

```python
import functools
import itertools

import jax
import jax.numpy as jnp
import numpy as np
from jax import lax
from jax.experimental import pallas as pl
from jax.experimental.pallas import tpu as pltpu
from jax.sharding import PartitionSpec as P

AXES = ("gx", "gy", "gz")
LANES = 128
TILE = 8
PITCH = 32
UNROLL = 64
SIDES = (0, 1, -1)
MESH = pl.DeviceIdType.MESH
f32 = jnp.float32
bf16 = jnp.bfloat16

SHARES = [
    (i, j, k)
    for i in SIDES
    for j in SIDES
    for k in SIDES
    if (i, j, k) != (0, 0, 0) and (i, j, k).count(-1) <= 1
]
SHARES.sort(key=lambda step: -2 * abs(step[1]) - abs(step[0]))
RIMS = [(i, j, k) for i in (0, 1) for j in (0, 1) for k in (0, 1) if (i, j, k) != (0, 0, 0)]
RIMS.sort(key=lambda step: -2 * step[1] - step[0])


def up_to(n, unit):
    return -(-n // unit) * unit


def weight(k):
    return max(0, 4 - abs(k)) / 16.0


def weight_beside(k):
    return weight(k - 1) + weight(k + 1)


def single(a, b):
    return jnp.dot(a, b, preferred_element_type=f32)


def single_back(a, b):
    return lax.dot_general(a, b, (((1,), (1,)), ((), ())), preferred_element_type=f32)


def halves(x):
    high = x.astype(bf16)
    return high, (x - high.astype(f32)).astype(bf16)


def stacked(x):
    high = x.astype(bf16).astype(f32)
    return jnp.concatenate([high, x - high], axis=0).astype(bf16)


def dot_exact(a, b, product=single):
    count = a.shape[0]
    both = product(stacked(a), b)
    return both[:count] + both[count:]


def dot(a, b, product=single):
    count = a.shape[0]
    both = product(stacked(a), b[0][...])
    return both[:count] + both[count:] + product(a.astype(bf16), b[1][...])


def dot_back(a, b):
    return dot(a, b, single_back)


def coarse_at(side, row, count):
    if side == 0:
        return row if row < count else None
    if side == 1:
        return count if row == 0 else None
    return -1 if row == count - 1 else None


def restriction(fine, pad, stencil):
    count = fine // 4
    out = np.zeros((3, pad, fine), np.float32)
    for s, side in enumerate(SIDES):
        for row in range(pad):
            at = coarse_at(side, row, count)
            if at is not None:
                for y in range(fine):
                    out[s, row, y] = stencil(y - 4 * at)
    return out


def at_first(table):
    table = table.copy()
    table[0, 0, 0] -= weight(-1)
    return table


def interpolation(fine, pad):
    count = fine // 4
    out = np.zeros((2, fine, pad), np.float32)
    for y in range(fine):
        for at in (y // 4, y // 4 + 1):
            value = 1.0 - abs(y - 4 * at) / 4.0
            if at < count:
                out[0, y, at] = value
            else:
                out[1, y, 0] = value
    return out


def face_cuts(side, side_y, side_z):
    faces = [side_y * side_z, side * side_z, side * side_y, side_y, side]
    starts = [0]
    for n in faces:
        starts.append(starts[-1] + up_to(n, 16))
    source = {
        (1, 0, 0): (0, 0), (0, 1, 0): (1, 1), (0, 0, 1): (2, 2), (1, 1, 0): (0, None),
        (1, 0, 1): (3, 3), (0, 1, 1): (4, 4), (1, 1, 1): (0, None),
    }
    cuts, at = {"rows": starts[-1], "starts": starts}, 0
    for step in RIMS:
        face, size = source[step]
        rows = up_to(side_z if size is None else faces[size], TILE)
        cuts[step] = (starts[face], rows, at)
        at += up_to(rows, 16)
    cuts["end"] = at
    return cuts


def constants(rhs, ny, nz, side, pad_y, pad_z):
    slabs = side + 2
    edge_rows = up_to(slabs, TILE)
    last = ny // 4 - 1
    eye = np.eye(slabs, dtype=np.float32)
    eye_edge = np.eye(edge_rows, slabs, dtype=np.float32)

    def over_rows(table):
        return np.concatenate([
            np.kron(eye, table[0]),
            np.kron(eye_edge, table[1][0:1]),
            np.kron(eye_edge, table[2][last:last + 1]),
        ], 0)

    plain = over_rows(restriction(ny, pad_y, weight))
    beside = restriction(ny, pad_y, weight_beside)
    rows = np.stack([
        np.concatenate([plain, over_rows(b)], 1) for b in (at_first(beside), beside)
    ])

    def over_lanes(table):
        out = np.zeros((3, rhs * nz, LANES), np.float32)
        for s in range(3):
            for r in range(rhs):
                out[s, r * nz:(r + 1) * nz, r * pad_z:(r + 1) * pad_z] = table[s].T
        return np.concatenate(list(out), 1)

    lanes = over_lanes(restriction(nz, pad_z, weight))
    table = restriction(nz, pad_z, weight_beside)
    lanes_beside = np.stack([over_lanes(at_first(table)), over_lanes(table)])
    grow = interpolation(nz, pad_z)
    pack = rhs // 2
    wide = np.zeros((rhs * nz, rhs * pad_z + TILE), np.float32)
    for r in range(rhs):
        wide[r * nz:(r + 1) * nz, r * pad_z:(r + 1) * pad_z] = grow[0]
        wide[r * nz:(r + 1) * nz, rhs * pad_z + r % 2 * pack + r // 2] = grow[1][:, 0]
    tall_of = interpolation(ny, pad_y)
    slab_rows = side * pad_y
    face_rows = up_to(side, TILE)
    tall = np.zeros(((side + 1) * ny, slab_rows + pad_y + 2 * face_rows), np.float32)
    cuts = face_cuts(side, ny // 4, nz // 4)
    beyond = np.zeros((TILE, up_to(cuts["end"], LANES)), np.float32)
    beyond[:2] = -1.0
    sizes = (side, ny // 4, nz // 4)
    for step in RIMS:
        ranges = [range(1) if d else range(n) for d, n in zip(step, sizes)]
        for at, (x, y, z) in enumerate(itertools.product(*ranges)):
            if step[1]:
                row = slab_rows + pad_y + (face_rows if step[0] else x)
            else:
                row = slab_rows + y if step[0] else x * pad_y + y
            slot = cuts[step][2] + at
            beyond[0, slot] = row
            beyond[1, slot] = -1 if step[2] else z
            beyond[2, slot] = step[2]
    for at in range(side + 1):
        here = slice(at * ny, (at + 1) * ny)
        tall[here, at * pad_y:(at + 1) * pad_y] = tall_of[0]
        corner = slab_rows + pad_y + (at if at < side else face_rows)
        tall[here, corner] = tall_of[1][:, 0]
    return rows, lanes, lanes_beside, wide, tall, beyond


def kernel(
    sizes,
    right_ref, u_ref, coef_ref, order_ref, leaf_ref, first_ref, second_ref, top_ref,
    fs_ref, ft_ref, st_ref, rows_first, rows_second, rows_top,
    mat_rows, mat_lanes, mat_beside, mat_wide, mat_tall, mat_beyond, blank,
    out_ref,
    right_in, u_in, coef_in, order_in, leaf_in, first_in, second_in, top_in,
    fs_in, ft_in, st_in, rows_in, m_rows, m_lanes, m_beside, m_wide, m_tall, m_beyond,
    leaf_split, link_split, fs_seat, ftst_seat, row_seat, rows0, rows1, big, w0, w1, zed, kay, face_hot, back_hot, face_out, face_in, base_out, base_in, face_top, upper,
    packed, shares, share_in, prev, scatter_out, scatter_in, gather_in, top_all, val,
    picked, slots, order_seat, ordered, stage, k_own, k_all,
    in_sem, ready, share_recv, face_recv, base_recv, upper_recv, prev_recv, k_sem, s_recv, g_recv,
):
    rhs, nx, ny, nz = u_in.shape
    side = nx // 4
    side_y, side_z = ny // 4, nz // 4
    slabs = side + 2
    pad_y, pad_z = sizes["pad_y"], sizes["pad_z"]
    edge_rows = up_to(slabs, TILE)
    main = side * pad_y
    spans, seats, widths = sizes["spans"], sizes["seats"], sizes["widths"]
    leaf = leaf_in.shape[0]
    at_first_level, at_second, at_top = sizes["starts"]
    peers = sizes["peers"]
    me = {a: lax.axis_index(a) for a in AXES}
    groups = (("gz",), ("gy", "gz"), AXES)
    shift_axis = ("gz", "gy", "gx")
    counts = [int(np.prod([peers[a] for a in g])) for g in groups]
    n_gz = peers["gz"]

    def place(group):
        at = 0
        for a in group:
            at = at * peers[a] + me[a]
        return at

    def coords(group, at):
        found = {}
        for a in reversed(group):
            found[a] = at % peers[a]
            at = at // peers[a]
        return {a: found[a] if a in found else me[a] for a in AXES}

    turned = {a: [me[a]] for a in AXES}
    for a in AXES:
        for k in range(1, peers[a]):
            at = me[a] + k
            if peers[a] & (peers[a] - 1):
                turned[a].append(jnp.where(at >= peers[a], at - peers[a], at))
            else:
                turned[a].append(me[a] ^ k)

    n_gx = peers["gx"]
    far = [jnp.where(2 * me["gx"] < n_gx, n_gx - 1 - k, k) for k in range(n_gx)]

    def for_others(group, send):
        count = int(np.prod([peers[a] for a in group]))
        if count <= UNROLL:
            for steps in itertools.product(*[range(peers[a]) for a in group]):
                target = dict(me)
                at = 0
                for a, k in zip(group, steps):
                    target[a] = far[k] if a == "gx" else turned[a][-k]
                    at = at * peers[a] + target[a]
                if any(steps[-2:]):
                    send(target, at)
                elif len(steps) == 3:
                    @pl.when(target["gx"] != me["gx"])
                    def _():
                        send(target, at)
        else:
            mine = place(group)

            def step(k, carry):
                at = (mine + k) % count
                send(coords(group, at), at)
                return carry

            lax.fori_loop(1, count, step, 0)

    def valid(step, sign):
        ok = None
        for a, d in zip(AXES, step):
            if d:
                at = me[a] + sign * d
                this = (at >= 0) & (at < peers[a])
                ok = this if ok is None else ok & this
        return ok

    def toward(step, sign):
        return {a: (me[a] + sign * d + peers[a]) % peers[a] for a, d in zip(AXES, step)}

    barrier = pltpu.get_barrier_semaphore()

    def greet(target, at):
        pl.semaphore_signal(barrier, inc=1, device_id=target, device_id_type=MESH)

    at_y, at_z = jnp.minimum(me["gy"], 1), jnp.minimum(me["gz"], 1)
    loads = {}

    def load(name, source, into):
        loads[name] = pltpu.make_async_copy(source, into, in_sem.at[len(loads)])
        loads[name].start()

    load("coef", coef_ref, coef_in)
    for r in range(rhs):
        load(("u", r), u_ref.at[r], u_in.at[r])
        load(("right", r), right_ref.at[r], right_in.at[r])
    load("m_rows", mat_rows.at[at_y], m_rows)
    load("m_lanes", mat_lanes, m_lanes)
    load("m_beside", mat_beside.at[at_z], m_beside)
    pack = rhs // 2

    def slot(r):
        return r % 2 * pack + r // 2

    row_sources = (rows_first, rows_second, rows_top)
    for level in range(3):
        load(("rows", level), row_sources[level], rows_in[level])
    load("leaf", leaf_ref, leaf_in)
    load("first", first_ref, first_in)
    load("second", second_ref, second_in)
    load("top", top_ref, top_in)
    load("order", order_ref, order_in)
    load("fs", fs_ref, fs_in)
    load("ft", ft_ref, ft_in)
    load("st", st_ref, st_in)
    load("m_wide", mat_wide, m_wide)
    load("m_tall", mat_tall, m_tall)
    load("m_beyond", mat_beyond, m_beyond)

    share_at = [0]
    for step in SHARES:
        dx, dy, dz = step
        share_at.append(share_at[-1] + (edge_rows if dy else (pad_y if dx else main)))
    for n, step in enumerate(SHARES):
        @pl.when(jnp.logical_not(valid(step, -1)))
        def _():
            part = pl.ds(share_at[n], share_at[n + 1] - share_at[n])
            pltpu.make_async_copy(
                blank.at[pl.ds(0, share_at[n + 1] - share_at[n]), pl.ds(0, LANES)], share_in.at[part], share_recv
            ).start()
    cuts = face_cuts(side, side_y, side_z)
    back_width = widths[1] + widths[0]
    for n, step in enumerate(RIMS):
        @pl.when(jnp.logical_not(valid(step, 1)))
        def _():
            _, rows, at = cuts[step]
            pltpu.make_async_copy(
                blank.at[pl.ds(0, rows), pl.ds(0, back_width)],
                face_in.at[pl.ds(at, rows), pl.ds(0, back_width)], face_recv
            ).start()
            pltpu.make_async_copy(
                blank.at[pl.ds(0, TILE), pl.ds(0, base_out.shape[1])], base_in.at[n], base_recv
            ).start()

    def clear(ref):
        ref[...] = jnp.zeros(ref.shape, ref.dtype)

    for_others(groups[1], greet)
    for step in itertools.product((1, -1), SIDES, SIDES):
        @pl.when(valid(step, 1))
        def _():
            greet(toward(step, 1), 0)

    def beside(a):
        return jnp.where(me[a] > 0, 1, 0) + jnp.where(me[a] < peers[a] - 1, 1, 0)

    near_count = counts[1] - 1 + beside("gx") * (1 + beside("gy")) * (1 + beside("gz"))

    def relay(step):
        if step:
            @pl.when(me["gx"] >= step)
            def _():
                pl.semaphore_wait(ready.at[0, step - 1], 1)

            @pl.when(me["gx"] + step < n_gx)
            def _():
                pl.semaphore_wait(ready.at[1, step - 1], 1)

        if step < n_gx - 1:
            @pl.when((me["gx"] < n_gx - 1) & (me["gx"] >= step))
            def _():
                pl.semaphore_signal(
                    ready.at[0, step], inc=1, device_id=toward((1, 0, 0), 1), device_id_type=MESH
                )

            @pl.when((me["gx"] > 0) & (me["gx"] + step < n_gx))
            def _():
                pl.semaphore_signal(
                    ready.at[1, step], inc=1, device_id=toward((1, 0, 0), -1), device_id_type=MESH
                )

    for level in range(3):
        @pl.when(me[shift_axis[level]] == 0)
        def _():
            clear(prev[level])

    @pl.when(me["gx"] == n_gx - 1)
    def _():
        clear(upper)

    clear(k_own)
    for level in range(2):
        clear(scatter_out[level])

    half = slabs * ny
    loads["coef"].wait()
    for r in range(rhs):
        loads["u", r].wait()
        loads["right", r].wait()
        acc_p = {}
        acc_u = {}

        def add(acc, at, factor, value):
            term = factor * value
            acc[at] = acc[at] + term if at in acc else term

        for x in range(nx):
            u = u_in[r, x]
            q = right_in[r, x] - (6.0 + coef_in[x]) * u
            for at in range(-1, side + 1):
                k = x - 4 * at
                if weight(k):
                    add(acc_p, at, weight(k), q)
                    add(acc_u, at, weight(k), u)
                if at == 0 and x == 0:
                    below = jnp.where(me["gx"] > 0, weight(-1), 0.0)
                    add(acc_p, at, weight(1) + below, u)
                elif weight_beside(k):
                    add(acc_p, at, weight_beside(k), u)
        for at in range(-1, side + 1):
            rows = slice((at + 1) * ny, (at + 2) * ny)
            packed[rows, r * nz:(r + 1) * nz] = acc_p[at]
            rows = slice(half + (at + 1) * ny, half + (at + 2) * ny)
            packed[rows, r * nz:(r + 1) * nz] = acc_u.get(at, jnp.zeros((ny, nz), f32))
    loads["m_rows"].wait()
    loads["m_lanes"].wait()
    loads["m_beside"].wait()
    high, low = halves(packed[...])
    a = single(m_rows[...], high) + single(m_rows[...], low)
    b = single(m_rows[:, :half], high[half:]) + single(m_rows[:, :half], low[half:])
    c = dot_exact(a, m_lanes[...]) + dot_exact(b, m_beside[...])
    for t in range(3):
        shares[t] = c[:, t * LANES:(t + 1) * LANES]

    for name in loads:
        if name not in ("coef", "m_rows", "m_lanes", "m_beside") and name[0] not in ("u", "right"):
            loads[name].wait()
    pl.semaphore_wait(barrier, near_count)

    prev_copies = []
    for level in range(3):
        axis = shift_axis[level]
        target = dict(me)
        target[axis] = (me[axis] + 1) % peers[axis]
        copy = pltpu.make_async_remote_copy(
            src_ref=rows_in[level], dst_ref=prev[level],
            send_sem=in_sem.at[len(SHARES) + level], recv_sem=prev_recv.at[level],
            device_id=target, device_id_type=MESH,
        )
        prev_copies.append(copy)

    def send_prev(level):
        @pl.when(me[shift_axis[level]] < peers[shift_axis[level]] - 1)
        def _():
            prev_copies[level].start()

    send_prev(1)
    share_copies = []
    for n, step in enumerate(SHARES):
        dx, dy, dz = step
        if dy == 0:
            cut = {0: pl.ds(pad_y, main), 1: pl.ds((side + 1) * pad_y, pad_y), -1: pl.ds(0, pad_y)}[dx]
        else:
            cut = pl.ds(slabs * pad_y + (edge_rows if dy < 0 else 0), edge_rows)
        copy = pltpu.make_async_remote_copy(
            src_ref=shares.at[SIDES.index(dz), cut],
            dst_ref=share_in.at[pl.ds(share_at[n], share_at[n + 1] - share_at[n])],
            send_sem=in_sem.at[n], recv_sem=share_recv,
            device_id=toward(step, 1), device_id_type=MESH,
        )
        share_copies.append(copy)

        @pl.when(valid(step, 1))
        def _():
            copy.start()

    send_prev(0)
    send_prev(2)
    relay(0)

    def keep(where, value, rows=None):
        high, low = halves(value)
        if rows is None:
            where[0][...], where[1][...] = high, low
        else:
            where[0][rows, :] = high
            where[1][rows, :] = low

    def keep_sum(pair):
        return pair[0][...].astype(f32) + pair[1][...].astype(f32)

    def rows_of(raw):
        return raw[:, 0, :] if len(raw.shape) == 3 else raw[...]

    keep(leaf_split, rows_of(leaf_in))
    link_at = [0, 2 * seats[0], 2 * (seats[0] + seats[1])]
    for pair in (link_split, rows0, rows1, big, w0, w1):
        for part in pair:
            clear(part)
    for level, raw in enumerate((first_in, second_in, top_in)):
        value = rows_of(raw)
        span = spans[level]
        for s in range(2):
            at = link_at[level] + s * seats[level]
            keep(link_split, value[s * span:(s + 1) * span], slice(at, at + span))

    clear(fs_seat)
    clear(ftst_seat)
    for s in range(2):
        span, seat = spans[1], seats[1]
        fs_seat[:spans[0], s * seat:s * seat + span] = rows_of(fs_in)[:, s * span:(s + 1) * span]
        span, seat = spans[2], seats[2]
        ftst_seat[:spans[1], s * seat:s * seat + span] = rows_of(st_in)[:, s * span:(s + 1) * span]
        ftst_seat[PITCH:PITCH + spans[0], s * seat:s * seat + span] = (
            rows_of(ft_in)[:, s * span:(s + 1) * span]
        )

    clear(order_seat)
    starts = (0, leaf, leaf + spans[0], leaf + spans[0] + spans[1], order_in.shape[1])
    seated = (0, at_first_level, at_second, at_top)
    order_seat[...] = jnp.full(order_seat.shape, -1e6, f32)
    for begin, end, at in zip(starts, starts[1:], seated):
        order_seat[:, at:at + end - begin] = order_in[:, begin:end].astype(f32)
    order = order_seat[...]
    first = jnp.floor((order + 0.5) / (side_y * side_z))
    rest = order - first * (side_y * side_z)
    second = jnp.floor((rest + 0.5) / side_z)
    third = rest - second * side_z
    cells = order.shape[1]

    def row_iota(count):
        return lax.broadcasted_iota(jnp.int32, (count, cells), 0).astype(f32)

    main_hot = (row_iota(main) == first * pad_y + second).astype(f32)
    edge_id = row_iota(edge_rows)
    near = (edge_id == first + 1) | ((edge_id == slabs - 1) & (first == 0)) | (
        (edge_id == 0) & (first == side - 1)
    )
    pick_hot = jnp.concatenate([
        main_hot,
        (near & (second == 0)).astype(f32),
        (near & (second == side_y - 1)).astype(f32),
    ], 0)
    pieces = []
    for n, value, zero in (
        (0, second * side_z + third, first), (1, first * side_z + third, second),
        (2, first * side_y + second, third), (3, second, first + third * side), (4, first, second + third * side),
    ):
        span = cuts["starts"][n + 1] - cuts["starts"][n]
        pieces.append(((row_iota(span) == value) & (zero == 0)).astype(f32))
    face_hot[...] = jnp.concatenate(pieces, 0).astype(bf16)
    clear(back_hot)
    back_hot[:main, :cells] = main_hot.astype(bf16)
    back_rows = m_tall.shape[1]
    beyond_width = m_beyond.shape[1]
    beyond_id = lax.broadcasted_iota(jnp.int32, (back_rows, beyond_width), 0).astype(f32)
    back_hot[:back_rows, cells:] = (beyond_id == m_beyond[0:1, :]).astype(f32).astype(bf16)
    z_id = lax.broadcasted_iota(jnp.int32, (pad_z, cells), 0).astype(f32)
    beyond_z = lax.broadcasted_iota(jnp.int32, (pad_z, beyond_width), 0).astype(f32)
    z_hot = jnp.concatenate([
        (z_id == third).astype(f32), (beyond_z == m_beyond[1:2, :]).astype(f32)
    ], 1)
    z_beyond = jnp.concatenate([jnp.zeros((1, cells), f32), m_beyond[2:3, :]], 1)
    clear(zed[0])
    clear(zed[1])
    clear(val)
    clear(ordered)
    clear(base_out)
    lane_id = lax.broadcasted_iota(jnp.int32, (LANES, cells), 0).astype(f32)

    def lane_hot(r):
        return (lane_id == third + r * pad_z).astype(f32).astype(bf16)

    def wait_prev(level):
        @pl.when(me[shift_axis[level]] > 0)
        def _():
            prev_copies[level].wait_recv()

    def seat_lanes(value, level):
        span = spans[level]
        row_seat[level][...] = jnp.zeros(row_seat[level].shape, f32)
        for d in range(counts[level]):
            row_seat[level][:, d * PITCH:d * PITCH + span] = value[:, d * span:(d + 1) * span]
        return row_seat[level][...]

    links = dot_back(rows_of(leaf_in), link_split)
    wait_prev(0)
    own0 = seat_lanes(rows_of(rows_in[0]), 0)
    keep(rows0, own0, slice(0, spans[0]))
    keep(w0, own0, slice(at_first_level, at_first_level + spans[0]))
    keep(rows0, seat_lanes(rows_of(prev[0]), 0), slice(seats[0], seats[0] + spans[0]))
    e0 = dot(links[:, :2 * seats[0]], rows0)
    keep(w0, -e0, slice(0, leaf))
    own1 = seat_lanes(rows_of(rows_in[1]), 1)
    keep(rows1, own1, slice(0, spans[1]))
    mine0 = place(groups[0])

    def send_k(target, at):
        pltpu.make_async_remote_copy(
            src_ref=k_own, dst_ref=k_all.at[mine0],
            send_sem=in_sem.at[len(SHARES) + 3], recv_sem=k_sem.at[0],
            device_id=target, device_id_type=MESH,
        ).start()

    def s_send(level):
        return in_sem.at[len(SHARES) + 4 + level]

    def g_send(level):
        return in_sem.at[len(SHARES) + 6 + level]

    def all_slots(buffer, sem, count):
        return pltpu.make_async_copy(
            buffer.at[pl.ds(0, count - 1)], buffer.at[pl.ds(0, count - 1)], sem
        )

    relay(1)
    wait_prev(1)
    keep(rows1, seat_lanes(rows_of(prev[1]), 1), slice(seats[1], seats[1] + spans[1]))
    k_own[...] = dot(fs_seat[...], rows1)
    for_others(groups[0], send_k)
    k_all[mine0] = k_own[...]
    e1 = dot(links[:, 2 * seats[0]:2 * (seats[0] + seats[1])], rows1)
    w1_value = jnp.concatenate([
        -e1, jnp.zeros((at_second - leaf, e1.shape[1]), f32), own1,
        jnp.zeros((at_top - at_second - spans[1], e1.shape[1]), f32),
    ], 0)
    keep(w1, w1_value)
    received = {}
    pltpu.make_async_copy(share_in, share_in, share_recv).wait()
    for n, step in enumerate(SHARES):
        part = share_in[share_at[n]:share_at[n + 1]]
        received[step[:2]] = received[step[:2]] + part if step[:2] in received else part

    total = shares[0, pad_y:pad_y + main] + received[0, 0]
    pieces = [total[:pad_y] + received[1, 0], total[pad_y:main - pad_y], total[main - pad_y:] + received[-1, 0]]
    edge_lane = lax.broadcasted_iota(jnp.int32, (edge_rows, LANES), 0)
    inside = (edge_lane >= 1) & (edge_lane <= side)
    for dy in (1, -1):
        tile = jnp.where(inside, received[0, dy], 0.0)
        tile = tile + jnp.where(edge_lane == slabs - 1, received[1, dy], 0.0)
        if (-1, dy) in received:
            tile = tile + jnp.where(edge_lane == 0, received[-1, dy], 0.0)
        pieces.append(tile)
    coarse = jnp.concatenate(pieces, 0)
    for r in range(rhs):
        spread = dot_exact(coarse, lane_hot(r))
        picked[slot(r):slot(r) + 1, :] = jnp.sum(spread * pick_hot, axis=0, keepdims=True)

    def scatter(level, terms, pitch, lane):
        span, group = spans[level], groups[level]
        out, into = scatter_out[level], scatter_in[level]
        for d in range(counts[level]):
            part = terms[:, d * pitch:d * pitch + span]
            if level == 2:
                out[d, :, :span] = part[:pack]
                out[d, :, LANES // 2:LANES // 2 + span] = part[pack:]
            else:
                out[d, :, lane:lane + span] = part
        mine = place(group)

        def send(target, d):
            pltpu.make_async_remote_copy(
                src_ref=out.at[d], dst_ref=into.at[mine],
                send_sem=s_send(level), recv_sem=s_recv.at[level],
                device_id=target, device_id_type=MESH,
            ).start()

        for_others(group, send)
        into[mine] = out[mine]

    def scatter_end(level):
        into = scatter_in[level]
        all_slots(into, s_recv.at[level], counts[level]).wait()
        return jnp.sum(into[...], axis=0)

    def gather(level, value):
        group = groups[level]
        into, own = gather_in[level], stage[level]
        mine = place(group)
        own[...] = value
        if level == 1:
            for target in itertools.product(range(peers["gy"]), range(n_gz)):
                @pl.when(me["gx"] > 0)
                def _():
                    pltpu.make_async_remote_copy(
                        src_ref=own, dst_ref=upper.at[mine],
                        send_sem=in_sem.at[len(SHARES) + 9], recv_sem=upper_recv,
                        device_id={
                            "gx": me["gx"] - 1, "gy": turned["gy"][-target[0]],
                            "gz": turned["gz"][-target[1]],
                        },
                        device_id_type=MESH,
                    ).start()

        def send(target, d):
            pltpu.make_async_remote_copy(
                src_ref=own, dst_ref=into.at[mine],
                send_sem=g_send(level), recv_sem=g_recv.at[level - 1],
                device_id=target, device_id_type=MESH,
            ).start()

        for_others(group, send)
        into[mine] = own[...]

    def gather_end(level):
        into = gather_in[level]
        all_slots(into, g_recv.at[level - 1], counts[level]).wait()
        return into

    terms0 = dot(picked[:, :at_top], w0)
    base1 = dot(picked[:, :at_top], w1)
    all_slots(k_all, k_sem.at[0], n_gz).wait()
    keep(kay, k_all[...].reshape(n_gz * PITCH, k_own.shape[1]))
    scatter(1, base1 - dot(terms0, kay), PITCH, 0)
    scatter(0, terms0, PITCH, PITCH)
    relay(2)
    w0_value = keep_sum(w0)
    gap_width, lead_width = widths[1], widths[0]
    gap_part = halves(keep_sum(w1) - dot(w0_value, kay))
    lead_part = (w0[0][...], w0[1][...])
    lead_at = 2 * gap_width

    def lead_cut(dx, dy):
        at = lead_at + (2 * dx + dy) * lead_width
        return slice(at, at + lead_width)

    def gap_cut(dx):
        return slice(dx * gap_width, (dx + 1) * gap_width)

    for part in range(2):
        zed[part][:at_top, gap_cut(0)] = gap_part[part]
        zed[part][:at_top, lead_cut(0, 0)] = lead_part[part]
    hot = face_hot[:, :at_top]
    face_out[:, :gap_width] = single(hot, gap_part[0]) + single(hot, gap_part[1])
    face_out[:, gap_width:back_width] = single(hot, lead_part[0]) + single(hot, lead_part[1])
    for n, step in enumerate(SHARES):
        @pl.when(valid(step, 1))
        def _():
            share_copies[n].wait_send()
    face_copies = []
    base_copies = []
    for n, step in enumerate(RIMS):
        start, rows, at = cuts[step]
        face_copies.append(pltpu.make_async_remote_copy(
            src_ref=face_out.at[pl.ds(start, rows), pl.ds(0, back_width)],
            dst_ref=face_in.at[pl.ds(at, rows), pl.ds(0, back_width)],
            send_sem=in_sem.at[n], recv_sem=face_recv,
            device_id=toward(step, -1), device_id_type=MESH,
        ))
        base_copies.append(pltpu.make_async_remote_copy(
            src_ref=base_out, dst_ref=base_in.at[n],
            send_sem=in_sem.at[len(RIMS) + n], recv_sem=base_recv,
            device_id=toward(step, -1), device_id_type=MESH,
        ))

        @pl.when(valid(step, -1))
        def _():
            face_copies[n].start()

    leaf_rhs = picked[:, :leaf]
    lows = dot(leaf_rhs, halves(links[:, 2 * (seats[0] + seats[1]):]))
    pair2 = 2 * seats[2]
    slots[...] = -lows
    slots[:, :spans[2]] = picked[:, at_top:at_top + spans[2]] - lows[:, :spans[2]]

    wait_prev(2)
    keep(big, rows_of(rows_in[2]), slice(0, spans[2]))
    keep(big, rows_of(prev[2]), slice(seats[2], seats[2] + spans[2]))
    rows2 = (big[0].at[pl.ds(0, pair2)], big[1].at[pl.ds(0, pair2)])
    queue = slice(LANES, LANES + 2 * PITCH)
    keep(big, dot(ftst_seat[...], rows2), queue)
    base2 = dot(slots[...], rows2)
    first_own = scatter_end(0)
    queue_rows = (big[0].at[queue], big[1].at[queue])
    base2 = base2 - dot(first_own[:, :2 * PITCH], queue_rows)
    leaf_solved = dot(leaf_rhs, leaf_split)
    second_own = scatter_end(1)
    for step in range(3, n_gx):
        relay(step)
    scatter(2, base2 - dot(second_own[:, :2 * PITCH], queue_rows), spans[2], 0)
    both_own = (first_own + second_own)[:, :2 * PITCH]
    top_links = links[:, 2 * (seats[0] + seats[1]):]
    link_high, link_low = halves(top_links)
    hot = face_hot[:, :leaf]
    keep(face_top, -(single(hot, link_high) + single(hot, link_low)))
    for part in range(1):
        face_top[part][:, :spans[2]] = (
            face_top[part][:, :spans[2]].astype(f32) + face_hot[:, at_top:at_top + spans[2]].astype(f32)
        ).astype(bf16)
    leaf_base = dot_back(leaf_solved, leaf_split)
    base0 = dot_exact(leaf_base, hot, single_back)
    top_own = scatter_end(2)
    gather(2, top_own)
    into = gather_end(2)
    for d in range(counts[2]):
        at = slice(d * spans[2], (d + 1) * spans[2])
        top_all[:pack, at] = into[d, :, :spans[2]]
        top_all[pack:, at] = into[d, :, LANES // 2:LANES // 2 + spans[2]]
    solved = dot_back(top_all[...], big)
    gap = both_own - solved[:, LANES:LANES + 2 * PITCH]
    gather(1, jnp.concatenate([gap[:pack], gap[pack:]], 1))
    top_pair = solved[:, :pair2]
    base_out[:rhs, :face_hot.shape[0]] = base0 + dot_back(top_pair, face_top)
    for n, step in enumerate(RIMS):
        @pl.when(valid(step, -1))
        def _():
            base_copies[n].start()

    base = leaf_base - dot_back(top_pair, halves(top_links))
    arrived = face_in.at[pl.ds(0, sum(cuts[step][1] for step in RIMS))]
    pltpu.make_async_copy(arrived, arrived, face_recv).wait()
    for n, step in enumerate(RIMS):
        dx, dy, dz = step
        _, rows, at = cuts[step]
        where = slice(cells + at, cells + at + rows)
        value = face_in[at:at + rows]
        for part, piece in zip(zed, halves(value[:, :gap_width])):
            part[where, gap_cut(dx)] = piece
        for part, piece in zip(zed, halves(value[:, gap_width:])):
            part[where, lead_cut(dx, dy)] = piece

    for level in range(3):
        @pl.when(me[shift_axis[level]] < peers[shift_axis[level]] - 1)
        def _():
            prev_copies[level].wait_send()

        all_slots(scatter_out[level], s_send(level), counts[level]).wait()
    all_slots(k_all, in_sem.at[len(SHARES) + 3], n_gz).wait()
    all_slots(gather_in[2], g_send(2), counts[2]).wait()
    for n, step in enumerate(RIMS):
        @pl.when(valid(step, -1))
        def _():
            face_copies[n].wait_send()

    into = gather_end(1)
    @pl.when(me["gx"] < n_gx - 1)
    def _():
        pltpu.make_async_copy(upper, upper, upper_recv).wait()

    far_gy = jnp.minimum(me["gy"] + 1, peers["gy"] - 1)
    middle = LANES // 2
    for dx, source in enumerate((into, upper)):
        for d in range(counts[1]):
            at = dx * gap_width + d * PITCH
            val[:pack, at:at + spans[1]] = source[d, :, :spans[1]]
            val[pack:, at:at + spans[1]] = source[d, :, middle:middle + spans[1]]
        for dy, gy in enumerate((me["gy"], far_gy)):
            for d in range(n_gz):
                at = lead_at + (2 * dx + dy) * lead_width + d * PITCH
                lead = source[gy * n_gz + d]
                val[:pack, at:at + spans[0]] = lead[:, PITCH:PITCH + spans[0]]
                val[pack:, at:at + spans[0]] = lead[:, middle + PITCH:middle + PITCH + spans[0]]
    back = dot_back(val[...], zed)
    pltpu.make_async_copy(base_in, base_in, base_recv).wait()
    ordered[:rhs, :at_top] = back[:, :at_top]
    ordered[:rhs, :leaf] = back[:, :leaf] + base
    ordered[:rhs, at_top:at_top + spans[2]] = solved[:, :spans[2]]
    for n, step in enumerate(RIMS):
        start, rows, at = cuts[step]
        where = slice(cells + at, cells + at + rows)
        ordered[:rhs, where] = back[:, where] + base_in[n, :rhs, start:start + rows]

    value = ordered[...]
    spread = jnp.concatenate(
        [z_hot * value[slot(r):slot(r) + 1] for r in range(rhs)] + [z_beyond * value], 0
    )
    cells_back = dot_exact(spread, back_hot[:back_rows], single_back)
    high, low = halves(cells_back)
    wide = single(m_wide[...], high) + single(m_wide[...], low)
    high, low = halves(wide)
    out_ref[...] = single_back(m_tall[...], high) + single_back(m_tall[...], low)

    all_slots(gather_in[1], g_send(1), counts[1]).wait()

    @pl.when(me["gx"] > 0)
    def _():
        pltpu.make_async_copy(upper, upper, in_sem.at[len(SHARES) + 9]).wait()

    for n, step in enumerate(RIMS):
        @pl.when(valid(step, -1))
        def _():
            base_copies[n].wait_send()


def spread_kernel(grown_ref, out_ref, held, sem):
    rhs, nx, ny, nz = out_ref.shape
    side = nx // 4
    copies = []
    for r in range(rhs):
        slices = [
            grown_ref[at * ny:(at + 1) * ny, r * nz:(r + 1) * nz] for at in range(side + 1)
        ]
        for x in range(nx):
            at, k = x // 4, x % 4
            if k == 0:
                held[r, x] = slices[at]
            else:
                held[r, x] = (1 - k / 4) * slices[at] + (k / 4) * slices[at + 1]
        copy = pltpu.make_async_copy(held.at[r], out_ref.at[r], sem.at[r])
        copy.start()
        copies.append(copy)
    for copy in copies:
        copy.wait()


def per_device(peers, right_side, iterate, coefficient, ordering, leaf_inverse, leaf_first,
               leaf_second, leaf_top, first_inverse, first_second, first_top, second_inverse,
               second_top, top_inverse):
    rhs, nx, ny, nz = iterate.shape
    side = nx // 4
    slabs = side + 2
    pad_y = up_to(ny // 4, TILE)
    pad_z = LANES // rhs // 4 if nz // 4 <= LANES // rhs // 4 else LANES // rhs
    mats = [jnp.asarray(m, bf16) for m in constants(rhs, ny, nz, side, pad_y, pad_z)]
    mats[-1] = mats[-1].astype(f32)
    flip = lambda m: jnp.swapaxes(m, -1, -2)
    flat = lambda m: m.reshape(m.shape[-2:])
    single_rows = lambda m: m.reshape(m.shape[-2], 1, m.shape[-1])
    rows = [single_rows(first_inverse), single_rows(second_inverse), top_inverse]
    spans = [m.shape[0] for m in rows]
    counts = [m.shape[-1] // s for m, s in zip(rows, spans)]
    seats = [up_to(s, 16) for s in spans]
    seats[0] = seats[1] = PITCH
    widths = [counts[0] * PITCH, up_to(counts[1] * PITCH, LANES), rows[2].shape[-1]]
    leaf = leaf_inverse.shape[-1]
    cells = ordering.shape[-1]
    at_first_level = up_to(leaf, 16)
    at_second = at_first_level + PITCH
    at_top = at_second + PITCH
    slots = up_to(at_top + spans[2], LANES)
    vmem = lambda *shape: pltpu.VMEM(shape, f32)
    split = lambda *shape: [pltpu.VMEM(shape, bf16)] * 2
    like = lambda m: pltpu.VMEM(m.shape, m.dtype)
    dma = lambda n: pltpu.SemaphoreType.DMA((n,))
    sizes = {
        "peers": peers, "pad_y": pad_y, "pad_z": pad_z, "spans": spans, "seats": seats,
        "widths": widths, "starts": (at_first_level, at_second, at_top),
    }
    matrices = (
        ordering.reshape(1, cells), single_rows(leaf_inverse),
        single_rows(flip(leaf_first)), single_rows(flip(leaf_second)), flat(flip(leaf_top)),
        single_rows(first_second), single_rows(first_top), single_rows(second_top),
    )
    edge_rows = up_to(slabs, TILE)
    face_rows = up_to(side, TILE)
    main = side * pad_y
    cuts = face_cuts(side, ny // 4, nz // 4)
    back_width = widths[0] + widths[1]
    face_width = up_to(cuts["rows"], LANES)
    blank_rows = max([main] + [cuts[step][1] for step in RIMS])
    blank = np.zeros((blank_rows + TILE, max(back_width, face_width)), np.float32)
    blank[blank_rows:] = 1.0
    operands = (right_side, iterate, coefficient, *matrices, *rows, *mats, jnp.asarray(blank))

    def share_shape(step):
        dx, dy, _ = step
        return (edge_rows if dy else (pad_y if dx else main), LANES)

    in_vmem = pl.BlockSpec(memory_space=pltpu.VMEM)
    anywhere = pl.BlockSpec(memory_space=pl.ANY)
    links = 2 * sum(seats)
    packs = (rhs, rhs, rhs // 2)
    gather_packs = (rhs, rhs // 2, rhs // 2)
    big_rows = LANES + 2 * PITCH
    grown = pl.pallas_call(
        functools.partial(kernel, sizes),
        out_shape=pltpu.VMEM(((side + 1) * ny, rhs * nz), f32),
        in_specs=jax.tree.map(lambda _: anywhere, operands),
        out_specs=in_vmem,
        scratch_shapes=[
            like(right_side), like(iterate), like(coefficient), *[like(m) for m in matrices],
            [like(m) for m in rows],
            pltpu.VMEM(mats[0].shape[1:], bf16), like(mats[1]),
            pltpu.VMEM(mats[2].shape[1:], bf16), like(mats[3]), like(mats[4]), like(mats[5]),
            split(leaf, leaf),
            split(links, leaf),
            vmem(PITCH, 2 * seats[1]),
            vmem(2 * PITCH, 2 * seats[2]),
            [vmem(spans[level], widths[level]) for level in range(2)],
            split(2 * seats[0], widths[0]),
            split(2 * seats[1], widths[1]),
            split(big_rows, widths[2]),
            split(at_top, widths[0]),
            split(at_top, widths[1]),
            split(slots + cuts["end"], 2 * widths[1] + 4 * widths[0]),
            split(counts[0] * PITCH, widths[1]),
            pltpu.VMEM((cuts["rows"], slots), bf16),
            pltpu.VMEM((up_to(main + pad_y + 2 * face_rows, 16), slots + mats[5].shape[1]), bf16),
            vmem(cuts["rows"], back_width), vmem(cuts["end"], back_width),
            vmem(TILE, face_width), vmem(len(RIMS), TILE, face_width),
            split(cuts["rows"], 2 * seats[2]),
            vmem(counts[1], rhs // 2, LANES),
            vmem(2 * slabs * ny, rhs * nz),
            vmem(3, slabs * pad_y + 2 * edge_rows, LANES),
            vmem(sum(share_shape(step)[0] for step in SHARES), LANES),
            [like(m) for m in rows],
            [vmem(n, p, LANES) for n, p in zip(counts, packs)],
            [vmem(n, p, LANES) for n, p in zip(counts, packs)],
            [vmem(n, p, LANES) for n, p in zip(counts, gather_packs)],
            vmem(rhs, widths[2]),
            vmem(rhs, 2 * widths[1] + 4 * widths[0]),
            vmem(rhs, slots),
            vmem(rhs, 2 * seats[2]),
            vmem(1, slots),
            vmem(TILE, slots + mats[5].shape[1]),
            [vmem(p, LANES) for p in gather_packs],
            vmem(PITCH, widths[1]),
            vmem(counts[0], PITCH, widths[1]),
            dma(max(len(SHARES) + 10, 2 * rhs + len(operands) - 3)),
            pltpu.SemaphoreType.REGULAR((2, max(peers["gx"] - 1, 1))),
            *[pltpu.SemaphoreType.DMA] * 4, dma(3), dma(1), dma(3), dma(2),
        ],
        compiler_params=pltpu.CompilerParams(has_side_effects=True, collective_id=0),
    )(*operands)
    return pl.pallas_call(
        spread_kernel,
        out_shape=jax.ShapeDtypeStruct(iterate.shape, f32),
        in_specs=[in_vmem],
        out_specs=anywhere,
        scratch_shapes=[like(iterate), dma(rhs)],
    )(pltpu.with_memory_space_constraint(grown, pltpu.VMEM))


def solution(mesh):
    peers = dict(mesh.shape)
    return jax.shard_map(
        functools.partial(per_device, peers),
        mesh=mesh,
        in_specs=(
            P(None, "gx", "gy", "gz"),
            P(None, "gx", "gy", "gz"),
            P("gx", "gy", "gz"),
            P("gx", "gy", "gz", None),
            P("gx", "gy", "gz", None, None),
            P("gx", "gy", "gz", None, None),
            P("gx", "gy", "gz", None, None),
            P("gx", "gy", "gz", None, None),
            P("gx", "gy", "gz", None),
            P("gx", "gy", "gz", None, None),
            P("gx", "gy", "gz", None, None),
            P("gx", ("gy", "gz"), None),
            P("gx", "gy", "gz", None, None),
            P(("gx", "gy", "gz"), None),
        ),
        out_specs=P(None, "gx", "gy", "gz"),
        check_vma=False,
    )
```

```python
import functools
import itertools

import jax
import jax.numpy as jnp
import numpy as np
from jax import lax
from jax.experimental import pallas as pl
from jax.experimental.pallas import tpu as pltpu
from jax.sharding import PartitionSpec as P

AXES = ("gx", "gy", "gz")
LANES = 128
TILE = 8
PITCH = 32
UNROLL = 64
SIDES = (0, 1, -1)
MESH = pl.DeviceIdType.MESH
f32 = jnp.float32
bf16 = jnp.bfloat16

SHARES = [
    (i, j, k)
    for i in SIDES
    for j in SIDES
    for k in SIDES
    if (i, j, k) != (0, 0, 0) and (i, j, k).count(-1) <= 1
]
SHARES.sort(key=lambda step: -2 * abs(step[1]) - abs(step[0]))
RIMS = [(i, j, k) for i in (0, 1) for j in (0, 1) for k in (0, 1) if (i, j, k) != (0, 0, 0)]
RIMS.sort(key=lambda step: -2 * step[0] - step[1])


def up_to(n, unit):
    return -(-n // unit) * unit


def weight(k):
    return max(0, 4 - abs(k)) / 16.0


def weight_beside(k):
    return weight(k - 1) + weight(k + 1)


def single(a, b):
    return jnp.dot(a, b, preferred_element_type=f32)


def single_back(a, b):
    return lax.dot_general(a, b, (((1,), (1,)), ((), ())), preferred_element_type=f32)


def halves(x):
    high = x.astype(bf16)
    return high, (x - high.astype(f32)).astype(bf16)


def stacked(x):
    high = x.astype(bf16).astype(f32)
    return jnp.concatenate([high, x - high], axis=0).astype(bf16)


def dot_exact(a, b, product=single):
    count = a.shape[0]
    both = product(stacked(a), b)
    return both[:count] + both[count:]


def dot(a, b, product=single):
    count = a.shape[0]
    both = product(stacked(a), b[0][...])
    return both[:count] + both[count:] + product(a.astype(bf16), b[1][...])


def dot_back(a, b):
    return dot(a, b, single_back)


def coarse_at(side, row, count):
    if side == 0:
        return row if row < count else None
    if side == 1:
        return count if row == 0 else None
    return -1 if row == count - 1 else None


def restriction(fine, pad, stencil):
    count = fine // 4
    out = np.zeros((3, pad, fine), np.float32)
    for s, side in enumerate(SIDES):
        for row in range(pad):
            at = coarse_at(side, row, count)
            if at is not None:
                for y in range(fine):
                    out[s, row, y] = stencil(y - 4 * at)
    return out


def at_first(table):
    table = table.copy()
    table[0, 0, 0] -= weight(-1)
    return table


def interpolation(fine, pad):
    count = fine // 4
    out = np.zeros((2, fine, pad), np.float32)
    for y in range(fine):
        for at in (y // 4, y // 4 + 1):
            value = 1.0 - abs(y - 4 * at) / 4.0
            if at < count:
                out[0, y, at] = value
            else:
                out[1, y, 0] = value
    return out


def face_cuts(side, side_y, side_z):
    faces = [side_y * side_z, side * side_z, side * side_y, side_y, side]
    starts = [0]
    for n in faces:
        starts.append(starts[-1] + up_to(n, 16))
    source = {
        (1, 0, 0): (0, 0), (0, 1, 0): (1, 1), (0, 0, 1): (2, 2), (1, 1, 0): (0, None),
        (1, 0, 1): (3, 3), (0, 1, 1): (4, 4), (1, 1, 1): (0, None),
    }
    cuts, at = {"rows": starts[-1], "starts": starts}, 0
    for dx in (0, 1):
        for step in RIMS:
            if step[0] == dx:
                face, size = source[step]
                rows = up_to(side_z if size is None else faces[size], TILE)
                cuts[step] = (starts[face], rows, at)
                at += up_to(rows, 16)
        at = up_to(at, LANES)
        cuts[dx] = at
    cuts["end"] = at
    return cuts


def constants(rhs, ny, nz, side, pad_y, pad_z):
    slabs = side + 2
    edge_rows = up_to(slabs, TILE)
    last = ny // 4 - 1
    eye = np.eye(slabs, dtype=np.float32)
    eye_edge = np.eye(edge_rows, slabs, dtype=np.float32)

    def over_rows(table):
        return np.concatenate([
            np.kron(eye, table[0]),
            np.kron(eye_edge, table[1][0:1]),
            np.kron(eye_edge, table[2][last:last + 1]),
        ], 0)

    plain = over_rows(restriction(ny, pad_y, weight))
    beside = restriction(ny, pad_y, weight_beside)
    rows = np.stack([
        np.concatenate([plain, over_rows(b)], 1) for b in (at_first(beside), beside)
    ])

    def over_lanes(table):
        out = np.zeros((3, rhs * nz, LANES), np.float32)
        for s in range(3):
            for r in range(rhs):
                out[s, r * nz:(r + 1) * nz, r * pad_z:(r + 1) * pad_z] = table[s].T
        return np.concatenate(list(out), 1)

    lanes = over_lanes(restriction(nz, pad_z, weight))
    table = restriction(nz, pad_z, weight_beside)
    lanes_beside = np.stack([over_lanes(at_first(table)), over_lanes(table)])
    grow = interpolation(nz, pad_z)
    wide = np.zeros((nz, 2 * TILE), np.float32)
    wide[:, :pad_z] = grow[0]
    wide[:, pad_z] = grow[1][:, 0]
    tall_of = interpolation(ny, pad_y)
    slab_rows = side * pad_y
    face_rows = up_to(side, TILE)
    tall = np.zeros(((side + 1) * ny, slab_rows + pad_y + 2 * face_rows), np.float32)
    cuts = face_cuts(side, ny // 4, nz // 4)
    beyond = np.zeros((TILE, up_to(cuts["end"], LANES)), np.float32)
    beyond[:2] = -1.0
    sizes = (side, ny // 4, nz // 4)
    for step in RIMS:
        ranges = [range(1) if d else range(n) for d, n in zip(step, sizes)]
        for at, (x, y, z) in enumerate(itertools.product(*ranges)):
            if step[1]:
                row = slab_rows + pad_y + (face_rows if step[0] else x)
            else:
                row = slab_rows + y if step[0] else x * pad_y + y
            slot = cuts[step][2] + at
            beyond[0, slot] = row
            beyond[1, slot] = -1 if step[2] else z
            beyond[2, slot] = step[2]
    for at in range(side + 1):
        here = slice(at * ny, (at + 1) * ny)
        tall[here, at * pad_y:(at + 1) * pad_y] = tall_of[0]
        corner = slab_rows + pad_y + (at if at < side else face_rows)
        tall[here, corner] = tall_of[1][:, 0]
    return rows / 16.0, lanes, lanes_beside, wide, tall, beyond


def kernel(
    sizes,
    right_ref, u_ref, coef_ref, order_ref, leaf_ref, first_ref, second_ref, top_ref,
    fs_ref, ft_ref, st_ref, rows_first, rows_second, rows_top,
    mat_rows, mat_lanes, mat_beside, mat_wide, mat_tall, mat_beyond, blank,
    out_ref,
    right_in, u_in, coef_in, order_in, leaf_in, first_in, second_in, top_in,
    fs_in, ft_in, st_in, rows_in, m_rows, m_lanes, m_beside, m_wide, m_tall, m_beyond,
    leaf_split, link_split, fs_seat, ftst_seat, row_seat, rows0, rows1, big, w0, w1, zed, zed_up, kay, z_wide, face_hot, back_hot, face_out, face_in, base_out, base_in, face_top, upper,
    packed, shares, share_in, prev, scatter_out, scatter_in, gather_in, top_all, val, val_up,
    picked, slots, order_seat, ordered, stage, k_own, k_all,
    in_sem, ready, share_recv, face_recv, base_recv, upper_recv, prev_recv, k_sem, s_recv, g_recv,
):
    rhs, nx, ny, nz = u_in.shape
    side = nx // 4
    side_y, side_z = ny // 4, nz // 4
    slabs = side + 2
    pad_y, pad_z = sizes["pad_y"], sizes["pad_z"]
    edge_rows = up_to(slabs, TILE)
    main = side * pad_y
    spans, seats, widths = sizes["spans"], sizes["seats"], sizes["widths"]
    leaf = leaf_in.shape[0]
    at_first_level, at_second, at_top = sizes["starts"]
    peers = sizes["peers"]
    me = {a: lax.axis_index(a) for a in AXES}
    groups = (("gz",), ("gy", "gz"), AXES)
    shift_axis = ("gz", "gy", "gx")
    counts = [int(np.prod([peers[a] for a in g])) for g in groups]
    n_gz = peers["gz"]

    def place(group):
        at = 0
        for a in group:
            at = at * peers[a] + me[a]
        return at

    def coords(group, at):
        found = {}
        for a in reversed(group):
            found[a] = at % peers[a]
            at = at // peers[a]
        return {a: found[a] if a in found else me[a] for a in AXES}

    turned = {a: [me[a]] for a in AXES}
    for a in AXES:
        for k in range(1, peers[a]):
            at = me[a] + k
            if peers[a] & (peers[a] - 1):
                turned[a].append(jnp.where(at >= peers[a], at - peers[a], at))
            else:
                turned[a].append(me[a] ^ k)

    n_gx = peers["gx"]
    far = [jnp.where(2 * me["gx"] < n_gx, n_gx - 1 - k, k) for k in range(n_gx)]

    def for_others(group, send):
        count = int(np.prod([peers[a] for a in group]))
        if count <= UNROLL:
            for steps in itertools.product(*[range(peers[a]) for a in group]):
                target = dict(me)
                at = 0
                for a, k in zip(group, steps):
                    target[a] = far[k] if a == "gx" else turned[a][-k]
                    at = at * peers[a] + target[a]
                if any(steps[-2:]):
                    send(target, at)
                elif len(steps) == 3:
                    @pl.when(target["gx"] != me["gx"])
                    def _():
                        send(target, at)
        else:
            mine = place(group)

            def step(k, carry):
                at = (mine + k) % count
                send(coords(group, at), at)
                return carry

            lax.fori_loop(1, count, step, 0)

    def valid(step, sign):
        ok = None
        for a, d in zip(AXES, step):
            if d:
                at = me[a] + sign * d
                this = (at >= 0) & (at < peers[a])
                ok = this if ok is None else ok & this
        return ok

    def toward(step, sign):
        return {a: (me[a] + sign * d + peers[a]) % peers[a] for a, d in zip(AXES, step)}

    barrier = pltpu.get_barrier_semaphore()

    def greet(target, at):
        pl.semaphore_signal(barrier, inc=1, device_id=target, device_id_type=MESH)

    at_y, at_z = jnp.minimum(me["gy"], 1), jnp.minimum(me["gz"], 1)
    loads = {}

    def load(name, source, into):
        loads[name] = pltpu.make_async_copy(source, into, in_sem.at[len(loads)])
        loads[name].start()

    load("coef", coef_ref, coef_in)
    for r in range(rhs):
        load(("u", r), u_ref.at[r], u_in.at[r])
        load(("right", r), right_ref.at[r], right_in.at[r])
    for_others(groups[1], greet)
    for step in itertools.product((1, -1), SIDES, SIDES):
        @pl.when(valid(step, 1))
        def _():
            greet(toward(step, 1), 0)

    load("m_rows", mat_rows.at[at_y], m_rows)
    load("m_lanes", mat_lanes, m_lanes)
    load("m_beside", mat_beside.at[at_z], m_beside)
    pack = rhs // 2

    def slot(r):
        return r % 2 * pack + r // 2

    row_sources = (rows_first, rows_second, rows_top)
    for level in range(3):
        load(("rows", level), row_sources[level], rows_in[level])
    load("leaf", leaf_ref, leaf_in)
    load("first", first_ref, first_in)
    load("second", second_ref, second_in)
    load("top", top_ref, top_in)
    load("order", order_ref, order_in)
    load("fs", fs_ref, fs_in)
    load("ft", ft_ref, ft_in)
    load("st", st_ref, st_in)
    load("m_wide", mat_wide, m_wide)
    load("m_tall", mat_tall, m_tall)
    load("m_beyond", mat_beyond, m_beyond)

    share_at = [0]
    for step in SHARES:
        dx, dy, dz = step
        share_at.append(share_at[-1] + (edge_rows if dy else (pad_y if dx else main)))
    for n, step in enumerate(SHARES):
        @pl.when(jnp.logical_not(valid(step, -1)))
        def _():
            part = pl.ds(share_at[n], share_at[n + 1] - share_at[n])
            pltpu.make_async_copy(
                blank.at[pl.ds(0, share_at[n + 1] - share_at[n]), pl.ds(0, LANES)], share_in.at[part], share_recv
            ).start()
    cuts = face_cuts(side, side_y, side_z)
    back_width = widths[1] + widths[0]
    for n, step in enumerate(RIMS):
        @pl.when(jnp.logical_not(valid(step, 1)))
        def _():
            _, rows, at = cuts[step]
            pltpu.make_async_copy(
                blank.at[pl.ds(0, rows), pl.ds(0, back_width)],
                face_in.at[pl.ds(at, rows), pl.ds(0, back_width)], face_recv
            ).start()
            pltpu.make_async_copy(
                blank.at[pl.ds(0, TILE), pl.ds(0, base_out.shape[1])], base_in.at[n], base_recv.at[step[0]]
            ).start()

    def clear(ref):
        ref[...] = jnp.zeros(ref.shape, ref.dtype)

    def beside(a):
        return jnp.where(me[a] > 0, 1, 0) + jnp.where(me[a] < peers[a] - 1, 1, 0)

    near_count = counts[1] - 1 + beside("gx") * (1 + beside("gy")) * (1 + beside("gz"))

    def relay(step):
        if step:
            @pl.when(me["gx"] >= step)
            def _():
                pl.semaphore_wait(ready.at[0, step - 1], 1)

            @pl.when(me["gx"] + step < n_gx)
            def _():
                pl.semaphore_wait(ready.at[1, step - 1], 1)

        if step < n_gx - 1:
            @pl.when((me["gx"] < n_gx - 1) & (me["gx"] >= step))
            def _():
                pl.semaphore_signal(
                    ready.at[0, step], inc=1, device_id=toward((1, 0, 0), 1), device_id_type=MESH
                )

            @pl.when((me["gx"] > 0) & (me["gx"] + step < n_gx))
            def _():
                pl.semaphore_signal(
                    ready.at[1, step], inc=1, device_id=toward((1, 0, 0), -1), device_id_type=MESH
                )

    for level in range(3):
        @pl.when(me[shift_axis[level]] == 0)
        def _():
            clear(prev[level])

    @pl.when(me["gx"] == n_gx - 1)
    def _():
        clear(upper)

    clear(k_own)
    for level in range(2):
        clear(scatter_out[level])

    half = slabs * ny
    loads["coef"].wait()
    coef_in[...] = coef_in[...] + 6.0
    for r in range(rhs):
        loads["u", r].wait()
        loads["right", r].wait()
        def put(at, value, lower):
            rows = slice((at + 1) * ny + lower, (at + 2) * ny + lower)
            packed[rows, r * nz:(r + 1) * nz] = value

        def source(x):
            q = right_in[r, x] - coef_in[x] * u_in[r, x]
            if x > 0:
                q = q + u_in[r, x - 1]
            return q + u_in[r, x + 1] if x < nx - 1 else q

        first = u_in[r, 0]
        put(-1, first, 0)
        put(-1, jnp.zeros((ny, nz), f32), half)
        q_last = jnp.where(me["gx"] > 0, first, 0.0)
        h_last, u_last, g_last = q_last, None, None
        for at in range(side):
            x = 4 * at
            q = [source(x + k) for k in range(4)]
            h = (q_last + q[1]) + (q[0] + q[0])
            h_next = (q[1] + q[3]) + (q[2] + q[2])
            put(at, (h_last + h_next) + (h + h), 0)
            q_last, h_last = q[3], h_next
            u = [u_in[r, x + k] for k in range(4)]
            g = u[1] + (u[0] + u[0])
            g = g if at == 0 else g + u_last
            g_next = (u[1] + u[3]) + (u[2] + u[2])
            g_sum = g_next + (g + g)
            put(at, g_sum if at == 0 else g_sum + g_last, half)
            u_last, g_last = u[3], g_next
        h = q_last + (u_last + u_last)
        put(side, h_last + (h + h), 0)
        put(side, g_last + (u_last + u_last), half)
    loads["m_rows"].wait()
    loads["m_lanes"].wait()
    loads["m_beside"].wait()
    high, low = halves(packed[...])
    a = single(m_rows[...], high) + single(m_rows[...], low)
    b = single(m_rows[:, :half], high[half:]) + single(m_rows[:, :half], low[half:])
    c = dot_exact(a, m_lanes[...]) + dot_exact(b, m_beside[...])
    for t in range(3):
        shares[t] = c[:, t * LANES:(t + 1) * LANES]

    for name in loads:
        if name not in ("coef", "m_rows", "m_lanes", "m_beside") and name[0] not in ("u", "right"):
            loads[name].wait()
    pl.semaphore_wait(barrier, near_count)

    prev_copies = []
    for level in range(3):
        axis = shift_axis[level]
        target = dict(me)
        target[axis] = (me[axis] + 1) % peers[axis]
        copy = pltpu.make_async_remote_copy(
            src_ref=rows_in[level], dst_ref=prev[level],
            send_sem=in_sem.at[len(SHARES) + level], recv_sem=prev_recv.at[level],
            device_id=target, device_id_type=MESH,
        )
        prev_copies.append(copy)

    def send_prev(level):
        @pl.when(me[shift_axis[level]] < peers[shift_axis[level]] - 1)
        def _():
            prev_copies[level].start()

    send_prev(1)
    share_copies = []
    for n, step in enumerate(SHARES):
        dx, dy, dz = step
        if dy == 0:
            cut = {0: pl.ds(pad_y, main), 1: pl.ds((side + 1) * pad_y, pad_y), -1: pl.ds(0, pad_y)}[dx]
        else:
            cut = pl.ds(slabs * pad_y + (edge_rows if dy < 0 else 0), edge_rows)
        copy = pltpu.make_async_remote_copy(
            src_ref=shares.at[SIDES.index(dz), cut],
            dst_ref=share_in.at[pl.ds(share_at[n], share_at[n + 1] - share_at[n])],
            send_sem=in_sem.at[n], recv_sem=share_recv,
            device_id=toward(step, 1), device_id_type=MESH,
        )
        share_copies.append(copy)

        @pl.when(valid(step, 1))
        def _():
            copy.start()

    send_prev(0)
    send_prev(2)
    relay(0)

    def keep(where, value, rows=None):
        high, low = halves(value)
        if rows is None:
            where[0][...], where[1][...] = high, low
        else:
            where[0][rows, :] = high
            where[1][rows, :] = low

    def keep_sum(pair):
        return pair[0][...].astype(f32) + pair[1][...].astype(f32)

    def rows_of(raw):
        return raw[:, 0, :] if len(raw.shape) == 3 else raw[...]

    keep(leaf_split, rows_of(leaf_in))
    link_at = [0, 2 * seats[0], 2 * (seats[0] + seats[1])]
    for pair in (link_split, rows0, rows1, big, w0, w1):
        for part in pair:
            clear(part)
    for level, raw in enumerate((first_in, second_in, top_in)):
        value = rows_of(raw)
        span = spans[level]
        for s in range(2):
            at = link_at[level] + s * seats[level]
            keep(link_split, value[s * span:(s + 1) * span], slice(at, at + span))

    clear(fs_seat)
    clear(ftst_seat)
    for s in range(2):
        span, seat = spans[1], seats[1]
        fs_seat[:spans[0], s * seat:s * seat + span] = rows_of(fs_in)[:, s * span:(s + 1) * span]
        span, seat = spans[2], seats[2]
        ftst_seat[:spans[1], s * seat:s * seat + span] = rows_of(st_in)[:, s * span:(s + 1) * span]
        ftst_seat[PITCH:PITCH + spans[0], s * seat:s * seat + span] = (
            rows_of(ft_in)[:, s * span:(s + 1) * span]
        )

    clear(order_seat)
    starts = (0, leaf, leaf + spans[0], leaf + spans[0] + spans[1], order_in.shape[1])
    seated = (0, at_first_level, at_second, at_top)
    order_seat[...] = jnp.full(order_seat.shape, -1e6, f32)
    for begin, end, at in zip(starts, starts[1:], seated):
        order_seat[:, at:at + end - begin] = order_in[:, begin:end].astype(f32)
    order = order_seat[...]
    first = jnp.floor((order + 0.5) / (side_y * side_z))
    rest = order - first * (side_y * side_z)
    second = jnp.floor((rest + 0.5) / side_z)
    third = rest - second * side_z
    cells = order.shape[1]

    def row_iota(count):
        return lax.broadcasted_iota(jnp.int32, (count, cells), 0).astype(f32)

    main_hot = (row_iota(main) == first * pad_y + second).astype(f32)
    edge_id = row_iota(edge_rows)
    near = (edge_id == first + 1) | ((edge_id == slabs - 1) & (first == 0)) | (
        (edge_id == 0) & (first == side - 1)
    )
    pick_hot = jnp.concatenate([
        main_hot,
        (near & (second == 0)).astype(f32),
        (near & (second == side_y - 1)).astype(f32),
    ], 0)
    pieces = []
    for n, value, zero in (
        (0, second * side_z + third, first), (1, first * side_z + third, second),
        (2, first * side_y + second, third), (3, second, first + third * side), (4, first, second + third * side),
    ):
        span = cuts["starts"][n + 1] - cuts["starts"][n]
        pieces.append(((row_iota(span) == value) & (zero == 0)).astype(f32))
    face_hot[...] = jnp.concatenate(pieces, 0).astype(bf16)
    clear(back_hot)
    back_hot[:main, :cells] = main_hot.astype(bf16)
    back_rows = m_tall.shape[1]
    beyond_width = m_beyond.shape[1]
    beyond_id = lax.broadcasted_iota(jnp.int32, (back_rows, beyond_width), 0).astype(f32)
    back_hot[:back_rows, cells:] = (beyond_id == m_beyond[0:1, :]).astype(f32).astype(bf16)
    z_id = lax.broadcasted_iota(jnp.int32, (pad_z, cells), 0).astype(f32)
    beyond_z = lax.broadcasted_iota(jnp.int32, (pad_z, beyond_width), 0).astype(f32)
    z_hot = jnp.concatenate([
        jnp.concatenate([
            (z_id == third).astype(f32), (beyond_z == m_beyond[1:2, :]).astype(f32)
        ], 1),
        jnp.concatenate([
            jnp.zeros((2 * TILE - pad_z, cells), f32),
            jnp.broadcast_to(m_beyond[2:3, :], (2 * TILE - pad_z, beyond_width)),
        ], 1),
    ], 0)
    z_wide[...] = single(m_wide[...], z_hot.astype(bf16))
    for part in (*zed, *zed_up, val, val_up):
        clear(part)
    clear(ordered)
    clear(base_out)
    lane_id = lax.broadcasted_iota(jnp.int32, (LANES, cells), 0).astype(f32)

    def lane_hot(r):
        return (lane_id == third + r * pad_z).astype(f32).astype(bf16)

    def wait_prev(level):
        @pl.when(me[shift_axis[level]] > 0)
        def _():
            prev_copies[level].wait_recv()

    def seat_lanes(value, level):
        span = spans[level]
        row_seat[level][...] = jnp.zeros(row_seat[level].shape, f32)
        for d in range(counts[level]):
            row_seat[level][:, d * PITCH:d * PITCH + span] = value[:, d * span:(d + 1) * span]
        return row_seat[level][...]

    links = dot_back(rows_of(leaf_in), link_split)
    wait_prev(0)
    own0 = seat_lanes(rows_of(rows_in[0]), 0)
    keep(rows0, own0, slice(0, spans[0]))
    keep(w0, own0, slice(at_first_level, at_first_level + spans[0]))
    keep(rows0, seat_lanes(rows_of(prev[0]), 0), slice(seats[0], seats[0] + spans[0]))
    e0 = dot(links[:, :2 * seats[0]], rows0)
    keep(w0, -e0, slice(0, leaf))
    own1 = seat_lanes(rows_of(rows_in[1]), 1)
    keep(rows1, own1, slice(0, spans[1]))
    mine0 = place(groups[0])

    def send_k(target, at):
        pltpu.make_async_remote_copy(
            src_ref=k_own, dst_ref=k_all.at[mine0],
            send_sem=in_sem.at[len(SHARES) + 3], recv_sem=k_sem.at[0],
            device_id=target, device_id_type=MESH,
        ).start()

    def s_send(level):
        return in_sem.at[len(SHARES) + 4 + level]

    def g_send(level):
        return in_sem.at[len(SHARES) + 6 + level]

    def all_slots(buffer, sem, count):
        return pltpu.make_async_copy(
            buffer.at[pl.ds(0, count - 1)], buffer.at[pl.ds(0, count - 1)], sem
        )

    relay(1)
    wait_prev(1)
    keep(rows1, seat_lanes(rows_of(prev[1]), 1), slice(seats[1], seats[1] + spans[1]))
    k_own[...] = dot(fs_seat[...], rows1)
    for_others(groups[0], send_k)
    k_all[mine0] = k_own[...]
    e1 = dot(links[:, 2 * seats[0]:2 * (seats[0] + seats[1])], rows1)
    w1_value = jnp.concatenate([
        -e1, jnp.zeros((at_second - leaf, e1.shape[1]), f32), own1,
        jnp.zeros((at_top - at_second - spans[1], e1.shape[1]), f32),
    ], 0)
    keep(w1, w1_value)
    received = {}
    pltpu.make_async_copy(share_in, share_in, share_recv).wait()
    for n, step in enumerate(SHARES):
        part = share_in[share_at[n]:share_at[n + 1]]
        received[step[:2]] = received[step[:2]] + part if step[:2] in received else part

    total = shares[0, pad_y:pad_y + main] + received[0, 0]
    pieces = [total[:pad_y] + received[1, 0], total[pad_y:main - pad_y], total[main - pad_y:] + received[-1, 0]]
    edge_lane = lax.broadcasted_iota(jnp.int32, (edge_rows, LANES), 0)
    inside = (edge_lane >= 1) & (edge_lane <= side)
    for dy in (1, -1):
        tile = jnp.where(inside, received[0, dy], 0.0)
        tile = tile + jnp.where(edge_lane == slabs - 1, received[1, dy], 0.0)
        if (-1, dy) in received:
            tile = tile + jnp.where(edge_lane == 0, received[-1, dy], 0.0)
        pieces.append(tile)
    coarse = jnp.concatenate(pieces, 0)
    for r in range(rhs):
        spread = dot_exact(coarse, lane_hot(r))
        picked[slot(r):slot(r) + 1, :] = jnp.sum(spread * pick_hot, axis=0, keepdims=True)

    def scatter(level, terms, pitch, lane):
        span, group = spans[level], groups[level]
        out, into = scatter_out[level], scatter_in[level]
        for d in range(counts[level]):
            part = terms[:, d * pitch:d * pitch + span]
            if level == 2:
                out[d, :, :span] = part[:pack]
                out[d, :, LANES // 2:LANES // 2 + span] = part[pack:]
            else:
                out[d, :, lane:lane + span] = part
        mine = place(group)

        def send(target, d):
            pltpu.make_async_remote_copy(
                src_ref=out.at[d], dst_ref=into.at[mine],
                send_sem=s_send(level), recv_sem=s_recv.at[level],
                device_id=target, device_id_type=MESH,
            ).start()

        for_others(group, send)
        into[mine] = out[mine]

    def scatter_end(level):
        into = scatter_in[level]
        all_slots(into, s_recv.at[level], counts[level]).wait()
        return jnp.sum(into[...], axis=0)

    def gather(level, value):
        group = groups[level]
        into, own = gather_in[level], stage[level]
        mine = place(group)
        own[...] = value
        if level == 1:
            for target in itertools.product(range(peers["gy"]), range(n_gz)):
                @pl.when(me["gx"] > 0)
                def _():
                    pltpu.make_async_remote_copy(
                        src_ref=own, dst_ref=upper.at[mine],
                        send_sem=in_sem.at[len(SHARES) + 9], recv_sem=upper_recv,
                        device_id={
                            "gx": me["gx"] - 1, "gy": turned["gy"][-target[0]],
                            "gz": turned["gz"][-target[1]],
                        },
                        device_id_type=MESH,
                    ).start()

        def send(target, d):
            pltpu.make_async_remote_copy(
                src_ref=own, dst_ref=into.at[mine],
                send_sem=g_send(level), recv_sem=g_recv.at[level - 1],
                device_id=target, device_id_type=MESH,
            ).start()

        for_others(group, send)
        into[mine] = own[...]

    def gather_end(level):
        into = gather_in[level]
        all_slots(into, g_recv.at[level - 1], counts[level]).wait()
        return into

    terms0 = dot(picked[:, :at_top], w0)
    base1 = dot(picked[:, :at_top], w1)
    all_slots(k_all, k_sem.at[0], n_gz).wait()
    keep(kay, k_all[...].reshape(n_gz * PITCH, k_own.shape[1]))
    scatter(1, base1 - dot(terms0, kay), PITCH, 0)
    scatter(0, terms0, PITCH, PITCH)
    relay(2)
    w0_value = keep_sum(w0)
    gap_width, lead_width = widths[1], widths[0]
    gap_part = halves(keep_sum(w1) - dot(w0_value, kay))
    lead_part = (w0[0][...], w0[1][...])
    def lead_cut(dy):
        return slice(gap_width + dy * lead_width, gap_width + (dy + 1) * lead_width)

    for part in range(2):
        zed[part][:at_top, :gap_width] = gap_part[part]
        zed[part][:at_top, lead_cut(0)] = lead_part[part]
    hot = face_hot[:, :at_top]
    face_out[:, :gap_width] = single(hot, gap_part[0]) + single(hot, gap_part[1])
    face_out[:, gap_width:back_width] = single(hot, lead_part[0]) + single(hot, lead_part[1])
    for n, step in enumerate(SHARES):
        @pl.when(valid(step, 1))
        def _():
            share_copies[n].wait_send()
    face_copies = []
    base_copies = []
    for n, step in enumerate(RIMS):
        start, rows, at = cuts[step]
        face_copies.append(pltpu.make_async_remote_copy(
            src_ref=face_out.at[pl.ds(start, rows), pl.ds(0, back_width)],
            dst_ref=face_in.at[pl.ds(at, rows), pl.ds(0, back_width)],
            send_sem=in_sem.at[n], recv_sem=face_recv,
            device_id=toward(step, -1), device_id_type=MESH,
        ))
        base_copies.append(pltpu.make_async_remote_copy(
            src_ref=base_out, dst_ref=base_in.at[n],
            send_sem=in_sem.at[len(RIMS) + n], recv_sem=base_recv.at[step[0]],
            device_id=toward(step, -1), device_id_type=MESH,
        ))

        @pl.when(valid(step, -1))
        def _():
            face_copies[n].start()

    leaf_rhs = picked[:, :leaf]
    lows = dot(leaf_rhs, halves(links[:, 2 * (seats[0] + seats[1]):]))
    pair2 = 2 * seats[2]
    slots[...] = -lows
    slots[:, :spans[2]] = picked[:, at_top:at_top + spans[2]] - lows[:, :spans[2]]

    wait_prev(2)
    keep(big, rows_of(rows_in[2]), slice(0, spans[2]))
    keep(big, rows_of(prev[2]), slice(seats[2], seats[2] + spans[2]))
    rows2 = (big[0].at[pl.ds(0, pair2)], big[1].at[pl.ds(0, pair2)])
    queue = slice(LANES, LANES + 2 * PITCH)
    keep(big, dot(ftst_seat[...], rows2), queue)
    base2 = dot(slots[...], rows2)
    first_own = scatter_end(0)
    queue_rows = (big[0].at[queue], big[1].at[queue])
    base2 = base2 - dot(first_own[:, :2 * PITCH], queue_rows)
    leaf_solved = dot(leaf_rhs, leaf_split)
    second_own = scatter_end(1)
    for step in range(3, n_gx):
        relay(step)
    scatter(2, base2 - dot(second_own[:, :2 * PITCH], queue_rows), spans[2], 0)
    both_own = (first_own + second_own)[:, :2 * PITCH]
    top_links = links[:, 2 * (seats[0] + seats[1]):]
    link_high, link_low = halves(top_links)
    hot = face_hot[:, :leaf]
    keep(face_top, -(single(hot, link_high) + single(hot, link_low)))
    for part in range(1):
        face_top[part][:, :spans[2]] = (
            face_top[part][:, :spans[2]].astype(f32) + face_hot[:, at_top:at_top + spans[2]].astype(f32)
        ).astype(bf16)
    leaf_base = dot_back(leaf_solved, leaf_split)
    base0 = dot_exact(leaf_base, hot, single_back)
    top_own = scatter_end(2)
    gather(2, top_own)
    into = gather_end(2)
    for d in range(counts[2]):
        at = slice(d * spans[2], (d + 1) * spans[2])
        top_all[:pack, at] = into[d, :, :spans[2]]
        top_all[pack:, at] = into[d, :, LANES // 2:LANES // 2 + spans[2]]
    top_value = top_all[...]
    gap = both_own - dot_back(top_value, queue_rows)
    gather(1, jnp.concatenate([gap[:pack], gap[pack:]], 1))
    top_pair = dot_back(top_value, rows2)
    base_out[:rhs, :face_hot.shape[0]] = base0 + dot_back(top_pair, face_top)
    for n, step in enumerate(RIMS):
        @pl.when(valid(step, -1))
        def _():
            base_copies[n].start()

    base = leaf_base - dot_back(top_pair, halves(top_links))
    arrived = face_in.at[pl.ds(0, sum(cuts[step][1] for step in RIMS))]
    pltpu.make_async_copy(arrived, arrived, face_recv).wait()
    for n, step in enumerate(RIMS):
        dx, dy, dz = step
        _, rows, at = cuts[step]
        into = zed_up if dx else zed
        begin = at - cuts[0] if dx else cells + at
        where = slice(begin, begin + rows)
        value = face_in[at:at + rows]
        for part, piece in zip(into, halves(value[:, :gap_width])):
            part[where, :gap_width] = piece
        for part, piece in zip(into, halves(value[:, gap_width:])):
            part[where, lead_cut(dy)] = piece

    for level in range(3):
        @pl.when(me[shift_axis[level]] < peers[shift_axis[level]] - 1)
        def _():
            prev_copies[level].wait_send()

        all_slots(scatter_out[level], s_send(level), counts[level]).wait()
    all_slots(k_all, in_sem.at[len(SHARES) + 3], n_gz).wait()
    all_slots(gather_in[2], g_send(2), counts[2]).wait()
    for n, step in enumerate(RIMS):
        @pl.when(valid(step, -1))
        def _():
            face_copies[n].wait_send()

    into = gather_end(1)
    far_gy = jnp.minimum(me["gy"] + 1, peers["gy"] - 1)
    middle = LANES // 2

    def seat_values(into, source):
        for d in range(counts[1]):
            at = slice(d * PITCH, d * PITCH + spans[1])
            into[:pack, at] = source[d, :, :spans[1]]
            into[pack:, at] = source[d, :, middle:middle + spans[1]]
        for dy, gy in enumerate((me["gy"], far_gy)):
            for d in range(n_gz):
                at = lead_cut(dy).start + d * PITCH
                lead = source[gy * n_gz + d]
                into[:pack, at:at + spans[0]] = lead[:, PITCH:PITCH + spans[0]]
                into[pack:, at:at + spans[0]] = lead[:, middle + PITCH:middle + PITCH + spans[0]]

    def wait_base(dx):
        some = base_in.at[pl.ds(0, sum(step[0] == dx for step in RIMS))]
        pltpu.make_async_copy(some, some, base_recv.at[dx]).wait()

    def beyond_values(back, dx, begin):
        for n, step in enumerate(RIMS):
            if step[0] == dx:
                start, rows, at = cuts[step]
                where = slice(cells + at, cells + at + rows)
                ordered[:rhs, where] = (
                    back[:, at - begin:at - begin + rows] + base_in[n, :rhs, start:start + rows]
                )

    def over_cells(begin, end):
        value = ordered[:, begin:end]
        weights = z_wide[:, begin:end]
        grown = jnp.concatenate([weights * value[slot(r):slot(r) + 1] for r in range(rhs)], 0)
        return dot_exact(grown, back_hot[:back_rows, begin:end], single_back)

    split_at = cells + cuts[0]
    seat_values(val, into)
    back = dot_back(val[...], zed)
    ordered[:rhs, :at_top] = back[:, :at_top]
    ordered[:rhs, :leaf] = back[:, :leaf] + base
    ordered[:rhs, at_top:at_top + spans[2]] = top_pair[:, :spans[2]]
    wait_base(0)
    beyond_values(back[:, cells:], 0, 0)
    wide = over_cells(0, split_at)

    @pl.when(me["gx"] < n_gx - 1)
    def _():
        pltpu.make_async_copy(upper, upper, upper_recv).wait()

    seat_values(val_up, upper)
    back = dot_back(val_up[...], zed_up)
    wait_base(1)
    beyond_values(back, 1, cuts[0])
    wide = wide + over_cells(split_at, cells + cuts["end"])
    high, low = halves(wide)
    out_ref[...] = single_back(m_tall[...], high) + single_back(m_tall[...], low)

    all_slots(gather_in[1], g_send(1), counts[1]).wait()

    @pl.when(me["gx"] > 0)
    def _():
        pltpu.make_async_copy(upper, upper, in_sem.at[len(SHARES) + 9]).wait()

    for n, step in enumerate(RIMS):
        @pl.when(valid(step, -1))
        def _():
            base_copies[n].wait_send()


def spread_kernel(grown_ref, out_ref, held, sem):
    rhs, nx, ny, nz = out_ref.shape
    side = nx // 4
    copies = []
    for r in range(rhs):
        slices = [
            grown_ref[at * ny:(at + 1) * ny, r * nz:(r + 1) * nz] for at in range(side + 1)
        ]
        for x in range(nx):
            at, k = x // 4, x % 4
            if k == 0:
                held[r, x] = slices[at]
            else:
                held[r, x] = (1 - k / 4) * slices[at] + (k / 4) * slices[at + 1]
        copy = pltpu.make_async_copy(held.at[r], out_ref.at[r], sem.at[r])
        copy.start()
        copies.append(copy)
    for copy in copies:
        copy.wait()


def per_device(peers, right_side, iterate, coefficient, ordering, leaf_inverse, leaf_first,
               leaf_second, leaf_top, first_inverse, first_second, first_top, second_inverse,
               second_top, top_inverse):
    rhs, nx, ny, nz = iterate.shape
    side = nx // 4
    slabs = side + 2
    pad_y = up_to(ny // 4, TILE)
    pad_z = LANES // rhs // 4 if nz // 4 <= LANES // rhs // 4 else LANES // rhs
    mats = [jnp.asarray(m, bf16) for m in constants(rhs, ny, nz, side, pad_y, pad_z)]
    mats[-1] = mats[-1].astype(f32)
    flip = lambda m: jnp.swapaxes(m, -1, -2)
    flat = lambda m: m.reshape(m.shape[-2:])
    single_rows = lambda m: m.reshape(m.shape[-2], 1, m.shape[-1])
    rows = [single_rows(first_inverse), single_rows(second_inverse), top_inverse]
    spans = [m.shape[0] for m in rows]
    counts = [m.shape[-1] // s for m, s in zip(rows, spans)]
    seats = [up_to(s, 16) for s in spans]
    seats[0] = seats[1] = PITCH
    widths = [counts[0] * PITCH, up_to(counts[1] * PITCH, LANES), rows[2].shape[-1]]
    leaf = leaf_inverse.shape[-1]
    cells = ordering.shape[-1]
    at_first_level = up_to(leaf, 16)
    at_second = at_first_level + PITCH
    at_top = at_second + PITCH
    slots = up_to(at_top + spans[2], LANES)
    vmem = lambda *shape: pltpu.VMEM(shape, f32)
    split = lambda *shape: [pltpu.VMEM(shape, bf16)] * 2
    like = lambda m: pltpu.VMEM(m.shape, m.dtype)
    dma = lambda n: pltpu.SemaphoreType.DMA((n,))
    sizes = {
        "peers": peers, "pad_y": pad_y, "pad_z": pad_z, "spans": spans, "seats": seats,
        "widths": widths, "starts": (at_first_level, at_second, at_top),
    }
    matrices = (
        ordering.reshape(1, cells), single_rows(leaf_inverse),
        single_rows(flip(leaf_first)), single_rows(flip(leaf_second)), flat(flip(leaf_top)),
        single_rows(first_second), single_rows(first_top), single_rows(second_top),
    )
    edge_rows = up_to(slabs, TILE)
    face_rows = up_to(side, TILE)
    main = side * pad_y
    cuts = face_cuts(side, ny // 4, nz // 4)
    back_width = widths[0] + widths[1]
    face_width = up_to(cuts["rows"], LANES)
    blank_rows = max([main] + [cuts[step][1] for step in RIMS])
    blank = np.zeros((blank_rows + TILE, max(back_width, face_width)), np.float32)
    blank[blank_rows:] = 1.0
    operands = (right_side, iterate, coefficient, *matrices, *rows, *mats, jnp.asarray(blank))

    def share_shape(step):
        dx, dy, _ = step
        return (edge_rows if dy else (pad_y if dx else main), LANES)

    in_vmem = pl.BlockSpec(memory_space=pltpu.VMEM)
    anywhere = pl.BlockSpec(memory_space=pl.ANY)
    links = 2 * sum(seats)
    packs = (rhs, rhs, rhs // 2)
    gather_packs = (rhs, rhs // 2, rhs // 2)
    big_rows = LANES + 2 * PITCH
    grown = pl.pallas_call(
        functools.partial(kernel, sizes),
        out_shape=pltpu.VMEM(((side + 1) * ny, rhs * nz), f32),
        in_specs=jax.tree.map(lambda _: anywhere, operands),
        out_specs=in_vmem,
        scratch_shapes=[
            like(right_side), like(iterate), like(coefficient), *[like(m) for m in matrices],
            [like(m) for m in rows],
            pltpu.VMEM(mats[0].shape[1:], bf16), like(mats[1]),
            pltpu.VMEM(mats[2].shape[1:], bf16), like(mats[3]), like(mats[4]), like(mats[5]),
            split(leaf, leaf),
            split(links, leaf),
            vmem(PITCH, 2 * seats[1]),
            vmem(2 * PITCH, 2 * seats[2]),
            [vmem(spans[level], widths[level]) for level in range(2)],
            split(2 * seats[0], widths[0]),
            split(2 * seats[1], widths[1]),
            split(big_rows, widths[2]),
            split(at_top, widths[0]),
            split(at_top, widths[1]),
            split(slots + cuts[0], widths[1] + 2 * widths[0]),
            split(cuts["end"] - cuts[0], widths[1] + 2 * widths[0]),
            split(counts[0] * PITCH, widths[1]),
            vmem(nz, slots + mats[5].shape[1]),
            pltpu.VMEM((cuts["rows"], slots), bf16),
            pltpu.VMEM((up_to(main + pad_y + 2 * face_rows, 16), slots + mats[5].shape[1]), bf16),
            vmem(cuts["rows"], back_width), vmem(cuts["end"], back_width),
            vmem(TILE, face_width), vmem(len(RIMS), TILE, face_width),
            split(cuts["rows"], 2 * seats[2]),
            vmem(counts[1], rhs // 2, LANES),
            vmem(2 * slabs * ny, rhs * nz),
            vmem(3, slabs * pad_y + 2 * edge_rows, LANES),
            vmem(sum(share_shape(step)[0] for step in SHARES), LANES),
            [like(m) for m in rows],
            [vmem(n, p, LANES) for n, p in zip(counts, packs)],
            [vmem(n, p, LANES) for n, p in zip(counts, packs)],
            [vmem(n, p, LANES) for n, p in zip(counts, gather_packs)],
            vmem(rhs, widths[2]),
            vmem(rhs, widths[1] + 2 * widths[0]),
            vmem(rhs, widths[1] + 2 * widths[0]),
            vmem(rhs, slots),
            vmem(rhs, 2 * seats[2]),
            vmem(1, slots),
            vmem(TILE, slots + mats[5].shape[1]),
            [vmem(p, LANES) for p in gather_packs],
            vmem(PITCH, widths[1]),
            vmem(counts[0], PITCH, widths[1]),
            dma(max(len(SHARES) + 10, 2 * rhs + len(operands) - 3)),
            pltpu.SemaphoreType.REGULAR((2, max(peers["gx"] - 1, 1))),
            *[pltpu.SemaphoreType.DMA] * 2, dma(2), pltpu.SemaphoreType.DMA, dma(3), dma(1), dma(3), dma(2),
        ],
        compiler_params=pltpu.CompilerParams(has_side_effects=True, collective_id=0),
    )(*operands)
    return pl.pallas_call(
        spread_kernel,
        out_shape=jax.ShapeDtypeStruct(iterate.shape, f32),
        in_specs=[in_vmem],
        out_specs=anywhere,
        scratch_shapes=[like(iterate), dma(rhs)],
    )(pltpu.with_memory_space_constraint(grown, pltpu.VMEM))


def solution(mesh):
    peers = dict(mesh.shape)
    return jax.shard_map(
        functools.partial(per_device, peers),
        mesh=mesh,
        in_specs=(
            P(None, "gx", "gy", "gz"),
            P(None, "gx", "gy", "gz"),
            P("gx", "gy", "gz"),
            P("gx", "gy", "gz", None),
            P("gx", "gy", "gz", None, None),
            P("gx", "gy", "gz", None, None),
            P("gx", "gy", "gz", None, None),
            P("gx", "gy", "gz", None, None),
            P("gx", "gy", "gz", None),
            P("gx", "gy", "gz", None, None),
            P("gx", "gy", "gz", None, None),
            P("gx", ("gy", "gz"), None),
            P("gx", "gy", "gz", None, None),
            P(("gx", "gy", "gz"), None),
        ),
        out_specs=P(None, "gx", "gy", "gz"),
        check_vma=False,
    )
```

```python
import functools
import itertools

import jax
import jax.numpy as jnp
import numpy as np
from jax import lax
from jax.experimental import pallas as pl
from jax.experimental.pallas import tpu as pltpu
from jax.sharding import PartitionSpec as P

AXES = ("gx", "gy", "gz")
LANES = 128
TILE = 8
PITCH = 32
UNROLL = 64
SIDES = (0, 1, -1)
MESH = pl.DeviceIdType.MESH
f32 = jnp.float32
bf16 = jnp.bfloat16

SHARES = [
    (i, j, k)
    for i in SIDES
    for j in SIDES
    for k in SIDES
    if (i, j, k) != (0, 0, 0) and (i, j, k).count(-1) <= 1
]
SHARES.sort(key=lambda step: -2 * abs(step[1]) - abs(step[0]))
RIMS = [(i, j, k) for i in (0, 1) for j in (0, 1) for k in (0, 1) if (i, j, k) != (0, 0, 0)]
RIMS.sort(key=lambda step: -2 * step[0] - step[1])


def up_to(n, unit):
    return -(-n // unit) * unit


def weight(k):
    return max(0, 4 - abs(k)) / 16.0


def weight_beside(k):
    return weight(k - 1) + weight(k + 1)


def single(a, b):
    return jnp.dot(a, b, preferred_element_type=f32)


def single_back(a, b):
    return lax.dot_general(a, b, (((1,), (1,)), ((), ())), preferred_element_type=f32)


def halves(x):
    high = x.astype(bf16)
    return high, (x - high.astype(f32)).astype(bf16)


def stacked(x):
    high = x.astype(bf16).astype(f32)
    return jnp.concatenate([high, x - high], axis=0).astype(bf16)


def dot_exact(a, b, product=single):
    count = a.shape[0]
    both = product(stacked(a), b)
    return both[:count] + both[count:]


def dot(a, b, product=single):
    count = a.shape[0]
    both = product(stacked(a), b[0][...])
    return both[:count] + both[count:] + product(a.astype(bf16), b[1][...])


def dot_back(a, b):
    return dot(a, b, single_back)


def coarse_at(side, row, count):
    if side == 0:
        return row if row < count else None
    if side == 1:
        return count if row == 0 else None
    return -1 if row == count - 1 else None


def restriction(fine, pad, stencil):
    count = fine // 4
    out = np.zeros((3, pad, fine), np.float32)
    for s, side in enumerate(SIDES):
        for row in range(pad):
            at = coarse_at(side, row, count)
            if at is not None:
                for y in range(fine):
                    out[s, row, y] = stencil(y - 4 * at)
    return out


def at_first(table):
    table = table.copy()
    table[0, 0, 0] -= weight(-1)
    return table


def interpolation(fine, pad):
    count = fine // 4
    out = np.zeros((2, fine, pad), np.float32)
    for y in range(fine):
        for at in (y // 4, y // 4 + 1):
            value = 1.0 - abs(y - 4 * at) / 4.0
            if at < count:
                out[0, y, at] = value
            else:
                out[1, y, 0] = value
    return out


def face_cuts(side, side_y, side_z):
    faces = [side_y * side_z, side * side_z, side * side_y, side_y, side]
    starts = [0]
    for n in faces:
        starts.append(starts[-1] + up_to(n, 16))
    source = {
        (1, 0, 0): (0, 0), (0, 1, 0): (1, 1), (0, 0, 1): (2, 2), (1, 1, 0): (0, None),
        (1, 0, 1): (3, 3), (0, 1, 1): (4, 4), (1, 1, 1): (0, None),
    }
    cuts, at = {"rows": starts[-1], "starts": starts}, 0
    for dx in (0, 1):
        for step in RIMS:
            if step[0] == dx:
                face, size = source[step]
                rows = up_to(side_z if size is None else faces[size], TILE)
                cuts[step] = (starts[face], rows, at)
                at += up_to(rows, 16)
        at = up_to(at, LANES)
        cuts[dx] = at
    cuts["end"] = at
    return cuts


def constants(rhs, ny, nz, side, pad_y, pad_z):
    slabs = side + 2
    edge_rows = up_to(slabs, TILE)
    last = ny // 4 - 1
    eye = np.eye(slabs, dtype=np.float32)
    eye_edge = np.eye(edge_rows, slabs, dtype=np.float32)

    def over_rows(table):
        return np.concatenate([
            np.kron(eye, table[0]),
            np.kron(eye_edge, table[1][0:1]),
            np.kron(eye_edge, table[2][last:last + 1]),
        ], 0)

    plain = over_rows(restriction(ny, pad_y, weight))
    beside = restriction(ny, pad_y, weight_beside)
    rows = np.stack([
        np.concatenate([plain, over_rows(b)], 1) for b in (at_first(beside), beside)
    ])

    def over_lanes(table):
        out = np.zeros((3, rhs * nz, LANES), np.float32)
        for s in range(3):
            for r in range(rhs):
                out[s, r * nz:(r + 1) * nz, r * pad_z:(r + 1) * pad_z] = table[s].T
        return np.concatenate(list(out), 1)

    lanes = over_lanes(restriction(nz, pad_z, weight))
    table = restriction(nz, pad_z, weight_beside)
    lanes_beside = np.stack([over_lanes(at_first(table)), over_lanes(table)])
    grow = interpolation(nz, pad_z)
    wide = np.zeros((nz, 2 * TILE), np.float32)
    wide[:, :pad_z] = grow[0]
    wide[:, pad_z] = grow[1][:, 0]
    tall_of = interpolation(ny, pad_y)
    slab_rows = side * pad_y
    face_rows = up_to(side, TILE)
    tall = np.zeros(((side + 1) * ny, slab_rows + pad_y + 2 * face_rows), np.float32)
    cuts = face_cuts(side, ny // 4, nz // 4)
    beyond = np.zeros((TILE, up_to(cuts["end"], LANES)), np.float32)
    beyond[:2] = -1.0
    sizes = (side, ny // 4, nz // 4)
    for step in RIMS:
        ranges = [range(1) if d else range(n) for d, n in zip(step, sizes)]
        for at, (x, y, z) in enumerate(itertools.product(*ranges)):
            if step[1]:
                row = slab_rows + pad_y + (face_rows if step[0] else x)
            else:
                row = slab_rows + y if step[0] else x * pad_y + y
            slot = cuts[step][2] + at
            beyond[0, slot] = row
            beyond[1, slot] = -1 if step[2] else z
            beyond[2, slot] = step[2]
    for at in range(side + 1):
        here = slice(at * ny, (at + 1) * ny)
        tall[here, at * pad_y:(at + 1) * pad_y] = tall_of[0]
        corner = slab_rows + pad_y + (at if at < side else face_rows)
        tall[here, corner] = tall_of[1][:, 0]
    return rows / 16.0, lanes, lanes_beside, wide, tall, beyond


def kernel(
    sizes,
    right_ref, u_ref, coef_ref, order_ref, leaf_ref, first_ref, second_ref, top_ref,
    fs_ref, ft_ref, st_ref, rows_first, rows_second, rows_top,
    mat_rows, mat_lanes, mat_beside, mat_wide, mat_tall, mat_beyond, blank,
    out_ref,
    fields_in, coef_in, order_in, leaf_in, first_in, second_in, top_in,
    fs_in, ft_in, st_in, rows_in, m_rows, m_lanes, m_beside, m_wide, m_tall, m_beyond,
    leaf_split, link_split, fs_seat, ftst_seat, row_seat, rows0, rows1, big, w0, w1, zed, zed_up, kay, z_wide, face_hot, back_hot, face_out, face_in, base_out, base_in, face_top, upper,
    packed, shares, share_in, prev, scatter_out, scatter_in, gather_in, top_all, val, val_up,
    picked, slots, order_seat, ordered, stage, k_own, k_all,
    in_sem, ready, share_recv, face_recv, base_recv, upper_recv, prev_recv, k_sem, s_recv, g_recv,
):
    rhs, nx, ny, nz = u_ref.shape
    side = nx // 4
    side_y, side_z = ny // 4, nz // 4
    slabs = side + 2
    pad_y, pad_z = sizes["pad_y"], sizes["pad_z"]
    edge_rows = up_to(slabs, TILE)
    main = side * pad_y
    spans, seats, widths = sizes["spans"], sizes["seats"], sizes["widths"]
    leaf = leaf_in.shape[0]
    at_first_level, at_second, at_top = sizes["starts"]
    peers = sizes["peers"]
    me = {a: lax.axis_index(a) for a in AXES}
    groups = (("gz",), ("gy", "gz"), AXES)
    shift_axis = ("gz", "gy", "gx")
    counts = [int(np.prod([peers[a] for a in g])) for g in groups]
    n_gz = peers["gz"]

    def place(group):
        at = 0
        for a in group:
            at = at * peers[a] + me[a]
        return at

    def coords(group, at):
        found = {}
        for a in reversed(group):
            found[a] = at % peers[a]
            at = at // peers[a]
        return {a: found[a] if a in found else me[a] for a in AXES}

    turned = {a: [me[a]] for a in AXES}
    for a in AXES:
        for k in range(1, peers[a]):
            at = me[a] + k
            if peers[a] & (peers[a] - 1):
                turned[a].append(jnp.where(at >= peers[a], at - peers[a], at))
            else:
                turned[a].append(me[a] ^ k)

    n_gx = peers["gx"]
    far = [jnp.where(2 * me["gx"] < n_gx, n_gx - 1 - k, k) for k in range(n_gx)]

    def for_others(group, send):
        count = int(np.prod([peers[a] for a in group]))
        if count <= UNROLL:
            for steps in itertools.product(*[range(peers[a]) for a in group]):
                target = dict(me)
                at = 0
                for a, k in zip(group, steps):
                    target[a] = far[k] if a == "gx" else turned[a][-k]
                    at = at * peers[a] + target[a]
                if any(steps[-2:]):
                    send(target, at)
                elif len(steps) == 3:
                    @pl.when(target["gx"] != me["gx"])
                    def _():
                        send(target, at)
        else:
            mine = place(group)

            def step(k, carry):
                at = (mine + k) % count
                send(coords(group, at), at)
                return carry

            lax.fori_loop(1, count, step, 0)

    def valid(step, sign):
        ok = None
        for a, d in zip(AXES, step):
            if d:
                at = me[a] + sign * d
                this = (at >= 0) & (at < peers[a])
                ok = this if ok is None else ok & this
        return ok

    def toward(step, sign):
        return {a: (me[a] + sign * d + peers[a]) % peers[a] for a, d in zip(AXES, step)}

    barrier = pltpu.get_barrier_semaphore()

    def greet(target, at):
        pl.semaphore_signal(barrier, inc=1, device_id=target, device_id_type=MESH)

    at_y, at_z = jnp.minimum(me["gy"], 1), jnp.minimum(me["gz"], 1)
    loads = {}

    def load(name, source, into):
        loads[name] = pltpu.make_async_copy(source, into, in_sem.at[len(loads)])
        loads[name].start()

    load("coef", coef_ref, coef_in)
    for r in range(rhs):
        for n, whole_field in enumerate((u_ref, right_ref)):
            pltpu.make_async_copy(
                whole_field.at[r], fields_in.at[r, n], in_sem.at[len(loads)]
            ).start()
        loads["fields", r] = pltpu.make_async_copy(
            fields_in.at[r], fields_in.at[r], in_sem.at[len(loads)]
        )
    for_others(groups[1], greet)
    for step in itertools.product((1, -1), SIDES, SIDES):
        @pl.when(valid(step, 1))
        def _():
            greet(toward(step, 1), 0)

    load("m_rows", mat_rows.at[at_y], m_rows)
    load("m_lanes", mat_lanes, m_lanes)
    load("m_beside", mat_beside.at[at_z], m_beside)
    pack = rhs // 2

    def slot(r):
        return r % 2 * pack + r // 2

    row_sources = (rows_first, rows_second, rows_top)
    for level in range(3):
        load(("rows", level), row_sources[level], rows_in[level])
    load("leaf", leaf_ref, leaf_in)
    load("first", first_ref, first_in)
    load("second", second_ref, second_in)
    load("top", top_ref, top_in)
    load("order", order_ref, order_in)
    load("fs", fs_ref, fs_in)
    load("ft", ft_ref, ft_in)
    load("st", st_ref, st_in)
    load("m_wide", mat_wide, m_wide)
    load("m_tall", mat_tall, m_tall)
    load("m_beyond", mat_beyond, m_beyond)

    share_at = [0]
    for step in SHARES:
        dx, dy, dz = step
        share_at.append(share_at[-1] + (edge_rows if dy else (pad_y if dx else main)))
    for n, step in enumerate(SHARES):
        @pl.when(jnp.logical_not(valid(step, -1)))
        def _():
            part = pl.ds(share_at[n], share_at[n + 1] - share_at[n])
            pltpu.make_async_copy(
                blank.at[pl.ds(0, share_at[n + 1] - share_at[n]), pl.ds(0, LANES)], share_in.at[part], share_recv
            ).start()
    cuts = face_cuts(side, side_y, side_z)
    back_width = widths[1] + widths[0]
    for n, step in enumerate(RIMS):
        @pl.when(jnp.logical_not(valid(step, 1)))
        def _():
            _, rows, at = cuts[step]
            pltpu.make_async_copy(
                blank.at[pl.ds(0, rows), pl.ds(0, back_width)],
                face_in.at[pl.ds(at, rows), pl.ds(0, back_width)], face_recv
            ).start()
            pltpu.make_async_copy(
                blank.at[pl.ds(0, TILE), pl.ds(0, base_out.shape[1])], base_in.at[n], base_recv.at[step[0]]
            ).start()

    def clear(ref):
        ref[...] = jnp.zeros(ref.shape, ref.dtype)

    def beside(a):
        return jnp.where(me[a] > 0, 1, 0) + jnp.where(me[a] < peers[a] - 1, 1, 0)

    near_count = counts[1] - 1 + beside("gx") * (1 + beside("gy")) * (1 + beside("gz"))

    def relay(step):
        if step:
            @pl.when(me["gx"] >= step)
            def _():
                pl.semaphore_wait(ready.at[0, step - 1], 1)

            @pl.when(me["gx"] + step < n_gx)
            def _():
                pl.semaphore_wait(ready.at[1, step - 1], 1)

        if step < n_gx - 1:
            @pl.when((me["gx"] < n_gx - 1) & (me["gx"] >= step))
            def _():
                pl.semaphore_signal(
                    ready.at[0, step], inc=1, device_id=toward((1, 0, 0), 1), device_id_type=MESH
                )

            @pl.when((me["gx"] > 0) & (me["gx"] + step < n_gx))
            def _():
                pl.semaphore_signal(
                    ready.at[1, step], inc=1, device_id=toward((1, 0, 0), -1), device_id_type=MESH
                )

    for level in range(3):
        @pl.when(me[shift_axis[level]] == 0)
        def _():
            clear(prev[level])

    @pl.when(me["gx"] == n_gx - 1)
    def _():
        clear(upper)

    clear(k_own)
    for level in range(2):
        clear(scatter_out[level])

    half = slabs * ny
    loads["coef"].wait()
    coef_in[...] = coef_in[...] + 6.0
    for r in range(rhs):
        loads["fields", r].wait()
        def put(at, value, lower):
            rows = slice((at + 1) * ny + lower, (at + 2) * ny + lower)
            packed[rows, r * nz:(r + 1) * nz] = value

        def source(x):
            q = fields_in[r, 1, x] - coef_in[x] * fields_in[r, 0, x]
            if x > 0:
                q = q + fields_in[r, 0, x - 1]
            return q + fields_in[r, 0, x + 1] if x < nx - 1 else q

        first = fields_in[r, 0, 0]
        put(-1, first, 0)
        put(-1, jnp.zeros((ny, nz), f32), half)
        q_last = jnp.where(me["gx"] > 0, first, 0.0)
        h_last, u_last, g_last = q_last, None, None
        for at in range(side):
            x = 4 * at
            q = [source(x + k) for k in range(4)]
            h = (q_last + q[1]) + (q[0] + q[0])
            h_next = (q[1] + q[3]) + (q[2] + q[2])
            put(at, (h_last + h_next) + (h + h), 0)
            q_last, h_last = q[3], h_next
            u = [fields_in[r, 0, x + k] for k in range(4)]
            g = u[1] + (u[0] + u[0])
            g = g if at == 0 else g + u_last
            g_next = (u[1] + u[3]) + (u[2] + u[2])
            g_sum = g_next + (g + g)
            put(at, g_sum if at == 0 else g_sum + g_last, half)
            u_last, g_last = u[3], g_next
        h = q_last + (u_last + u_last)
        put(side, h_last + (h + h), 0)
        put(side, g_last + (u_last + u_last), half)
    loads["m_rows"].wait()
    loads["m_lanes"].wait()
    loads["m_beside"].wait()
    high, low = halves(packed[...])
    a = single(m_rows[...], high) + single(m_rows[...], low)
    b = single(m_rows[:, :half], high[half:]) + single(m_rows[:, :half], low[half:])
    c = dot_exact(a, m_lanes[...]) + dot_exact(b, m_beside[...])
    for t in range(3):
        shares[t] = c[:, t * LANES:(t + 1) * LANES]

    for name in loads:
        if name not in ("coef", "m_rows", "m_lanes", "m_beside") and name[0] != "fields":
            loads[name].wait()
    pl.semaphore_wait(barrier, near_count)

    prev_copies = []
    for level in range(3):
        axis = shift_axis[level]
        target = dict(me)
        target[axis] = (me[axis] + 1) % peers[axis]
        copy = pltpu.make_async_remote_copy(
            src_ref=rows_in[level], dst_ref=prev[level],
            send_sem=in_sem.at[len(SHARES) + level], recv_sem=prev_recv.at[level],
            device_id=target, device_id_type=MESH,
        )
        prev_copies.append(copy)

    def send_prev(level):
        @pl.when(me[shift_axis[level]] < peers[shift_axis[level]] - 1)
        def _():
            prev_copies[level].start()

    send_prev(1)
    share_copies = []
    for n, step in enumerate(SHARES):
        dx, dy, dz = step
        if dy == 0:
            cut = {0: pl.ds(pad_y, main), 1: pl.ds((side + 1) * pad_y, pad_y), -1: pl.ds(0, pad_y)}[dx]
        else:
            cut = pl.ds(slabs * pad_y + (edge_rows if dy < 0 else 0), edge_rows)
        copy = pltpu.make_async_remote_copy(
            src_ref=shares.at[SIDES.index(dz), cut],
            dst_ref=share_in.at[pl.ds(share_at[n], share_at[n + 1] - share_at[n])],
            send_sem=in_sem.at[n], recv_sem=share_recv,
            device_id=toward(step, 1), device_id_type=MESH,
        )
        share_copies.append(copy)

        @pl.when(valid(step, 1))
        def _():
            copy.start()

    send_prev(0)
    send_prev(2)
    relay(0)

    def keep(where, value, rows=None):
        high, low = halves(value)
        if rows is None:
            where[0][...], where[1][...] = high, low
        else:
            where[0][rows, :] = high
            where[1][rows, :] = low

    def keep_sum(pair):
        return pair[0][...].astype(f32) + pair[1][...].astype(f32)

    def rows_of(raw):
        return raw[:, 0, :] if len(raw.shape) == 3 else raw[...]

    keep(leaf_split, rows_of(leaf_in))
    link_at = [0, 2 * seats[0], 2 * (seats[0] + seats[1])]
    for pair in (link_split, rows0, rows1, big, w0, w1):
        for part in pair:
            clear(part)
    for level, raw in enumerate((first_in, second_in, top_in)):
        value = rows_of(raw)
        span = spans[level]
        for s in range(2):
            at = link_at[level] + s * seats[level]
            keep(link_split, value[s * span:(s + 1) * span], slice(at, at + span))

    clear(fs_seat)
    clear(ftst_seat)
    for s in range(2):
        span, seat = spans[1], seats[1]
        fs_seat[:spans[0], s * seat:s * seat + span] = rows_of(fs_in)[:, s * span:(s + 1) * span]
        span, seat = spans[2], seats[2]
        ftst_seat[:spans[1], s * seat:s * seat + span] = rows_of(st_in)[:, s * span:(s + 1) * span]
        ftst_seat[PITCH:PITCH + spans[0], s * seat:s * seat + span] = (
            rows_of(ft_in)[:, s * span:(s + 1) * span]
        )

    clear(order_seat)
    starts = (0, leaf, leaf + spans[0], leaf + spans[0] + spans[1], order_in.shape[1])
    seated = (0, at_first_level, at_second, at_top)
    order_seat[...] = jnp.full(order_seat.shape, -1e6, f32)
    for begin, end, at in zip(starts, starts[1:], seated):
        order_seat[:, at:at + end - begin] = order_in[:, begin:end].astype(f32)
    order = order_seat[...]
    first = jnp.floor((order + 0.5) / (side_y * side_z))
    rest = order - first * (side_y * side_z)
    second = jnp.floor((rest + 0.5) / side_z)
    third = rest - second * side_z
    cells = order.shape[1]

    def row_iota(count):
        return lax.broadcasted_iota(jnp.int32, (count, cells), 0).astype(f32)

    main_hot = (row_iota(main) == first * pad_y + second).astype(f32)
    edge_id = row_iota(edge_rows)
    near = (edge_id == first + 1) | ((edge_id == slabs - 1) & (first == 0)) | (
        (edge_id == 0) & (first == side - 1)
    )
    pick_hot = jnp.concatenate([
        main_hot,
        (near & (second == 0)).astype(f32),
        (near & (second == side_y - 1)).astype(f32),
    ], 0)
    pieces = []
    for n, value, zero in (
        (0, second * side_z + third, first), (1, first * side_z + third, second),
        (2, first * side_y + second, third), (3, second, first + third * side), (4, first, second + third * side),
    ):
        span = cuts["starts"][n + 1] - cuts["starts"][n]
        pieces.append(((row_iota(span) == value) & (zero == 0)).astype(f32))
    face_hot[...] = jnp.concatenate(pieces, 0).astype(bf16)
    clear(back_hot)
    back_hot[:main, :cells] = main_hot.astype(bf16)
    back_rows = m_tall.shape[1]
    beyond_width = m_beyond.shape[1]
    beyond_id = lax.broadcasted_iota(jnp.int32, (back_rows, beyond_width), 0).astype(f32)
    back_hot[:back_rows, cells:] = (beyond_id == m_beyond[0:1, :]).astype(f32).astype(bf16)
    z_id = lax.broadcasted_iota(jnp.int32, (pad_z, cells), 0).astype(f32)
    beyond_z = lax.broadcasted_iota(jnp.int32, (pad_z, beyond_width), 0).astype(f32)
    z_hot = jnp.concatenate([
        jnp.concatenate([
            (z_id == third).astype(f32), (beyond_z == m_beyond[1:2, :]).astype(f32)
        ], 1),
        jnp.concatenate([
            jnp.zeros((2 * TILE - pad_z, cells), f32),
            jnp.broadcast_to(m_beyond[2:3, :], (2 * TILE - pad_z, beyond_width)),
        ], 1),
    ], 0)
    z_wide[...] = single(m_wide[...], z_hot.astype(bf16))
    for part in (*zed, *zed_up, val, val_up):
        clear(part)
    clear(ordered)
    clear(base_out)
    lane_id = lax.broadcasted_iota(jnp.int32, (LANES, cells), 0).astype(f32)

    def lane_hot(r):
        return (lane_id == third + r * pad_z).astype(f32).astype(bf16)

    def wait_prev(level):
        @pl.when(me[shift_axis[level]] > 0)
        def _():
            prev_copies[level].wait_recv()

    def seat_lanes(value, level):
        span = spans[level]
        row_seat[level][...] = jnp.zeros(row_seat[level].shape, f32)
        for d in range(counts[level]):
            row_seat[level][:, d * PITCH:d * PITCH + span] = value[:, d * span:(d + 1) * span]
        return row_seat[level][...]

    links = dot_back(rows_of(leaf_in), link_split)
    wait_prev(0)
    own0 = seat_lanes(rows_of(rows_in[0]), 0)
    keep(rows0, own0, slice(0, spans[0]))
    keep(w0, own0, slice(at_first_level, at_first_level + spans[0]))
    keep(rows0, seat_lanes(rows_of(prev[0]), 0), slice(seats[0], seats[0] + spans[0]))
    e0 = dot(links[:, :2 * seats[0]], rows0)
    keep(w0, -e0, slice(0, leaf))
    own1 = seat_lanes(rows_of(rows_in[1]), 1)
    keep(rows1, own1, slice(0, spans[1]))
    mine0 = place(groups[0])

    def send_k(target, at):
        pltpu.make_async_remote_copy(
            src_ref=k_own, dst_ref=k_all.at[mine0],
            send_sem=in_sem.at[len(SHARES) + 3], recv_sem=k_sem.at[0],
            device_id=target, device_id_type=MESH,
        ).start()

    def s_send(level):
        return in_sem.at[len(SHARES) + 4 + level]

    def g_send(level):
        return in_sem.at[2 * len(RIMS) + level]

    def all_slots(buffer, sem, count):
        return pltpu.make_async_copy(
            buffer.at[pl.ds(0, count - 1)], buffer.at[pl.ds(0, count - 1)], sem
        )

    relay(1)
    wait_prev(1)
    keep(rows1, seat_lanes(rows_of(prev[1]), 1), slice(seats[1], seats[1] + spans[1]))
    k_own[...] = dot(fs_seat[...], rows1)
    for_others(groups[0], send_k)
    k_all[mine0] = k_own[...]
    e1 = dot(links[:, 2 * seats[0]:2 * (seats[0] + seats[1])], rows1)
    w1_value = jnp.concatenate([
        -e1, jnp.zeros((at_second - leaf, e1.shape[1]), f32), own1,
        jnp.zeros((at_top - at_second - spans[1], e1.shape[1]), f32),
    ], 0)
    keep(w1, w1_value)
    received = {}
    pltpu.make_async_copy(share_in, share_in, share_recv).wait()
    for n, step in enumerate(SHARES):
        part = share_in[share_at[n]:share_at[n + 1]]
        received[step[:2]] = received[step[:2]] + part if step[:2] in received else part

    total = shares[0, pad_y:pad_y + main] + received[0, 0]
    pieces = [total[:pad_y] + received[1, 0], total[pad_y:main - pad_y], total[main - pad_y:] + received[-1, 0]]
    edge_lane = lax.broadcasted_iota(jnp.int32, (edge_rows, LANES), 0)
    inside = (edge_lane >= 1) & (edge_lane <= side)
    for dy in (1, -1):
        tile = jnp.where(inside, received[0, dy], 0.0)
        tile = tile + jnp.where(edge_lane == slabs - 1, received[1, dy], 0.0)
        if (-1, dy) in received:
            tile = tile + jnp.where(edge_lane == 0, received[-1, dy], 0.0)
        pieces.append(tile)
    coarse = jnp.concatenate(pieces, 0)
    for r in range(rhs):
        spread = dot_exact(coarse, lane_hot(r))
        picked[slot(r):slot(r) + 1, :] = jnp.sum(spread * pick_hot, axis=0, keepdims=True)

    def scatter(level, terms, pitch, lane):
        span, group = spans[level], groups[level]
        out, into = scatter_out[level], scatter_in[level]
        for d in range(counts[level]):
            part = terms[:, d * pitch:d * pitch + span]
            if level == 2:
                out[d, :, :span] = part[:pack]
                out[d, :, LANES // 2:LANES // 2 + span] = part[pack:]
            else:
                out[d, :, lane:lane + span] = part
        mine = place(group)

        def send(target, d):
            pltpu.make_async_remote_copy(
                src_ref=out.at[d], dst_ref=into.at[mine],
                send_sem=s_send(level), recv_sem=s_recv.at[level],
                device_id=target, device_id_type=MESH,
            ).start()

        for_others(group, send)
        into[mine] = out[mine]

    def scatter_end(level):
        into = scatter_in[level]
        all_slots(into, s_recv.at[level], counts[level]).wait()
        return jnp.sum(into[...], axis=0)

    def gather(level, value):
        group = groups[level]
        into, own = gather_in[level], stage[level]
        mine = place(group)
        own[...] = value
        if level == 1:
            for target in itertools.product(range(peers["gy"]), range(n_gz)):
                @pl.when(me["gx"] > 0)
                def _():
                    pltpu.make_async_remote_copy(
                        src_ref=own, dst_ref=upper.at[mine],
                        send_sem=in_sem.at[2 * len(RIMS)], recv_sem=upper_recv,
                        device_id={
                            "gx": me["gx"] - 1, "gy": turned["gy"][-target[0]],
                            "gz": turned["gz"][-target[1]],
                        },
                        device_id_type=MESH,
                    ).start()

        def send(target, d):
            pltpu.make_async_remote_copy(
                src_ref=own, dst_ref=into.at[mine],
                send_sem=g_send(level), recv_sem=g_recv.at[level - 1],
                device_id=target, device_id_type=MESH,
            ).start()

        for_others(group, send)
        into[mine] = own[...]

    def gather_end(level):
        into = gather_in[level]
        all_slots(into, g_recv.at[level - 1], counts[level]).wait()
        return into

    terms0 = dot(picked[:, :at_top], w0)
    base1 = dot(picked[:, :at_top], w1)
    all_slots(k_all, k_sem.at[0], n_gz).wait()
    keep(kay, k_all[...].reshape(n_gz * PITCH, k_own.shape[1]))
    scatter(1, base1 - dot(terms0, kay), PITCH, 0)
    scatter(0, terms0, PITCH, PITCH)
    relay(2)
    w0_value = keep_sum(w0)
    gap_width, lead_width = widths[1], widths[0]
    gap_part = halves(keep_sum(w1) - dot(w0_value, kay))
    lead_part = (w0[0][...], w0[1][...])
    def lead_cut(dy):
        return slice(gap_width + dy * lead_width, gap_width + (dy + 1) * lead_width)

    for part in range(2):
        zed[part][:at_top, :gap_width] = gap_part[part]
        zed[part][:at_top, lead_cut(0)] = lead_part[part]
    hot = face_hot[:, :at_top]
    face_out[:, :gap_width] = single(hot, gap_part[0]) + single(hot, gap_part[1])
    face_out[:, gap_width:back_width] = single(hot, lead_part[0]) + single(hot, lead_part[1])
    for n, step in enumerate(SHARES):
        @pl.when(valid(step, 1))
        def _():
            share_copies[n].wait_send()
    face_copies = []
    base_copies = []
    for n, step in enumerate(RIMS):
        start, rows, at = cuts[step]
        face_copies.append(pltpu.make_async_remote_copy(
            src_ref=face_out.at[pl.ds(start, rows), pl.ds(0, back_width)],
            dst_ref=face_in.at[pl.ds(at, rows), pl.ds(0, back_width)],
            send_sem=in_sem.at[n], recv_sem=face_recv,
            device_id=toward(step, -1), device_id_type=MESH,
        ))
        base_copies.append(pltpu.make_async_remote_copy(
            src_ref=base_out, dst_ref=base_in.at[n],
            send_sem=in_sem.at[len(RIMS) + n], recv_sem=base_recv.at[step[0]],
            device_id=toward(step, -1), device_id_type=MESH,
        ))

        @pl.when(valid(step, -1))
        def _():
            face_copies[n].start()

    leaf_rhs = picked[:, :leaf]
    lows = dot(leaf_rhs, halves(links[:, 2 * (seats[0] + seats[1]):]))
    pair2 = 2 * seats[2]
    slots[...] = -lows
    slots[:, :spans[2]] = picked[:, at_top:at_top + spans[2]] - lows[:, :spans[2]]

    wait_prev(2)
    keep(big, rows_of(rows_in[2]), slice(0, spans[2]))
    keep(big, rows_of(prev[2]), slice(seats[2], seats[2] + spans[2]))
    rows2 = (big[0].at[pl.ds(0, pair2)], big[1].at[pl.ds(0, pair2)])
    queue = slice(LANES, LANES + 2 * PITCH)
    keep(big, dot(ftst_seat[...], rows2), queue)
    base2 = dot(slots[...], rows2)
    first_own = scatter_end(0)
    queue_rows = (big[0].at[queue], big[1].at[queue])
    base2 = base2 - dot(first_own[:, :2 * PITCH], queue_rows)
    leaf_solved = dot(leaf_rhs, leaf_split)
    second_own = scatter_end(1)
    for step in range(3, n_gx):
        relay(step)
    scatter(2, base2 - dot(second_own[:, :2 * PITCH], queue_rows), spans[2], 0)
    both_own = (first_own + second_own)[:, :2 * PITCH]
    top_links = links[:, 2 * (seats[0] + seats[1]):]
    link_high, link_low = halves(top_links)
    hot = face_hot[:, :leaf]
    keep(face_top, -(single(hot, link_high) + single(hot, link_low)))
    for part in range(1):
        face_top[part][:, :spans[2]] = (
            face_top[part][:, :spans[2]].astype(f32) + face_hot[:, at_top:at_top + spans[2]].astype(f32)
        ).astype(bf16)
    leaf_base = dot_back(leaf_solved, leaf_split)
    base0 = dot_exact(leaf_base, hot, single_back)
    top_own = scatter_end(2)
    gather(2, top_own)
    into = gather_end(2)
    for d in range(counts[2]):
        at = slice(d * spans[2], (d + 1) * spans[2])
        top_all[:pack, at] = into[d, :, :spans[2]]
        top_all[pack:, at] = into[d, :, LANES // 2:LANES // 2 + spans[2]]
    top_value = top_all[...]
    gap = both_own - dot_back(top_value, queue_rows)
    gather(1, jnp.concatenate([gap[:pack], gap[pack:]], 1))
    top_pair = dot_back(top_value, rows2)
    base_out[:rhs, :face_hot.shape[0]] = base0 + dot_back(top_pair, face_top)
    for n, step in enumerate(RIMS):
        @pl.when(valid(step, -1))
        def _():
            base_copies[n].start()

    base = leaf_base - dot_back(top_pair, halves(top_links))
    arrived = face_in.at[pl.ds(0, sum(cuts[step][1] for step in RIMS))]
    pltpu.make_async_copy(arrived, arrived, face_recv).wait()
    for n, step in enumerate(RIMS):
        dx, dy, dz = step
        _, rows, at = cuts[step]
        into = zed_up if dx else zed
        begin = at - cuts[0] if dx else cells + at
        where = slice(begin, begin + rows)
        value = face_in[at:at + rows]
        for part, piece in zip(into, halves(value[:, :gap_width])):
            part[where, :gap_width] = piece
        for part, piece in zip(into, halves(value[:, gap_width:])):
            part[where, lead_cut(dy)] = piece

    for level in range(3):
        @pl.when(me[shift_axis[level]] < peers[shift_axis[level]] - 1)
        def _():
            prev_copies[level].wait_send()

        all_slots(scatter_out[level], s_send(level), counts[level]).wait()
    all_slots(k_all, in_sem.at[len(SHARES) + 3], n_gz).wait()
    all_slots(gather_in[2], g_send(2), counts[2]).wait()
    for n, step in enumerate(RIMS):
        @pl.when(valid(step, -1))
        def _():
            face_copies[n].wait_send()

    into = gather_end(1)
    far_gy = jnp.minimum(me["gy"] + 1, peers["gy"] - 1)
    middle = LANES // 2

    def seat_values(into, source):
        for d in range(counts[1]):
            at = slice(d * PITCH, d * PITCH + spans[1])
            into[:pack, at] = source[d, :, :spans[1]]
            into[pack:, at] = source[d, :, middle:middle + spans[1]]
        for dy, gy in enumerate((me["gy"], far_gy)):
            for d in range(n_gz):
                at = lead_cut(dy).start + d * PITCH
                lead = source[gy * n_gz + d]
                into[:pack, at:at + spans[0]] = lead[:, PITCH:PITCH + spans[0]]
                into[pack:, at:at + spans[0]] = lead[:, middle + PITCH:middle + PITCH + spans[0]]

    def wait_base(dx):
        some = base_in.at[pl.ds(0, sum(step[0] == dx for step in RIMS))]
        pltpu.make_async_copy(some, some, base_recv.at[dx]).wait()

    def beyond_values(back, dx, begin):
        for n, step in enumerate(RIMS):
            if step[0] == dx:
                start, rows, at = cuts[step]
                where = slice(cells + at, cells + at + rows)
                ordered[:rhs, where] = (
                    back[:, at - begin:at - begin + rows] + base_in[n, :rhs, start:start + rows]
                )

    def over_cells(begin, end):
        value = ordered[:, begin:end]
        weights = z_wide[:, begin:end]
        grown = jnp.concatenate([weights * value[slot(r):slot(r) + 1] for r in range(rhs)], 0)
        return dot_exact(grown, back_hot[:back_rows, begin:end], single_back)

    split_at = cells + cuts[0]
    seat_values(val, into)
    back = dot_back(val[...], zed)
    ordered[:rhs, :at_top] = back[:, :at_top]
    ordered[:rhs, :leaf] = back[:, :leaf] + base
    ordered[:rhs, at_top:at_top + spans[2]] = top_pair[:, :spans[2]]
    wait_base(0)
    beyond_values(back[:, cells:], 0, 0)
    wide = over_cells(0, split_at)

    @pl.when(me["gx"] < n_gx - 1)
    def _():
        pltpu.make_async_copy(upper, upper, upper_recv).wait()

    seat_values(val_up, upper)
    back = dot_back(val_up[...], zed_up)
    wait_base(1)
    beyond_values(back, 1, cuts[0])
    wide = wide + over_cells(split_at, cells + cuts["end"])
    high, low = halves(wide)
    out_ref[...] = single_back(m_tall[...], high) + single_back(m_tall[...], low)

    all_slots(gather_in[1], g_send(1), counts[1]).wait()

    @pl.when(me["gx"] > 0)
    def _():
        pltpu.make_async_copy(upper, upper, in_sem.at[2 * len(RIMS)]).wait()

    for n, step in enumerate(RIMS):
        @pl.when(valid(step, -1))
        def _():
            base_copies[n].wait_send()


def spread_kernel(grown_ref, out_ref, held, sem):
    rhs, nx, ny, nz = out_ref.shape
    side = nx // 4
    copies = []
    for r in range(rhs):
        slices = [
            grown_ref[at * ny:(at + 1) * ny, r * nz:(r + 1) * nz] for at in range(side + 1)
        ]
        for x in range(nx):
            at, k = x // 4, x % 4
            if k == 0:
                held[r, x] = slices[at]
            else:
                held[r, x] = (1 - k / 4) * slices[at] + (k / 4) * slices[at + 1]
        copy = pltpu.make_async_copy(held.at[r], out_ref.at[r], sem.at[r])
        copy.start()
        copies.append(copy)
    for copy in copies:
        copy.wait()


def per_device(peers, right_side, iterate, coefficient, ordering, leaf_inverse, leaf_first,
               leaf_second, leaf_top, first_inverse, first_second, first_top, second_inverse,
               second_top, top_inverse):
    rhs, nx, ny, nz = iterate.shape
    side = nx // 4
    slabs = side + 2
    pad_y = up_to(ny // 4, TILE)
    pad_z = LANES // rhs // 4 if nz // 4 <= LANES // rhs // 4 else LANES // rhs
    mats = [jnp.asarray(m, bf16) for m in constants(rhs, ny, nz, side, pad_y, pad_z)]
    mats[-1] = mats[-1].astype(f32)
    flip = lambda m: jnp.swapaxes(m, -1, -2)
    flat = lambda m: m.reshape(m.shape[-2:])
    single_rows = lambda m: m.reshape(m.shape[-2], 1, m.shape[-1])
    rows = [single_rows(first_inverse), single_rows(second_inverse), top_inverse]
    spans = [m.shape[0] for m in rows]
    counts = [m.shape[-1] // s for m, s in zip(rows, spans)]
    seats = [up_to(s, 16) for s in spans]
    seats[0] = seats[1] = PITCH
    widths = [counts[0] * PITCH, up_to(counts[1] * PITCH, LANES), rows[2].shape[-1]]
    leaf = leaf_inverse.shape[-1]
    cells = ordering.shape[-1]
    at_first_level = up_to(leaf, 16)
    at_second = at_first_level + PITCH
    at_top = at_second + PITCH
    slots = up_to(at_top + spans[2], LANES)
    vmem = lambda *shape: pltpu.VMEM(shape, f32)
    split = lambda *shape: [pltpu.VMEM(shape, bf16)] * 2
    like = lambda m: pltpu.VMEM(m.shape, m.dtype)
    dma = lambda n: pltpu.SemaphoreType.DMA((n,))
    sizes = {
        "peers": peers, "pad_y": pad_y, "pad_z": pad_z, "spans": spans, "seats": seats,
        "widths": widths, "starts": (at_first_level, at_second, at_top),
    }
    matrices = (
        ordering.reshape(1, cells), single_rows(leaf_inverse),
        single_rows(flip(leaf_first)), single_rows(flip(leaf_second)), flat(flip(leaf_top)),
        single_rows(first_second), single_rows(first_top), single_rows(second_top),
    )
    edge_rows = up_to(slabs, TILE)
    face_rows = up_to(side, TILE)
    main = side * pad_y
    cuts = face_cuts(side, ny // 4, nz // 4)
    back_width = widths[0] + widths[1]
    face_width = up_to(cuts["rows"], LANES)
    blank_rows = max([main] + [cuts[step][1] for step in RIMS])
    blank = np.zeros((blank_rows + TILE, max(back_width, face_width)), np.float32)
    blank[blank_rows:] = 1.0
    operands = (right_side, iterate, coefficient, *matrices, *rows, *mats, jnp.asarray(blank))

    def share_shape(step):
        dx, dy, _ = step
        return (edge_rows if dy else (pad_y if dx else main), LANES)

    in_vmem = pl.BlockSpec(memory_space=pltpu.VMEM)
    anywhere = pl.BlockSpec(memory_space=pl.ANY)
    links = 2 * sum(seats)
    packs = (rhs, rhs, rhs // 2)
    gather_packs = (rhs, rhs // 2, rhs // 2)
    big_rows = LANES + 2 * PITCH
    grown = pl.pallas_call(
        functools.partial(kernel, sizes),
        out_shape=pltpu.VMEM(((side + 1) * ny, rhs * nz), f32),
        in_specs=jax.tree.map(lambda _: anywhere, operands),
        out_specs=in_vmem,
        scratch_shapes=[
            vmem(rhs, 2, nx, ny, nz), like(coefficient), *[like(m) for m in matrices],
            [like(m) for m in rows],
            pltpu.VMEM(mats[0].shape[1:], bf16), like(mats[1]),
            pltpu.VMEM(mats[2].shape[1:], bf16), like(mats[3]), like(mats[4]), like(mats[5]),
            split(leaf, leaf),
            split(links, leaf),
            vmem(PITCH, 2 * seats[1]),
            vmem(2 * PITCH, 2 * seats[2]),
            [vmem(spans[level], widths[level]) for level in range(2)],
            split(2 * seats[0], widths[0]),
            split(2 * seats[1], widths[1]),
            split(big_rows, widths[2]),
            split(at_top, widths[0]),
            split(at_top, widths[1]),
            split(slots + cuts[0], widths[1] + 2 * widths[0]),
            split(cuts["end"] - cuts[0], widths[1] + 2 * widths[0]),
            split(counts[0] * PITCH, widths[1]),
            vmem(nz, slots + mats[5].shape[1]),
            pltpu.VMEM((cuts["rows"], slots), bf16),
            pltpu.VMEM((up_to(main + pad_y + 2 * face_rows, 16), slots + mats[5].shape[1]), bf16),
            vmem(cuts["rows"], back_width), vmem(cuts["end"], back_width),
            vmem(TILE, face_width), vmem(len(RIMS), TILE, face_width),
            split(cuts["rows"], 2 * seats[2]),
            vmem(counts[1], rhs // 2, LANES),
            vmem(2 * slabs * ny, rhs * nz),
            vmem(3, slabs * pad_y + 2 * edge_rows, LANES),
            vmem(sum(share_shape(step)[0] for step in SHARES), LANES),
            [like(m) for m in rows],
            [vmem(n, p, LANES) for n, p in zip(counts, packs)],
            [vmem(n, p, LANES) for n, p in zip(counts, packs)],
            [vmem(n, p, LANES) for n, p in zip(counts, gather_packs)],
            vmem(rhs, widths[2]),
            vmem(rhs, widths[1] + 2 * widths[0]),
            vmem(rhs, widths[1] + 2 * widths[0]),
            vmem(rhs, slots),
            vmem(rhs, 2 * seats[2]),
            vmem(1, slots),
            vmem(TILE, slots + mats[5].shape[1]),
            [vmem(p, LANES) for p in gather_packs],
            vmem(PITCH, widths[1]),
            vmem(counts[0], PITCH, widths[1]),
            dma(max(len(SHARES) + 7, rhs + len(operands) - 3)),
            pltpu.SemaphoreType.REGULAR((2, max(peers["gx"] - 1, 1))),
            *[pltpu.SemaphoreType.DMA] * 2, dma(2), pltpu.SemaphoreType.DMA, dma(3), dma(1), dma(3), dma(2),
        ],
        compiler_params=pltpu.CompilerParams(has_side_effects=True, collective_id=0),
    )(*operands)
    return pl.pallas_call(
        spread_kernel,
        out_shape=jax.ShapeDtypeStruct(iterate.shape, f32),
        in_specs=[in_vmem],
        out_specs=anywhere,
        scratch_shapes=[like(iterate), dma(rhs)],
    )(pltpu.with_memory_space_constraint(grown, pltpu.VMEM))


def solution(mesh):
    peers = dict(mesh.shape)
    return jax.shard_map(
        functools.partial(per_device, peers),
        mesh=mesh,
        in_specs=(
            P(None, "gx", "gy", "gz"),
            P(None, "gx", "gy", "gz"),
            P("gx", "gy", "gz"),
            P("gx", "gy", "gz", None),
            P("gx", "gy", "gz", None, None),
            P("gx", "gy", "gz", None, None),
            P("gx", "gy", "gz", None, None),
            P("gx", "gy", "gz", None, None),
            P("gx", "gy", "gz", None),
            P("gx", "gy", "gz", None, None),
            P("gx", "gy", "gz", None, None),
            P("gx", ("gy", "gz"), None),
            P("gx", "gy", "gz", None, None),
            P(("gx", "gy", "gz"), None),
        ),
        out_specs=P(None, "gx", "gy", "gz"),
        check_vma=False,
    )
```
